32 devices in a mesh: wide: 2 (over x), context: 4 (over z), tensor: 4 (over y, core).
Axes of the slice: x: 2, y: 2, z: 4, core: 2. Of those that a mesh axis runs over, the one named last changes fastest.
Arguments:
- layer_input: bfloat16 [96, 197, 768], P(('wide', 'tensor')), may hold values from -6 to 6
- qkv_weight: bfloat16 [768, 3, 768], P(('wide', 'tensor'), None, 'context'), may hold values from -0.21875 to 0.21875
- proj_weight: bfloat16 [768, 768], P('context', ('wide', 'tensor')), may hold values from -0.875 to 0.875
- norm_gains: bfloat16 [2, 768], P(None, ('wide', 'tensor')), may hold values from 0.5 to 1.5
- norm_biases: bfloat16 [2, 768], P(None, ('wide', 'tensor')), may hold values from -1.796875 to 1.796875
- router_keys: bfloat16 [768, 8], P(('wide', 'tensor')), may hold values from -0.21875 to 0.21875
- up_weight: bfloat16 [8, 768, 3072], P(('wide', 'context'), None, 'tensor'), may hold values from -0.4375 to 0.4375
- down_weight: bfloat16 [8, 3072, 768], P(('wide', 'context'), 'tensor'), may hold values from -0.4375 to 0.4375
- out_cotangent: bfloat16 [96, 197, 768], P(('wide', 'tensor')), may hold values from -6 to 6
Outputs:
- layer_output: bfloat16 [96, 197, 768], P(('wide', 'tensor'))
- rms_stats: float32 [96, 3], P(('wide', 'tensor'))
- input_grad: bfloat16 [96, 197, 768], P(('wide', 'tensor'))
- qkv_grad: float32 [768, 3, 768], P(('wide', 'tensor'), None, 'context')
- proj_grad: float32 [768, 768], P('context', ('wide', 'tensor'))
- gains_grad: float32 [2, 768], P(None, ('wide', 'tensor'))
- biases_grad: float32 [2, 768], P(None, ('wide', 'tensor'))
- router_grad: float32 [768, 8], P(('wide', 'tensor'))
- up_grad: float32 [8, 768, 3072], P(('wide', 'context'), None, 'tensor')
- down_grad: float32 [8, 3072, 768], P(('wide', 'context'), 'tensor')
The draws below stay inside these ranges and needn't reach their ends.
All inputs are finite; a program needn't handle non-finite values.
Results may differ from the reference program's by a relative error of at most 0.02.
Values may be sent and summed in bfloat16 or wider, within the bound.
A program may use at most 192 MiB of HBM per device.

```python
import math
import jax
import jax.numpy as jnp
from jax import lax

D = 768
HEADS = 12
HEAD_DIM = 64
FF = 3072
L = 197
IMG_DEV = 12
EXPERTS = 8
IMAGES = 96


def raised(values, stream_key, source, target, blocks, factor):
    owner, partner = [(jnp.arange(values.shape[position]) // (values.shape[position] // blocks)).reshape([-1 if axis == position else 1 for axis in range(values.ndim)]) for position in (source, target)]
    chosen = jax.random.permutation(stream_key, blocks)[partner]
    strong = (owner == chosen) | (owner == (partner + blocks // 2) % blocks)
    return jnp.where(strong, factor * values, values)


def level_of(rng, dims, pieces, low, largest):
    level = 1.0
    for dim, shards_of in pieces:
        steps = jax.random.uniform(jax.random.fold_in(jax.random.fold_in(rng, 6), dim), (shards_of,), jnp.float32, low / len(pieces), largest / len(pieces))
        level = level * jnp.repeat(jnp.exp(steps), dims[dim] // shards_of).reshape((-1,) + (1,) * (len(dims) - 1 - dim))
    return level


def normal_values(own_key, extent, deviation, bound, split=(), kind=jnp.bfloat16):
    values = deviation * jax.random.normal(own_key, extent, jnp.float32)
    if split:
        values = values * level_of(own_key, extent, split, -0.22, 0.18)
    return jnp.clip(values, -bound, bound).astype(kind)


def bell_draw_with(own_key, shape, deviation, most, split, heavy, kind=jnp.bfloat16):
    values = deviation * jax.random.normal(own_key, shape, jnp.float32)
    if split:
        values = values * level_of(own_key, shape, split, -0.22, 0.18)
    return jnp.clip(raised(values, jax.random.fold_in(own_key, 3), *heavy), -most, most).astype(kind)


def setup_inputs(seed: int = 0) -> dict:
    arg_keys = jax.random.split(jax.random.key(seed), 10)
    return {
        "layer_input": bell_draw_with(arg_keys[0], (IMAGES, L, D), 1.0, 6.0, ((0, 8),), (0, 2, 8, 2.0)),
        "qkv_weight": normal_values(arg_keys[1], (D, 3, D), D ** -0.5, 0.21875, ((0, 8), (2, 4))),
        "proj_weight": normal_values(arg_keys[2], (D, D), (D // 16) ** -0.5, 0.875, ((0, 4), (1, 8))),
        "norm_gains": jnp.clip(1.0 + 0.1 * jax.random.normal(arg_keys[3], (2, D), jnp.float32), 0.5, 1.5).astype(jnp.bfloat16),
        "norm_biases": normal_values(arg_keys[4], (2, D), 0.3, 1.796875, ((1, 8),)),
        "router_keys": normal_values(arg_keys[5], (D, EXPERTS), D ** -0.5, 0.21875, ((0, 8),)),
        "up_weight": normal_values(arg_keys[6], (EXPERTS, D, FF), (D // 4) ** -0.5, 0.4375, ((0, 8), (2, 4))),
        "down_weight": normal_values(arg_keys[7], (EXPERTS, FF, D), (FF // 16) ** -0.5, 0.4375, ((0, 8), (1, 4))),
        "out_cotangent": bell_draw_with(arg_keys[8], (IMAGES, L, D), 1.0, 6.0, ((0, 8),), (0, 2, 8, 2.0)),
    }


norm_eps = 1e-06
highest = lax.Precision.HIGHEST

@jax.custom_vjp
def low(v):
    return lax.optimization_barrier(v.astype(jnp.bfloat16)).astype(jnp.float32)

@jax.custom_vjp
def low_back(v):
    return v

def low_keep(v):
    return (low(v), None)

def low_pass(kept, grad):
    return (grad,)

def back_keep(v):
    return (v, None)

def back_low(kept, grad):
    return (low(grad),)
low.defvjp(low_keep, low_pass)
low_back.defvjp(back_keep, back_low)

def normalize(values, gain_row, shift_row):
    center = values - lax.optimization_barrier(jnp.mean(values, axis=-1, keepdims=True))
    spread = lax.rsqrt(lax.optimization_barrier(jnp.mean(center * center, axis=-1, keepdims=True)) + norm_eps)
    return center * spread * gain_row + shift_row

def attend_group(packed):
    queries = packed[:, :, 0]
    keyset = packed[:, :, 1]
    valueset = packed[:, :, 2]
    scores = low_back(jnp.einsum('bqhd,bkhd->bhqk', queries, keyset, precision=highest) * 0.125)
    attn_probs = jax.nn.softmax(scores, axis=-1)
    head_mix = jnp.einsum('bhqk,bkhd->bqhd', low(attn_probs), valueset, precision=highest)
    return low_back(low(head_mix))

def root_mean(values):
    return jnp.sqrt(lax.optimization_barrier(jnp.mean(values * values, axis=(1, 2))))

def forward(layer_input, qkv_weight, proj_weight, norm_gains, norm_biases, router_keys, up_weight, down_weight):
    normed = low(normalize(layer_input, norm_gains[0], norm_biases[0]))
    packed = low_back(low(jnp.einsum('bld,dkn->blkn', normed, qkv_weight, precision=highest)))
    packed = packed.reshape(IMAGES // IMG_DEV, IMG_DEV, L, 3, HEADS, HEAD_DIM)
    head_mix = lax.map(jax.checkpoint(attend_group), packed).reshape(IMAGES, L, D)
    attention = low_back(jnp.einsum('bld,de->ble', head_mix, proj_weight, precision=highest))
    residual = layer_input + attention
    second = normalize(residual, norm_gains[1], norm_biases[1])
    tokens = low(second)
    unit_rows = second * lax.rsqrt(lax.optimization_barrier(jnp.sum(second * second, axis=-1, keepdims=True)) + norm_eps)
    keys_unit = router_keys * lax.rsqrt(lax.optimization_barrier(jnp.sum(router_keys * router_keys, axis=0, keepdims=True)) + norm_eps)
    logits = 1.6 * math.sqrt(D) * jnp.einsum('bld,ds->bls', unit_rows, keys_unit, precision=highest)
    dispatch = jax.nn.softmax(logits, axis=1)
    combine = jax.nn.softmax(logits, axis=2)
    slot_rows = low_back(low(jnp.einsum('bls,bld->sbd', low(dispatch), tokens, precision=highest)))
    hidden = low_back(jnp.einsum('sbd,sdf->sbf', slot_rows, up_weight, precision=highest))
    active = low(jax.nn.gelu(hidden))
    expert_out = low_back(low(jnp.einsum('sbf,sfd->sbd', active, down_weight, precision=highest)))
    mixture = low_back(jnp.einsum('bls,sbd->bld', low(combine), expert_out, precision=highest))
    result = residual + mixture
    summary = jnp.stack([root_mean(result), root_mean(attention), root_mean(mixture)], axis=-1)
    return (result, summary)

def reference(layer_input, qkv_weight, proj_weight, norm_gains, norm_biases, router_keys, up_weight, down_weight, out_cotangent):
    primals = tuple((argument.astype(jnp.float32) for argument in (layer_input, qkv_weight, proj_weight, norm_gains, norm_biases, router_keys, up_weight, down_weight)))
    result, pullback, summary = jax.vjp(forward, *primals, has_aux=True)
    gradients = pullback(out_cotangent.astype(jnp.float32))
    return (result.astype(jnp.bfloat16), summary, gradients[0].astype(jnp.bfloat16), gradients[1], gradients[2], gradients[3], gradients[4], gradients[5], gradients[6], gradients[7])
```

```python
import math

import jax
import jax.numpy as jnp
from jax import lax
from jax.sharding import PartitionSpec as P

HEAD_DIM = 64

norm_eps = 1e-06
highest = lax.Precision.HIGHEST
f32 = jnp.float32
bf16 = jnp.bfloat16


def layer_stats(values):
    center = values - jnp.mean(values, axis=-1, keepdims=True)
    spread = lax.rsqrt(jnp.mean(center * center, axis=-1, keepdims=True) + norm_eps)
    return (center * spread, spread)


def norm_back(upstream, scaled, spread):
    return spread * (
        upstream
        - jnp.mean(upstream, axis=-1, keepdims=True)
        - scaled * jnp.mean(upstream * scaled, axis=-1, keepdims=True)
    )


def root_mean(values):
    return jnp.sqrt(jnp.mean(values * values, axis=(1, 2)))


def dot32(spec, a, b, **kw):
    return jnp.einsum(spec, a, b, preferred_element_type=f32, **kw)


def on_device(
    layer_input,
    qkv_weight,
    proj_weight,
    norm_gains,
    norm_biases,
    router_keys,
    up_weight,
    down_weight,
    out_cotangent,
):
    images, length, width = layer_input.shape
    wide_n = lax.axis_size("wide")
    ctx_n = lax.axis_size("context")
    ten_n = lax.axis_size("tensor")
    share = images // ctx_n
    start = lax.axis_index("context") * share
    slots_n = router_keys.shape[1]
    cols = qkv_weight.shape[2]
    rows = qkv_weight.shape[0]
    heads_b = cols // HEAD_DIM
    logit_scale = 1.6 * math.sqrt(width)
    everyone = ("context", "wide", "tensor")
    plane = ("wide", "tensor")

    pack = jnp.concatenate([qkv_weight.reshape(rows, 3 * cols), proj_weight.T], axis=1)
    weights = lax.all_gather(pack, everyone, axis=0, tiled=True).reshape(ctx_n, width, 4 * cols)
    small = jnp.concatenate([norm_gains, norm_biases, router_keys.T], axis=0)
    small = lax.all_gather(small, plane, axis=1, tiled=True).astype(f32)
    gain_vals, bias_vals, router_vals = small[0:2], small[2:4], small[4:].T
    qkv_full = weights[:, :, : 3 * cols]
    proj_t = weights[:, :, 3 * cols :]

    x = lax.dynamic_slice_in_dim(layer_input, start, share, 0).astype(f32)
    g = lax.dynamic_slice_in_dim(out_cotangent, start, share, 0)
    hat1, spread1 = layer_stats(x)
    normed1 = (hat1 * gain_vals[0] + bias_vals[0]).astype(bf16)
    qkv = dot32("bld,cdk->cblk", normed1, qkv_full).astype(bf16)
    qkv = qkv.reshape(ctx_n, share, length, 3, heads_b, HEAD_DIM)
    q, k, v = qkv[:, :, :, 0], qkv[:, :, :, 1], qkv[:, :, :, 2]
    scores = dot32("cbqhd,cbkhd->cbhqk", q, k) * 0.125
    top = jnp.max(scores, axis=-1, keepdims=True)
    exps = jnp.exp(scores - top)
    probs = exps / jnp.sum(exps, axis=-1, keepdims=True)
    probs_low = probs.astype(bf16)
    heads = dot32("cbhqk,cbkhd->cbqhd", probs_low, v).astype(bf16)
    heads = heads.reshape(ctx_n, share, length, cols)
    attention = dot32("cblh,ceh->ble", heads, proj_t)

    residual = x + attention
    hat2, spread2 = layer_stats(residual)
    second = hat2 * gain_vals[1] + bias_vals[1]
    tokens = second.astype(bf16)
    row_scale = lax.rsqrt(jnp.sum(second * second, axis=-1, keepdims=True) + norm_eps)
    unit = second * row_scale
    col_scale = lax.rsqrt(jnp.sum(router_vals * router_vals, axis=0, keepdims=True) + norm_eps)
    keys_unit = router_vals * col_scale
    logits = logit_scale * jnp.einsum("bld,ds->bls", unit, keys_unit, precision=highest)
    dispatch = jax.nn.softmax(logits, axis=1)
    combine = jax.nn.softmax(logits, axis=2)
    dispatch_low = dispatch.astype(bf16)
    combine_low = combine.astype(bf16)
    slots = dot32("bls,bld->sbd", dispatch_low, tokens).astype(bf16)
    dexp = dot32("bls,bld->sbd", combine_low, g).astype(bf16)

    out = jnp.concatenate([slots, dexp], axis=1)
    got = lax.all_to_all(out, ("wide", "context"), split_axis=0, concat_axis=0, tiled=True)
    got = lax.all_gather(got, "tensor", axis=0, tiled=True)
    n = got.shape[0]
    slot_all = got[:, :share].reshape(n * share, width)
    dexp_all = got[:, share:].reshape(n * share, width)
    up, down = up_weight[0], down_weight[0]
    hidden = dot32("rd,df->rf", slot_all, up)
    active = jax.nn.gelu(hidden).astype(bf16)
    part_out = dot32("rf,fd->rd", active, down)
    active_grad = dot32("rd,fd->rf", dexp_all, down)
    hidden_grad = jax.vjp(jax.nn.gelu, hidden)[1](active_grad)[0].astype(bf16)
    down_grad = dot32("rf,rd->fd", active, dexp_all)[None]
    up_grad = dot32("rd,rf->df", slot_all, hidden_grad)[None]
    part_slot = dot32("rf,df->rd", hidden_grad, up)
    back = jnp.concatenate(
        [part_out.reshape(n, share, width), part_slot.reshape(n, share, width)], axis=1
    ).astype(bf16)
    back = lax.psum_scatter(back, "tensor", scatter_dimension=0, tiled=True)
    back = lax.all_to_all(back, ("wide", "context"), split_axis=0, concat_axis=0, tiled=True)
    expert_out = back[:, :share]
    dslots = back[:, share:]

    mixture = dot32("bls,sbd->bld", combine_low, expert_out)
    result = residual + mixture
    rms = jnp.stack([root_mean(result), root_mean(attention), root_mean(mixture)], axis=-1)
    layer_output = lax.all_gather(result.astype(bf16), "context", axis=0, tiled=True)
    dcomb = dot32("bld,sbd->bls", g, expert_out)
    ddisp = dot32("bld,sbd->bls", tokens, dslots)
    dtokens = dot32("bls,sbd->bld", dispatch_low, dslots)
    dlogits = combine * (dcomb - jnp.sum(combine * dcomb, axis=2, keepdims=True)) + dispatch * (
        ddisp - jnp.sum(dispatch * ddisp, axis=1, keepdims=True)
    )
    dunit = logit_scale * jnp.einsum("bls,ds->bld", dlogits, keys_unit, precision=highest)
    dkeys = logit_scale * jnp.einsum("bld,bls->ds", unit, dlogits, precision=highest)
    drouter = col_scale * (dkeys - keys_unit * jnp.sum(keys_unit * dkeys, axis=0, keepdims=True))
    dsecond = dtokens + row_scale * (dunit - unit * jnp.sum(unit * dunit, axis=-1, keepdims=True))
    dgain2 = jnp.sum(dsecond * hat2, axis=(0, 1))
    dbias2 = jnp.sum(dsecond, axis=(0, 1))
    dresid = g.astype(f32) + norm_back(dsecond * gain_vals[1], hat2, spread2)
    dattn = dresid.astype(bf16)
    dproj = dot32("ble,cblh->ceh", dattn, heads)
    dheads = dot32("ble,ceh->cblh", dattn, proj_t).astype(bf16)
    dheads = dheads.reshape(ctx_n, share, length, heads_b, HEAD_DIM)
    dprobs = dot32("cbqhd,cbkhd->cbhqk", dheads, v)
    dv = dot32("cbhqk,cbqhd->cbkhd", probs_low, dheads)
    ds = (probs * (dprobs - jnp.sum(probs * dprobs, axis=-1, keepdims=True))).astype(bf16)
    dq = dot32("cbhqk,cbkhd->cbqhd", ds, k) * 0.125
    dk = dot32("cbhqk,cbqhd->cbkhd", ds, q) * 0.125
    dqkv = jnp.stack([dq, dk, dv], axis=3).astype(bf16).reshape(ctx_n, share, length, 3 * cols)
    dqkv_w = dot32("bld,cblk->cdk", normed1, dqkv)
    dnormed1 = dot32("cblk,cdk->bld", dqkv, qkv_full)
    dgain1 = jnp.sum(dnormed1 * hat1, axis=(0, 1))
    dbias1 = jnp.sum(dnormed1, axis=(0, 1))
    dx = (dresid + norm_back(dnormed1 * gain_vals[0], hat1, spread1)).astype(bf16)
    input_grad = lax.all_gather(dx, "context", axis=0, tiled=True)
    rms = lax.all_gather(rms, "context", axis=0, tiled=True)

    dpack = jnp.concatenate([dqkv_w, dproj], axis=2).reshape(ctx_n * width, 4 * cols)
    dpack = lax.psum_scatter(dpack.astype(bf16), everyone, scatter_dimension=0, tiled=True)
    dpack = dpack.astype(f32)
    dsmall = jnp.concatenate(
        [jnp.stack([dgain1, dgain2, dbias1, dbias2], axis=1), drouter], axis=1
    )
    dsmall = lax.psum(dsmall, "context")
    dsmall = lax.psum_scatter(dsmall, plane, scatter_dimension=0, tiled=True)
    return (
        layer_output,
        rms,
        input_grad,
        dpack[:, : 3 * cols].reshape(rows, 3, cols),
        dpack[:, 3 * cols :].T,
        dsmall[:, 0:2].T,
        dsmall[:, 2:4].T,
        dsmall[:, 4:],
        up_grad,
        down_grad,
    )


def solution(mesh):
    images = P(("wide", "tensor"), None, None)
    qkv = P(("wide", "tensor"), None, "context")
    proj = P("context", ("wide", "tensor"))
    lane = P(None, ("wide", "tensor"))
    rowed = P(("wide", "tensor"), None)
    up = P(("wide", "context"), None, "tensor")
    down = P(("wide", "context"), "tensor", None)
    return jax.shard_map(
        on_device,
        mesh=mesh,
        in_specs=(images, qkv, proj, lane, lane, rowed, up, down, images),
        out_specs=(images, rowed, images, qkv, proj, lane, lane, rowed, up, down),
        check_vma=False,
    )
```

```python
import functools
import math

import jax
import jax.numpy as jnp
from jax import lax
from jax.experimental import pallas as pl
from jax.experimental.pallas import tpu as pltpu
from jax.sharding import PartitionSpec as P

f32 = jnp.float32
bf16 = jnp.bfloat16

HEAD_DIM = 64
norm_eps = 1e-06
highest = lax.Precision.HIGHEST
NN = (((1,), (0,)), ((), ()))
NT = (((1,), (1,)), ((), ()))
TN = (((0,), (0,)), ((), ()))


def mm(a, b, dims=NN, precision=None):
    return lax.dot_general(a, b, dims, precision=precision, preferred_element_type=f32)


def layer_stats(values):
    center = values - jnp.mean(values, axis=-1, keepdims=True)
    spread = lax.rsqrt(jnp.mean(center * center, axis=-1, keepdims=True) + norm_eps)
    return (center * spread, spread)


def norm_back(upstream, scaled, spread):
    return spread * (
        upstream
        - jnp.mean(upstream, axis=-1, keepdims=True)
        - scaled * jnp.mean(upstream * scaled, axis=-1, keepdims=True)
    )


def soft(values, axis):
    e = jnp.exp(values - jnp.max(values, axis=axis, keepdims=True))
    return e / jnp.sum(e, axis=axis, keepdims=True)


def pick_rows(slots_n, row):
    r = lax.broadcasted_iota(jnp.int32, (slots_n * 8, slots_n), 0)
    s = lax.broadcasted_iota(jnp.int32, (slots_n * 8, slots_n), 1)
    return jnp.where(r == s * 8 + row, 1.0, 0.0).astype(bf16)


def router_unit(keys):
    scale = lax.rsqrt(jnp.sum(keys * keys, axis=1, keepdims=True) + norm_eps)
    return keys * scale, scale


def head_parts(block, h, per):
    at = [j * per * HEAD_DIM + h * HEAD_DIM for j in range(3)]
    return [block[:, a : a + HEAD_DIM] for a in at]


def forward_kernel(share, x_all, g_all, full, small, qkv, heads, resid, logits, asq, send, x_s, g_s, rows_s, sems):
    c0 = lax.axis_index("context") * share
    ctx_n, width, packed = full.shape
    cols = packed // 4
    per = cols // HEAD_DIM
    slots_n = small.shape[0] - 4
    length = x_s.shape[1]
    ins = [
        pltpu.make_async_copy(x_all.at[pl.ds(c0, share)], x_s, sems.at[0]),
        pltpu.make_async_copy(g_all.at[pl.ds(c0, share)], g_s, sems.at[1]),
    ]
    for cp in ins:
        cp.start()
    rows_s[...] = jnp.zeros_like(rows_s)
    keys, _ = router_unit(small[4:, :].astype(f32))
    logit_scale = 1.6 * math.sqrt(width)
    for cp in ins:
        cp.wait()

    def image(i, carry):
        x = x_s[i].astype(f32)
        hat, spread = layer_stats(x)
        normed = (hat * small[0:1, :].astype(f32) + small[2:3, :].astype(f32)).astype(bf16)
        resid[i] = x

        def block(cb, carry):
            qkv_c = mm(normed, full[cb, :, : 3 * cols]).astype(bf16)
            qkv[i, cb] = qkv_c
            mixed = []
            for h in range(per):
                q, k, v = head_parts(qkv_c, h, per)
                p = soft(mm(q, k, NT) * 0.125, 1)
                mixed.append(mm(p.astype(bf16), v).astype(bf16))
            heads_c = jnp.concatenate(mixed, axis=1)
            heads[i, cb] = heads_c
            resid[i] += mm(heads_c, full[cb, :, 3 * cols :], NT)
            return carry

        lax.fori_loop(0, ctx_n, block, 0)
        res = resid[i]
        att = res - x
        asq[i] = jnp.full(asq.shape[1:], jnp.sum(att * att), f32)
        hat2, _ = layer_stats(res)
        second = hat2 * small[1:2, :].astype(f32) + small[3:4, :].astype(f32)
        unit = second * lax.rsqrt(jnp.sum(second * second, axis=-1, keepdims=True) + norm_eps)
        lg = logit_scale * mm(keys, unit, NT, highest)
        logits[i] = lg
        disp = soft(lg, 1).astype(bf16)
        comb = soft(lg, 0).astype(bf16)
        slots = mm(disp, second.astype(bf16)).astype(bf16)
        dexp = mm(comb, g_s[i]).astype(bf16)
        rows_s[...] += mm(pick_rows(slots_n, i), slots) + mm(pick_rows(slots_n, i + 4), dexp)
        return carry

    lax.fori_loop(0, share, image, 0)
    send[...] = rows_s[...].astype(bf16)


def run_forward(x_all, g_all, full, small, share):
    ctx_n, width, packed = full.shape
    length = x_all.shape[1]
    cols = packed // 4
    slots_n = small.shape[0] - 4
    vm = pl.BlockSpec(memory_space=pltpu.VMEM)
    hbm = pl.BlockSpec(memory_space=pl.ANY)
    return pl.pallas_call(
        functools.partial(forward_kernel, share),
        out_shape=(
            jax.ShapeDtypeStruct((share, ctx_n, length, 3 * cols), bf16),
            jax.ShapeDtypeStruct((share, ctx_n, length, cols), bf16),
            jax.ShapeDtypeStruct((share, length, width), f32),
            jax.ShapeDtypeStruct((share, slots_n, length), f32),
            jax.ShapeDtypeStruct((share, 8, 128), f32),
            jax.ShapeDtypeStruct((slots_n * 8, width), bf16),
        ),
        in_specs=[hbm, hbm, vm, vm],
        out_specs=(vm,) * 6,
        scratch_shapes=[
            pltpu.VMEM((share, length, width), bf16),
            pltpu.VMEM((share, length, width), bf16),
            pltpu.VMEM((slots_n * 8, width), f32),
            pltpu.SemaphoreType.DMA((2,)),
        ],
        compiler_params=pltpu.CompilerParams(vmem_limit_bytes=60 << 20),
    )(x_all, g_all, full, small)


def backward_kernel(share, x_all, g_all, full, small, qkv, heads, resid, logits, asq, back, low_out, dx, dfull, dsmall, rms, x_s, g_s, acc, dres_s, dn_s, sems):
    c0 = lax.axis_index("context") * share
    ctx_n, width, packed = full.shape
    cols = packed // 4
    per = cols // HEAD_DIM
    slots_n = small.shape[0] - 4
    length = x_s.shape[1]
    ins = [
        pltpu.make_async_copy(x_all.at[pl.ds(c0, share)], x_s, sems.at[0]),
        pltpu.make_async_copy(g_all.at[pl.ds(c0, share)], g_s, sems.at[1]),
    ]
    for cp in ins:
        cp.start()
    acc[...] = jnp.zeros_like(acc)
    dsmall[...] = jnp.zeros_like(dsmall)
    keys, key_scale = router_unit(small[4:, :].astype(f32))
    logit_scale = 1.6 * math.sqrt(width)
    for cp in ins:
        cp.wait()

    def image(i, carry):
        gain1, gain2 = small[0:1, :].astype(f32), small[1:2, :].astype(f32)
        g_low = g_s[i]
        res = resid[i]
        hat2, spread2 = layer_stats(res)
        second = hat2 * gain2 + small[3:4, :].astype(f32)
        tokens = second.astype(bf16)
        row_scale = lax.rsqrt(jnp.sum(second * second, axis=-1, keepdims=True) + norm_eps)
        unit = second * row_scale
        eo = mm(pick_rows(slots_n, i), back[...], TN).astype(bf16)
        ds = mm(pick_rows(slots_n, i + 4), back[...], TN).astype(bf16)
        lg = logits[i]
        disp = soft(lg, 1)
        comb = soft(lg, 0)
        mixture = mm(comb.astype(bf16), eo, TN)
        result = res + mixture
        low_out[i] = result.astype(bf16)
        count = 1.0 / (length * width)
        lane = lax.broadcasted_iota(jnp.int32, rms.shape[1:], 1)
        total = jnp.where(
            lane == 0,
            jnp.sum(result * result),
            jnp.where(lane == 1, asq[i], jnp.sum(mixture * mixture)),
        )
        rms[i] = jnp.sqrt(total * count)
        dcomb = mm(eo, g_low, NT)
        ddisp = mm(ds, tokens, NT)
        dtok = mm(disp.astype(bf16), ds, TN)
        dlg = comb * (dcomb - jnp.sum(comb * dcomb, axis=0, keepdims=True)) + disp * (
            ddisp - jnp.sum(disp * ddisp, axis=1, keepdims=True)
        )
        dunit = logit_scale * mm(dlg, keys, TN, highest)
        dsmall[4 : 4 + slots_n, :] += logit_scale * mm(dlg, unit, NN, highest)
        dsec = dtok + row_scale * (dunit - unit * jnp.sum(unit * dunit, axis=-1, keepdims=True))
        dsmall[1:2, :] += jnp.sum(dsec * hat2, axis=0, keepdims=True)
        dsmall[3:4, :] += jnp.sum(dsec, axis=0, keepdims=True)
        dres = g_low.astype(f32) + norm_back(dsec * gain2, hat2, spread2)
        dres_s[...] = dres
        dattn = dres.astype(bf16)
        dattn_t = dattn.T
        hat, spread = layer_stats(x_s[i].astype(f32))
        normed = (hat * gain1 + small[2:3, :].astype(f32)).astype(bf16)
        normed_t = normed.T
        dn_s[...] = jnp.zeros_like(dn_s)

        def block(cb, carry):
            proj = full[cb, :, 3 * cols :]
            dheads = mm(dattn, proj).astype(bf16)
            acc[cb, :, 3 * cols :] += mm(dattn_t, heads[i, cb])
            qkv_c = qkv[i, cb]
            grads = [[], [], []]
            for h in range(per):
                q, k, v = head_parts(qkv_c, h, per)
                dh = dheads[:, h * HEAD_DIM : (h + 1) * HEAD_DIM]
                p = soft(mm(q, k, NT) * 0.125, 1)
                dp = mm(dh, v, NT)
                dsc = (p * (dp - jnp.sum(p * dp, axis=1, keepdims=True))).astype(bf16)
                grads[0].append((mm(dsc, k) * 0.125).astype(bf16))
                grads[1].append((mm(dsc, q, TN) * 0.125).astype(bf16))
                grads[2].append(mm(p.astype(bf16), dh, TN).astype(bf16))
            dqkv = jnp.concatenate(grads[0] + grads[1] + grads[2], axis=1)
            acc[cb, :, : 3 * cols] += mm(normed_t, dqkv)
            dn_s[...] += mm(dqkv, full[cb, :, : 3 * cols], NT)
            return carry

        lax.fori_loop(0, ctx_n, block, 0)
        dn = dn_s[...]
        dsmall[0:1, :] += jnp.sum(dn * hat, axis=0, keepdims=True)
        dsmall[2:3, :] += jnp.sum(dn, axis=0, keepdims=True)
        dx[i] = (dres_s[...] + norm_back(dn * gain1, hat, spread)).astype(bf16)
        return carry

    lax.fori_loop(0, share, image, 0)
    dkeys = dsmall[4 : 4 + slots_n, :]
    dsmall[4 : 4 + slots_n, :] = key_scale * (dkeys - keys * jnp.sum(keys * dkeys, axis=1, keepdims=True))
    for cb in range(ctx_n):
        dfull[cb] = acc[cb].astype(bf16)


def run_backward(x_all, g_all, full, small, saved, back, share):
    ctx_n, width, packed = full.shape
    length = x_all.shape[1]
    slots_n = small.shape[0] - 4
    vm = pl.BlockSpec(memory_space=pltpu.VMEM)
    hbm = pl.BlockSpec(memory_space=pl.ANY)
    acts = jax.ShapeDtypeStruct((share, length, width), bf16)
    return pl.pallas_call(
        functools.partial(backward_kernel, share),
        out_shape=(
            acts,
            acts,
            jax.ShapeDtypeStruct((ctx_n, width, packed), bf16),
            jax.ShapeDtypeStruct((4 + slots_n + -(4 + slots_n) % 8, width), f32),
            jax.ShapeDtypeStruct((share, 8, 128), f32),
        ),
        in_specs=[hbm, hbm] + [vm] * 8,
        out_specs=(vm,) * 5,
        scratch_shapes=[
            pltpu.VMEM((share, length, width), bf16),
            pltpu.VMEM((share, length, width), bf16),
            pltpu.VMEM((ctx_n, width, packed), f32),
            pltpu.VMEM((length, width), f32),
            pltpu.VMEM((length, width), f32),
            pltpu.SemaphoreType.DMA((2,)),
        ],
        compiler_params=pltpu.CompilerParams(vmem_limit_bytes=60 << 20),
    )(x_all, g_all, full, small, *saved, back)


def remote(src, dst, ssem, rsem, **where):
    return pltpu.make_async_remote_copy(
        src_ref=src,
        dst_ref=dst,
        send_sem=ssem,
        recv_sem=rsem,
        device_id=where,
        device_id_type=pl.DeviceIdType.MESH,
    )


def spot():
    wide_n, ctx_n, ten_n = (lax.axis_size(a) for a in ("wide", "context", "tensor"))
    w, c, t = (lax.axis_index(a) for a in ("wide", "context", "tensor"))
    return wide_n, ctx_n, ten_n // 2, w, c, t // 2, lax.rem(t, 2)


def greet_plane(bar, wide_n, y_n, w, y, k):
    for o in range(1, wide_n * y_n * 2):
        j = lax.rem((w * y_n + y) * 2 + k + o, wide_n * y_n * 2)
        pl.semaphore_signal(
            bar,
            inc=1,
            device_id={"wide": j // (y_n * 2), "tensor": lax.rem(j, y_n * 2)},
            device_id_type=pl.DeviceIdType.MESH,
        )
    return wide_n * y_n * 2 - 1


def near_first(c, ctx_n):
    seq = []
    for j in range(ctx_n):
        cb = 0
        for p in range(ctx_n):
            order = sorted(range(ctx_n), key=lambda q: (abs(q - p), q))
            cb = jnp.where(c == p, order[j], cb)
        seq.append(cb)
    return seq


def gather_kernel(pack, small, full, smalls, csem, crecv, wsem, wrecv, ysem, yrecv, ksem, krecv, ssem, srecv, local):
    wide_n, ctx_n, y_n, w, c, y, k = spot()
    bar = pltpu.get_barrier_semaphore()
    met = greet_plane(bar, wide_n, y_n, w, y, k)

    @pl.when(c > 0)
    def _():
        pl.semaphore_signal(bar, inc=1, device_id={"context": c - 1}, device_id_type=pl.DeviceIdType.MESH)

    @pl.when(c < ctx_n - 1)
    def _():
        pl.semaphore_signal(bar, inc=1, device_id={"context": c + 1}, device_id_type=pl.DeviceIdType.MESH)

    mine = pltpu.make_async_copy(pack, full.at[c, w, y, k], local.at[0])
    mine_small = pltpu.make_async_copy(small, smalls.at[w, y, k], local.at[1])
    mine.start()
    mine_small.start()
    pl.semaphore_wait(bar, met + (c + ctx_n - 1) // ctx_n + (2 * ctx_n - 2 - c) // ctx_n)

    def along(cb, side, src):
        return remote(src, full.at[cb, w, y, k], csem.at[side, cb], crecv.at[cb], context=c + 2 * side - 1)

    for side in (0, 1):

        @pl.when((c > 0) if side == 0 else (c < ctx_n - 1))
        def _():
            along(c, side, pack).start()

    def small_copy(o):
        j = lax.rem((w * y_n + y) * 2 + k + o, wide_n * y_n * 2)
        return remote(
            small, smalls.at[w, y, k], ssem.at[o], srecv.at[o], wide=j // (y_n * 2), tensor=lax.rem(j, y_n * 2)
        )

    for o in range(1, wide_n * y_n * 2):
        small_copy(o).start()

    seq = near_first(c, ctx_n)

    def leg(cb, number, o, start):
        even = lax.rem(cb, 2) == 0
        for on_wide in (True, False):
            n = wide_n if on_wide else y_n
            if o >= n:
                continue
            first = number == 0
            want_even = on_wide == first

            @pl.when(even if want_even else jnp.logical_not(even))
            def _():
                if on_wide:
                    ref = full.at[cb, w, y, k] if first else full.at[cb, w, :, k]
                    to = {"wide": lax.rem(w + o, wide_n)}
                    sems = (wsem.at[cb, o], wrecv.at[cb, o])
                else:
                    ref = full.at[cb, w, y, k] if first else full.at[cb, :, y, k]
                    to = {"tensor": lax.rem(y + o, y_n) * 2 + k}
                    sems = (ysem.at[cb, o], yrecv.at[cb, o])
                cp = remote(ref, ref, *sems, **to)
                if start == "start":
                    cp.start()
                elif start == "recv":
                    cp.wait_recv()
                else:
                    cp.wait_send()

    most = max(wide_n, y_n)

    def core(cb):
        ref = full.at[cb, :, :, k]
        return remote(ref, ref, ksem.at[cb], krecv.at[cb], tensor=y * 2 + 1 - k)

    mine.wait()
    mine_small.wait()
    for step in range(ctx_n + 2):
        if step < ctx_n:
            cb = seq[step]
            if step > 0:
                along(cb, 0, pack).wait_recv()
                for side in (0, 1):
                    go = jnp.logical_and(cb > c, c > 0) if side == 0 else jnp.logical_and(cb < c, c < ctx_n - 1)

                    @pl.when(go)
                    def _():
                        along(cb, side, full.at[cb, w, y, k]).start()

            for o in range(1, most):
                leg(cb, 0, o, "start")
        if 0 < step <= ctx_n:
            cb = seq[step - 1]
            for o in range(1, most):
                leg(cb, 0, o, "recv")
            for o in range(1, most):
                leg(cb, 1, o, "start")
        if step > 1:
            cb = seq[step - 2]
            for o in range(1, most):
                leg(cb, 1, o, "recv")
            core(cb).start()
    for step in range(ctx_n):
        core(seq[step]).wait_recv()
    for o in range(1, wide_n * y_n * 2):
        cp = small_copy(o)
        cp.wait_recv()
        cp.wait_send()
    for step in range(ctx_n):
        cb = seq[step]
        for side in (0, 1):
            go = jnp.logical_and(cb >= c, c > 0) if side == 0 else jnp.logical_and(cb <= c, c < ctx_n - 1)

            @pl.when(go)
            def _():
                along(cb, side, pack).wait_send()

        for number in (0, 1):
            for o in range(1, most):
                leg(cb, number, o, "send")
        core(cb).wait_send()


def gather_weights(pack, small):
    wide_n, ctx_n, ten_n = (lax.axis_size(a) for a in ("wide", "context", "tensor"))
    y_n = ten_n // 2
    dma = pltpu.SemaphoreType.DMA
    vm = pl.BlockSpec(memory_space=pltpu.VMEM)
    return pl.pallas_call(
        gather_kernel,
        out_shape=(
            jax.ShapeDtypeStruct((ctx_n, wide_n, y_n, 2) + pack.shape, pack.dtype),
            jax.ShapeDtypeStruct((wide_n, y_n, 2) + small.shape, small.dtype),
        ),
        in_specs=[vm, vm],
        out_specs=(vm, vm),
        scratch_shapes=[
            dma((2, ctx_n)), dma((ctx_n,)),
            dma((ctx_n, wide_n)), dma((ctx_n, wide_n)),
            dma((ctx_n, y_n)), dma((ctx_n, y_n)),
            dma((ctx_n,)), dma((ctx_n,)),
            dma((wide_n * ten_n,)), dma((wide_n * ten_n,)),
            dma((2,)),
        ],
        compiler_params=pltpu.CompilerParams(collective_id=1, has_side_effects=True),
    )(pack, small)


def gelu_parts(x):
    a = 0.7978845608028654
    x2 = x * x
    th = jnp.tanh(a * x * (1.0 + 0.044715 * x2))
    val = 0.5 * x * (1.0 + th)
    der = 0.5 * (1.0 + th) + 0.5 * x * (1.0 - th * th) * (a * (1.0 + 3 * 0.044715 * x2))
    return val, der


def expert_kernel(share, out, up, down, back, up_grad, down_grad, got, r32, ret, got2, sems):
    wide_n, ctx_n, y_n, w, c, y, k = spot()
    ten_n = y_n * 2
    n = wide_n * ctx_n * ten_n
    me = (w * ctx_n + c) * ten_n + y * 2 + k
    bar = pltpu.get_barrier_semaphore()

    def place(d):
        return {"wide": d // (ctx_n * ten_n), "context": lax.rem(d // ten_n, ctx_n), "tensor": lax.rem(d, ten_n)}

    def hello(o, _):
        pl.semaphore_signal(bar, inc=1, device_id=place(lax.rem(me + o, n)), device_id_type=pl.DeviceIdType.MESH)
        return _

    lax.fori_loop(1, n, hello, 0)
    got[me] = out[w * ctx_n + c]
    pl.semaphore_wait(bar, n - 1)

    def send_out(o, _):
        d = lax.rem(me + o, n)
        remote(out.at[d // ten_n], got.at[me], sems.at[0], sems.at[1], **place(d)).start()
        return _

    lax.fori_loop(1, n, send_out, 0)

    def drain(ref, sem):
        part = ref.at[pl.ds(0, n - 1)]
        pltpu.make_async_copy(part, part, sem).wait()

    drain(got, sems.at[1])

    def widen(i, _):
        r32[pl.ds(pl.multiple_of(i * 8, 8), 8), :] = got[i].astype(f32)
        return _

    lax.fori_loop(0, n, widen, 0)
    rows = n * 8
    low = r32[...].astype(bf16)
    first = lax.rem(lax.broadcasted_iota(jnp.int32, (rows, 1), 0), 8) < 4
    hidden = jnp.dot(low, up[...], preferred_element_type=f32)
    act_g = lax.dot_general(low, down[...], (((1,), (1,)), ((), ())), preferred_element_type=f32)
    act_g = pltpu.roll(act_g, rows - 4, 0)
    val, der = gelu_parts(hidden)
    active = jnp.where(first, val, 0.0).astype(bf16)
    hid_g = jnp.where(first, act_g * der, 0.0).astype(bf16)
    part_o = jnp.dot(active, down[...], preferred_element_type=f32)
    part_s = lax.dot_general(hid_g, up[...], (((1,), (1,)), ((), ())), preferred_element_type=f32)
    dexp = pltpu.roll(r32[...], rows - 4, 0).astype(bf16)
    r32[...] = jnp.where(first, part_o, pltpu.roll(part_s, 4, 0))

    def narrow(i, _):
        ret[i] = r32[pl.ds(pl.multiple_of(i * 8, 8), 8), :].astype(bf16)
        return _

    lax.fori_loop(0, n, narrow, 0)

    def send_back(o, _):
        d = lax.rem(me + o, n)
        remote(ret.at[d], got2.at[me], sems.at[2], sems.at[3], **place(d)).start()
        return _

    lax.fori_loop(1, n, send_back, 0)
    got2[me] = ret[me]
    tn = (((0,), (0,)), ((), ()))
    up_grad[...] = lax.dot_general(low, hid_g, tn, preferred_element_type=f32)
    down_grad[...] = lax.dot_general(active, dexp, tn, preferred_element_type=f32)
    drain(got2, sems.at[3])

    def total(e, _):
        s = got2[e * ten_n].astype(f32)
        for t in range(1, ten_n):
            s = s + got2[e * ten_n + t].astype(f32)
        back[e] = s.astype(bf16)
        return _

    lax.fori_loop(0, wide_n * ctx_n, total, 0)
    drain(ret, sems.at[2])

    def sent(o, _):
        pltpu.make_async_copy(out.at[0], out.at[0], sems.at[0]).wait()
        return _

    lax.fori_loop(1, n, sent, 0)


def run_experts(out, up, down, share):
    wide_n, ctx_n, ten_n = (lax.axis_size(a) for a in ("wide", "context", "tensor"))
    n = wide_n * ctx_n * ten_n
    width, ff = up.shape
    vm = pl.BlockSpec(memory_space=pltpu.VMEM)
    return pl.pallas_call(
        functools.partial(expert_kernel, share),
        out_shape=(
            jax.ShapeDtypeStruct(out.shape, bf16),
            jax.ShapeDtypeStruct((width, ff), f32),
            jax.ShapeDtypeStruct((ff, width), f32),
        ),
        in_specs=[vm, vm, vm],
        out_specs=(vm, vm, vm),
        scratch_shapes=[
            pltpu.VMEM((n, 8, width), bf16),
            pltpu.VMEM((n * 8, width), f32),
            pltpu.VMEM((n, 8, width), bf16),
            pltpu.VMEM((n, 8, width), bf16),
            pltpu.SemaphoreType.DMA((4,)),
        ],
        compiler_params=pltpu.CompilerParams(collective_id=2, has_side_effects=True),
    )(out, up, down)


def tail_kernel(n_arr, share, *refs):
    arrs = refs[:n_arr]
    part, small = refs[n_arr : n_arr + 2]
    outs = refs[n_arr + 2 : 2 * n_arr + 2]
    grad, smalls = refs[2 * n_arr + 2 : 2 * n_arr + 4]
    (rcv1, acc1, rcv2, acc2, rcv3, acc3, rcv4, srcv, gsem, grecv, lsem, ksem, krecv, s2, r2, s3, r3, s4, r4, ss, sr) = refs[2 * n_arr + 4 :]
    wide_n, ctx_n, y_n, w, c, y, k = spot()
    ten_n = 2 * y_n
    plane = wide_n * ten_n
    bar = pltpu.get_barrier_semaphore()
    met = greet_plane(bar, wide_n, y_n, w, y, k)
    for o in range(1, ctx_n):
        pl.semaphore_signal(bar, inc=1, device_id={"context": lax.rem(c + o, ctx_n)}, device_id_type=pl.DeviceIdType.MESH)
    own = []
    for a in range(n_arr):
        cp = pltpu.make_async_copy(arrs[a], outs[a].at[pl.ds(c * share, share)], lsem.at[a])
        cp.start()
        own.append(cp)
    pl.semaphore_wait(bar, met + ctx_n - 1)

    def along(a, cb, i, side, src=None):
        ref = outs[a].at[cb * share + i]
        return remote(ref if src is None else src, ref, gsem.at[a, side, cb, i], grecv.at[a, cb, i], context=c + 2 * side - 1)

    for a in range(n_arr):
        for i in range(share):
            for side in (0, 1):

                @pl.when((c > 0) if side == 0 else (c < ctx_n - 1))
                def _():
                    along(a, c, i, side, arrs[a].at[i]).start()

    me = (w * y_n + y) * 2 + k

    def small1(o):
        j = lax.rem(me + o, plane)
        return remote(small.at[j], srcv.at[o], ss.at[o], sr.at[o], wide=j // ten_n, tensor=lax.rem(j, ten_n))

    for o in range(1, plane):
        small1(o).start()

    def core(cc):
        return remote(part.at[cc, :, :, 1 - k], rcv1.at[cc], ksem.at[cc], krecv.at[cc], tensor=y * 2 + 1 - k)

    for cc in range(ctx_n):
        core(cc).start()

    def hop(cc, number, o):
        on_wide = (cc % 2 == 0) == (number == 2)
        src = acc1 if number == 2 else acc2
        dst = rcv2 if number == 2 else rcv3
        ss_, rr_ = (s2, r2) if number == 2 else (s3, r3)
        if on_wide:
            p = lax.rem(w + o, wide_n)
            to = {"wide": p}
            if number == 2:
                frm = src.at[cc, p]
                into = dst.at[cc, o, pl.ds(0, y_n)]
            else:
                frm = src.at[cc, p]
                into = dst.at[cc, o]
        else:
            p = lax.rem(y + o, y_n)
            to = {"tensor": p * 2 + k}
            if number == 2:
                frm = src.at[cc, :, p]
                into = dst.at[cc, o, pl.ds(0, wide_n)]
            else:
                frm = src.at[cc, p]
                into = dst.at[cc, o]
        return remote(frm, into, ss_.at[cc, o], rr_.at[cc, o], **to)

    def peers(cc, number):
        on_wide = (cc % 2 == 0) == (number == 2)
        return range(1, wide_n if on_wide else y_n)

    for cc in range(ctx_n):
        core(cc).wait_recv()
        for wi in range(wide_n):
            for yi in range(y_n):
                acc1[cc, wi, yi] = (part[cc, wi, yi, k].astype(f32) + rcv1[cc, wi, yi].astype(f32)).astype(bf16)
        for o in peers(cc, 2):
            hop(cc, 2, o).start()

    acc = small[me]
    for o in range(1, plane):
        small1(o).wait_recv()
        acc = acc + srcv[o]
    smalls[c] = acc

    def small2(o):
        return remote(smalls.at[c], smalls.at[c], ss.at[plane + o], sr.at[plane + o], context=lax.rem(c + o, ctx_n))

    def small2_in(o):
        ref = smalls.at[lax.rem(c + ctx_n - o, ctx_n)]
        return remote(ref, ref, ss.at[plane + o], sr.at[plane + o], context=lax.rem(c + o, ctx_n))

    for o in range(1, ctx_n):
        small2(o).start()

    def forward(step):
        cb = near_first(c, ctx_n)[step]
        for a in range(n_arr):
            for i in range(share):
                along(a, cb, i, 0).wait_recv()
                for side in (0, 1):
                    go = jnp.logical_and(cb > c, c > 0) if side == 0 else jnp.logical_and(cb < c, c < ctx_n - 1)

                    @pl.when(go)
                    def _():
                        along(a, cb, i, side).start()

    if ctx_n > 1:
        forward(1)
    for cc in range(ctx_n):
        on_wide = cc % 2 == 0
        for o in peers(cc, 2):
            hop(cc, 2, o).wait_recv()
        for j in range(y_n if on_wide else wide_n):
            tot = (acc1[cc, w, j] if on_wide else acc1[cc, j, y]).astype(f32)
            for o in peers(cc, 2):
                tot = tot + rcv2[cc, o, j].astype(f32)
            acc2[cc, j] = tot.astype(bf16)
        for o in peers(cc, 3):
            hop(cc, 3, o).start()
    if ctx_n > 2:
        forward(2)

    def last(cc):
        return remote(acc3.at[cc], rcv4.at[c], s4.at[cc], r4.at[c], context=cc)

    for cc in range(ctx_n):
        for o in peers(cc, 3):
            hop(cc, 3, o).wait_recv()
        tot = (acc2[cc, y] if cc % 2 == 0 else acc2[cc, w]).astype(f32)
        for o in peers(cc, 3):
            tot = tot + rcv3[cc, o].astype(f32)
        acc3[cc] = tot.astype(bf16)

        @pl.when(c != cc)
        def _():
            last(cc).start()

    for step in range(3, ctx_n):
        forward(step)
    tot = acc3[c].astype(f32)
    for o in range(1, ctx_n):
        p = lax.rem(c + o, ctx_n)
        remote(acc3.at[0], rcv4.at[p], s4.at[p], r4.at[p], context=p).wait_recv()
        tot = tot + rcv4[p].astype(f32)
    grad[...] = tot
    for o in range(1, ctx_n):
        small2_in(o).wait_recv()
        small2(o).wait_send()
        p = lax.rem(c + o, ctx_n)
        last(p).wait_send()
    for o in range(1, plane):
        small1(o).wait_send()
    for cc in range(ctx_n):
        core(cc).wait_send()
        for number in (2, 3):
            for o in peers(cc, number):
                hop(cc, number, o).wait_send()
    for a in range(n_arr):
        own[a].wait()
        for cb in range(ctx_n):
            for i in range(share):
                for side in (0, 1):
                    go = jnp.logical_and(c <= cb, c > 0) if side == 0 else jnp.logical_and(c >= cb, c < ctx_n - 1)

                    @pl.when(go)
                    def _():
                        along(a, cb, i, side).wait_send()


def finish(arrs, part, small, share):
    wide_n, ctx_n, ten_n = (lax.axis_size(a) for a in ("wide", "context", "tensor"))
    y_n = ten_n // 2
    most = max(wide_n, y_n)
    blk = part.shape[-2:]
    dma = pltpu.SemaphoreType.DMA
    vm = pl.BlockSpec(memory_space=pltpu.VMEM)
    hbm = pl.BlockSpec(memory_space=pl.ANY)
    n_arr = len(arrs)
    return pl.pallas_call(
        functools.partial(tail_kernel, n_arr, share),
        out_shape=tuple(
            jax.ShapeDtypeStruct((a.shape[0] * ctx_n,) + a.shape[1:], a.dtype) for a in arrs
        )
        + (
            jax.ShapeDtypeStruct(blk, f32),
            jax.ShapeDtypeStruct((ctx_n,) + small.shape[1:], f32),
        ),
        in_specs=[vm] * n_arr + [vm, vm],
        out_specs=(hbm,) * n_arr + (vm, vm),
        scratch_shapes=[
            pltpu.VMEM((ctx_n, wide_n, y_n) + blk, bf16),
            pltpu.VMEM((ctx_n, wide_n, y_n) + blk, bf16),
            pltpu.VMEM((ctx_n, most, most) + blk, bf16),
            pltpu.VMEM((ctx_n, most) + blk, bf16),
            pltpu.VMEM((ctx_n, most) + blk, bf16),
            pltpu.VMEM((ctx_n,) + blk, bf16),
            pltpu.VMEM((ctx_n,) + blk, bf16),
            pltpu.VMEM((wide_n * ten_n,) + small.shape[1:], f32),
            dma((n_arr, 2, ctx_n, share)), dma((n_arr, ctx_n, share)), dma((n_arr,)),
            dma((ctx_n,)), dma((ctx_n,)),
            dma((ctx_n, most)), dma((ctx_n, most)),
            dma((ctx_n, most)), dma((ctx_n, most)),
            dma((ctx_n,)), dma((ctx_n,)),
            dma((wide_n * ten_n + ctx_n,)), dma((wide_n * ten_n + ctx_n,)),
        ],
        compiler_params=pltpu.CompilerParams(collective_id=3, has_side_effects=True),
    )(*arrs, part, small)


def on_device(
    layer_input,
    qkv_weight,
    proj_weight,
    norm_gains,
    norm_biases,
    router_keys,
    up_weight,
    down_weight,
    out_cotangent,
):
    images, length, width = layer_input.shape
    wide_n, ctx_n, ten_n = (lax.axis_size(a) for a in ("wide", "context", "tensor"))
    share = images // ctx_n
    slots_n = router_keys.shape[1]
    rows, _, cols = qkv_weight.shape
    plane = wide_n * ten_n
    lanes = rows + -rows % 128

    pack = jnp.concatenate([qkv_weight.reshape(rows, 3 * cols), proj_weight.T], axis=1)
    small = jnp.concatenate([norm_gains, norm_biases, router_keys.T], axis=0)
    params = small.shape[0]
    small = jnp.pad(small, ((0, -params % 16), (0, lanes - rows)))
    weights, small = gather_weights(pack, small)
    weights = weights.reshape(ctx_n, width, 4 * cols)
    small = small.reshape((-1,) + small.shape[3:])[:, :params, :rows]
    small = small.transpose(1, 0, 2).reshape(params, width)
    *saved, send = run_forward(layer_input, out_cotangent, weights, small, share)
    back, up_grad, down_grad = run_experts(
        send.reshape(slots_n, 8, width), up_weight[0], down_weight[0], share
    )
    back = back.reshape(slots_n * 8, width)
    low, dx, dpack, dsmall, rms = run_backward(
        layer_input, out_cotangent, weights, small, saved, back, share
    )
    dpack = dpack.reshape(ctx_n, wide_n, ten_n // 2, 2, rows, 4 * cols)
    mark = dsmall.shape[0]
    dsmall = dsmall.reshape(mark, plane, rows).transpose(1, 0, 2)
    rms = jnp.broadcast_to(rms[:, 0, :3].reshape(1, 1, share * 3), (plane, 8, share * 3))
    me = lax.axis_index("wide") * ten_n + lax.axis_index("tensor")
    rms = jnp.where(lax.broadcasted_iota(jnp.int32, rms.shape, 0) == me, rms, 0.0)
    dsmall = jnp.concatenate(
        [
            jnp.pad(dsmall, ((0, 0), (0, 0), (0, lanes - rows))),
            jnp.pad(rms, ((0, 0), (0, 0), (0, lanes - share * 3))),
        ],
        axis=1,
    )
    layer_output, input_grad, dpack, dsmall = finish([low, dx], dpack, dsmall, share)
    rms = dsmall[:, mark, : share * 3].reshape(images, 3)
    dsmall = jnp.sum(dsmall[:, :params, :rows], axis=0)
    return (
        layer_output,
        rms,
        input_grad,
        dpack[:, : 3 * cols].reshape(rows, 3, cols),
        dpack[:, 3 * cols :].T,
        dsmall[0:2],
        dsmall[2:4],
        dsmall[4:].T,
        up_grad[None],
        down_grad[None],
    )


def solution(mesh):
    images = P(("wide", "tensor"), None, None)
    qkv = P(("wide", "tensor"), None, "context")
    proj = P("context", ("wide", "tensor"))
    lane = P(None, ("wide", "tensor"))
    rowed = P(("wide", "tensor"), None)
    up = P(("wide", "context"), None, "tensor")
    down = P(("wide", "context"), "tensor", None)
    return jax.shard_map(
        on_device,
        mesh=mesh,
        in_specs=(images, qkv, proj, lane, lane, rowed, up, down, images),
        out_specs=(images, rowed, images, qkv, proj, lane, lane, rowed, up, down),
        check_vma=False,
    )
```

```python
import functools
import math

import jax
import jax.numpy as jnp
from jax import lax
from jax.experimental import pallas as pl
from jax.experimental.pallas import tpu as pltpu
from jax.sharding import PartitionSpec as P

f32 = jnp.float32
bf16 = jnp.bfloat16

HEAD_DIM = 64
norm_eps = 1e-06
highest = lax.Precision.HIGHEST
NN = (((1,), (0,)), ((), ()))
NT = (((1,), (1,)), ((), ()))
TN = (((0,), (0,)), ((), ()))


def mm(a, b, dims=NN, precision=None):
    return lax.dot_general(a, b, dims, precision=precision, preferred_element_type=f32)


def layer_stats(values):
    center = values - jnp.mean(values, axis=-1, keepdims=True)
    spread = lax.rsqrt(jnp.mean(center * center, axis=-1, keepdims=True) + norm_eps)
    return (center * spread, spread)


def norm_back(upstream, scaled, spread):
    return spread * (
        upstream
        - jnp.mean(upstream, axis=-1, keepdims=True)
        - scaled * jnp.mean(upstream * scaled, axis=-1, keepdims=True)
    )


def soft(values, axis):
    e = jnp.exp(values - jnp.max(values, axis=axis, keepdims=True))
    return e / jnp.sum(e, axis=axis, keepdims=True)


def pick_rows(slots_n, row):
    r = lax.broadcasted_iota(jnp.int32, (slots_n * 8, slots_n), 0)
    s = lax.broadcasted_iota(jnp.int32, (slots_n * 8, slots_n), 1)
    return jnp.where(r == s * 8 + row, 1.0, 0.0).astype(bf16)


def router_unit(keys):
    scale = lax.rsqrt(jnp.sum(keys * keys, axis=1, keepdims=True) + norm_eps)
    return keys * scale, scale


def head_parts(block, h, per):
    at = [j * per * HEAD_DIM + h * HEAD_DIM for j in range(3)]
    return [block[:, a : a + HEAD_DIM] for a in at]


def remote(src, dst, ssem, rsem, **where):
    return pltpu.make_async_remote_copy(
        src_ref=src,
        dst_ref=dst,
        send_sem=ssem,
        recv_sem=rsem,
        device_id=where,
        device_id_type=pl.DeviceIdType.MESH,
    )


def spot():
    wide_n, ctx_n, ten_n = (lax.axis_size(a) for a in ("wide", "context", "tensor"))
    w, c, t = (lax.axis_index(a) for a in ("wide", "context", "tensor"))
    return wide_n, ctx_n, ten_n // 2, w, c, t // 2, lax.rem(t, 2)


def greet_plane(bar, wide_n, y_n, w, y, k):
    for o in range(1, wide_n * y_n * 2):
        j = lax.rem((w * y_n + y) * 2 + k + o, wide_n * y_n * 2)
        pl.semaphore_signal(
            bar,
            inc=1,
            device_id={"wide": j // (y_n * 2), "tensor": lax.rem(j, y_n * 2)},
            device_id_type=pl.DeviceIdType.MESH,
        )
    return wide_n * y_n * 2 - 1


def near_first(c, ctx_n):
    seq = []
    for j in range(ctx_n):
        cb = 0
        for p in range(ctx_n):
            order = sorted(range(ctx_n), key=lambda q: (abs(q - p), q))
            cb = jnp.where(c == p, order[j], cb)
        seq.append(cb)
    return seq


def gather_kernel(pack, small, full, smalls, csem, crecv, wsem, wrecv, ysem, yrecv, ksem, krecv, ssem, srecv, local):
    wide_n, ctx_n, y_n, w, c, y, k = spot()
    bar = pltpu.get_barrier_semaphore()
    met = greet_plane(bar, wide_n, y_n, w, y, k)

    @pl.when(c > 0)
    def _():
        pl.semaphore_signal(bar, inc=1, device_id={"context": c - 1}, device_id_type=pl.DeviceIdType.MESH)

    @pl.when(c < ctx_n - 1)
    def _():
        pl.semaphore_signal(bar, inc=1, device_id={"context": c + 1}, device_id_type=pl.DeviceIdType.MESH)

    mine = pltpu.make_async_copy(pack, full.at[c, w, y, k], local.at[0])
    mine_small = pltpu.make_async_copy(small, smalls.at[w, y, k], local.at[1])
    mine.start()
    mine_small.start()
    pl.semaphore_wait(bar, met + (c + ctx_n - 1) // ctx_n + (2 * ctx_n - 2 - c) // ctx_n)

    def along(cb, side, src):
        return remote(src, full.at[cb, w, y, k], csem.at[side, cb], crecv.at[cb], context=c + 2 * side - 1)

    for side in (0, 1):

        @pl.when((c > 0) if side == 0 else (c < ctx_n - 1))
        def _():
            along(c, side, pack).start()

    def small_copy(o):
        j = lax.rem((w * y_n + y) * 2 + k + o, wide_n * y_n * 2)
        return remote(
            small, smalls.at[w, y, k], ssem.at[o], srecv.at[o], wide=j // (y_n * 2), tensor=lax.rem(j, y_n * 2)
        )

    for o in range(1, wide_n * y_n * 2):
        small_copy(o).start()

    seq = near_first(c, ctx_n)

    def leg(cb, number, o, start):
        even = lax.rem(cb, 2) == 0
        for on_wide in (True, False):
            n = wide_n if on_wide else y_n
            if o >= n:
                continue
            first = number == 0
            want_even = on_wide == first

            @pl.when(even if want_even else jnp.logical_not(even))
            def _():
                if on_wide:
                    ref = full.at[cb, w, y, k] if first else full.at[cb, w, :, k]
                    to = {"wide": lax.rem(w + o, wide_n)}
                    sems = (wsem.at[cb, o], wrecv.at[cb, o])
                else:
                    ref = full.at[cb, w, y, k] if first else full.at[cb, :, y, k]
                    to = {"tensor": lax.rem(y + o, y_n) * 2 + k}
                    sems = (ysem.at[cb, o], yrecv.at[cb, o])
                cp = remote(ref, ref, *sems, **to)
                if start == "start":
                    cp.start()
                elif start == "recv":
                    cp.wait_recv()
                else:
                    cp.wait_send()

    most = max(wide_n, y_n)

    def core(cb):
        ref = full.at[cb, :, :, k]
        return remote(ref, ref, ksem.at[cb], krecv.at[cb], tensor=y * 2 + 1 - k)

    mine.wait()
    mine_small.wait()
    for step in range(ctx_n + 2):
        if step < ctx_n:
            cb = seq[step]
            if step > 0:
                along(cb, 0, pack).wait_recv()
                for side in (0, 1):
                    go = jnp.logical_and(cb > c, c > 0) if side == 0 else jnp.logical_and(cb < c, c < ctx_n - 1)

                    @pl.when(go)
                    def _():
                        along(cb, side, full.at[cb, w, y, k]).start()

            for o in range(1, most):
                leg(cb, 0, o, "start")
        if 0 < step <= ctx_n:
            cb = seq[step - 1]
            for o in range(1, most):
                leg(cb, 0, o, "recv")
            for o in range(1, most):
                leg(cb, 1, o, "start")
        if step > 1:
            cb = seq[step - 2]
            for o in range(1, most):
                leg(cb, 1, o, "recv")
            core(cb).start()
    for step in range(ctx_n):
        core(seq[step]).wait_recv()
    for o in range(1, wide_n * y_n * 2):
        cp = small_copy(o)
        cp.wait_recv()
        cp.wait_send()
    for step in range(ctx_n):
        cb = seq[step]
        for side in (0, 1):
            go = jnp.logical_and(cb >= c, c > 0) if side == 0 else jnp.logical_and(cb <= c, c < ctx_n - 1)

            @pl.when(go)
            def _():
                along(cb, side, pack).wait_send()

        for number in (0, 1):
            for o in range(1, most):
                leg(cb, number, o, "send")
        core(cb).wait_send()


def gather_weights(pack, small):
    wide_n, ctx_n, ten_n = (lax.axis_size(a) for a in ("wide", "context", "tensor"))
    y_n = ten_n // 2
    dma = pltpu.SemaphoreType.DMA
    vm = pl.BlockSpec(memory_space=pltpu.VMEM)
    return pl.pallas_call(
        gather_kernel,
        out_shape=(
            jax.ShapeDtypeStruct((ctx_n, wide_n, y_n, 2) + pack.shape, pack.dtype),
            jax.ShapeDtypeStruct((wide_n, y_n, 2) + small.shape, small.dtype),
        ),
        in_specs=[vm, vm],
        out_specs=(vm, vm),
        scratch_shapes=[
            dma((2, ctx_n)), dma((ctx_n,)),
            dma((ctx_n, wide_n)), dma((ctx_n, wide_n)),
            dma((ctx_n, y_n)), dma((ctx_n, y_n)),
            dma((ctx_n,)), dma((ctx_n,)),
            dma((wide_n * ten_n,)), dma((wide_n * ten_n,)),
            dma((2,)),
        ],
        compiler_params=pltpu.CompilerParams(collective_id=1, has_side_effects=True),
    )(pack, small)


def gelu_parts(x):
    a = 0.7978845608028654
    x2 = x * x
    th = jnp.tanh(a * x * (1.0 + 0.044715 * x2))
    val = 0.5 * x * (1.0 + th)
    der = 0.5 * (1.0 + th) + 0.5 * x * (1.0 - th * th) * (a * (1.0 + 3 * 0.044715 * x2))
    return val, der


def block_kernel(share, *refs):
    (
        x_all, g_all, full, small, up, down,
        lo, dxo, grad, smalls, e_in, e_act, e_hid, e_dexp,
        x_s, g_s, att_s, dx_s, nt_s, dt_s, qkv, heads, resid, logits, asq, dres_s, dn_s, rows_s,
        send_s, got, r32, e_s, ret, got2, eo_all, comb_all, dsm, sblk,
        part, rcv1, rcv2, rcv3, acc3, rcv4, srcv, a_buf, x_buf,
        lsem, esem, xsem, gsem, grecv, ksem, krecv, s2, r2, s3, r3, s4, r4, ss, sr, es, er, obuf_sem,
    ) = refs
    wide_n, ctx_n, y_n, w, c, y, k = spot()
    ten_n = 2 * y_n
    plane = wide_n * ten_n
    n = plane * ctx_n
    me = (w * ctx_n + c) * ten_n + y * 2 + k
    mine = (w * y_n + y) * 2 + k
    width, packed = full.shape[1:]
    cols = packed // 4
    per = cols // HEAD_DIM
    slots_n = small.shape[0] - 4
    length = x_s.shape[1]
    rows = grad.shape[0]
    logit_scale = 1.6 * math.sqrt(width)
    seq = near_first(c, ctx_n)
    bar = pltpu.get_barrier_semaphore()

    def place(d):
        return {"wide": d // (ctx_n * ten_n), "context": lax.rem(d // ten_n, ctx_n), "tensor": lax.rem(d, ten_n)}

    def hello(o, carry):
        pl.semaphore_signal(bar, inc=1, device_id=place(lax.rem(me + o, n)), device_id_type=pl.DeviceIdType.MESH)
        return carry

    lax.fori_loop(1, n, hello, 0)
    ins = [
        pltpu.make_async_copy(x_all.at[pl.ds(c * share, share)], x_s, lsem.at[0]),
        pltpu.make_async_copy(g_all.at[pl.ds(c * share, share)], g_s, lsem.at[1]),
    ]
    for cp in ins:
        cp.start()
    rows_s[...] = jnp.zeros_like(rows_s)
    dsm[...] = jnp.zeros_like(dsm)
    keys, key_scale = router_unit(small[4:, :].astype(f32))

    def along(a, cb, i, side, own):
        ref = (lo, dxo)[a].at[cb * share + i]
        src = (att_s, dx_s)[a].at[i] if own else ref
        return remote(src, ref, gsem.at[a, side, cb, i], grecv.at[a, cb, i], context=c + 2 * side - 1)

    def launch(a, i):
        for side in (0, 1):

            @pl.when((c > 0) if side == 0 else (c < ctx_n - 1))
            def _():
                along(a, c, i, side, True).start()

    def onward(cb, side):
        if side == 0:
            return jnp.logical_and(cb > c, c > 0)
        return jnp.logical_and(cb < c, c < ctx_n - 1)

    def pump(a, todo):
        for step, i in todo:
            cb = seq[step]
            along(a, cb, i, 0, False).wait_recv()
            for side in (0, 1):

                @pl.when(onward(cb, side))
                def _():
                    along(a, cb, i, side, False).start()

    pairs = [(s, i) for s in range(1, ctx_n) for i in range(share)]
    pairs.sort(key=lambda p: (p[0] + p[1], p[1]))
    early, middle, late = pairs[:1], pairs[1:3], pairs[3:5]
    rest = pairs[5:]
    waves = [[p for p in pairs if p[0] + p[1] == d] for d in range(1, ctx_n + share - 1)]
    for cp in ins:
        cp.wait()
    pl.semaphore_wait(bar, n - 1)

    def forward(i, carry):
        x = x_s[i].astype(f32)
        hat, spread = layer_stats(x)
        normed = (hat * small[0:1, :].astype(f32) + small[2:3, :].astype(f32)).astype(bf16)
        nt_s[i] = normed.T
        resid[i] = x

        def block(cb, carry):
            qkv_c = mm(normed, full[cb, :, : 3 * cols]).astype(bf16)
            qkv[i, cb] = qkv_c
            mixed = []
            for h in range(per):
                q, kk, v = head_parts(qkv_c, h, per)
                p = soft(mm(q, kk, NT) * 0.125, 1)
                mixed.append(mm(p.astype(bf16), v).astype(bf16))
            heads_c = jnp.concatenate(mixed, axis=1)
            heads[i, cb] = heads_c
            resid[i] += mm(heads_c, full[cb, :, 3 * cols :], NT)
            return carry

        lax.fori_loop(0, ctx_n, block, 0)
        res = resid[i]
        att = res - x
        att_s[i] = att.astype(bf16)
        asq[i] = jnp.full(asq.shape[1:], jnp.sum(att * att), f32)
        launch(0, i)

        @pl.when(i == 1)
        def _():
            pump(0, early)

        hat2, _ = layer_stats(res)
        second = hat2 * small[1:2, :].astype(f32) + small[3:4, :].astype(f32)
        unit = second * lax.rsqrt(jnp.sum(second * second, axis=-1, keepdims=True) + norm_eps)
        lg = logit_scale * mm(keys, unit, NT, highest)
        logits[i] = lg
        disp = soft(lg, 1).astype(bf16)
        comb = soft(lg, 0).astype(bf16)
        comb_all[c, i, :, :length] = comb
        slots = mm(disp, second.astype(bf16)).astype(bf16)
        dexp = mm(comb, g_s[i]).astype(bf16)
        rows_s[...] += mm(pick_rows(slots_n, i), slots) + mm(pick_rows(slots_n, i + 4), dexp)
        return carry

    lax.fori_loop(0, share, forward, 0)

    for e in range(slots_n):
        send_s[e] = rows_s[e * 8 : e * 8 + 8, :].astype(bf16)
    got[me] = send_s[w * ctx_n + c]

    def send_out(o, carry):
        d = lax.rem(me + o, n)
        remote(send_s.at[d // ten_n], got.at[me], esem.at[0], esem.at[1], **place(d)).start()
        return carry

    lax.fori_loop(1, n, send_out, 0)

    def drain(ref, sem):
        some = ref.at[pl.ds(0, n - 1)]
        pltpu.make_async_copy(some, some, sem).wait()

    pump(0, middle)
    drain(got, esem.at[1])

    group = min(n, 32)
    chunk = group * 8
    first = lax.rem(lax.broadcasted_iota(jnp.int32, (chunk, 1), 0), 8) < 4

    def expert_out(b, j):
        dst = (e_in, e_act, e_hid, e_dexp)[j]
        at = pl.ds(pl.multiple_of(b * chunk, chunk), chunk)
        return pltpu.make_async_copy(e_s.at[j], dst.at[at, :], xsem.at[j])

    def experts(b, carry):
        def widen(j, carry):
            r32[pl.ds(pl.multiple_of(j * 8, 8), 8), :] = got[b * group + j].astype(f32)
            return carry

        lax.fori_loop(0, group, widen, 0)

        @pl.when(b > 0)
        def _():
            for j in range(4):
                expert_out(b, j).wait()

        low = r32[...].astype(bf16)
        e_s[0] = low
        e_s[3] = pltpu.roll(r32[...], chunk - 4, 0).astype(bf16)
        hidden = mm(low, up[...])
        act_g = pltpu.roll(mm(low, down[...], NT), chunk - 4, 0)
        val, der = gelu_parts(hidden)
        active = jnp.where(first, val, 0.0).astype(bf16)
        hid_g = jnp.where(first, act_g * der, 0.0).astype(bf16)
        e_s[1] = active
        e_s[2] = hid_g
        part_o = mm(active, down[...])
        part_s = mm(hid_g, up[...], NT)
        r32[...] = jnp.where(first, part_o, pltpu.roll(part_s, 4, 0))
        for j in range(4):
            expert_out(b, j).start()

        def narrow(j, carry):
            ret[b * group + j] = r32[pl.ds(pl.multiple_of(j * 8, 8), 8), :].astype(bf16)
            return carry

        lax.fori_loop(0, group, narrow, 0)
        return carry

    lax.fori_loop(0, n // group, experts, 0)

    def send_back(o, carry):
        d = lax.rem(me + o, n)
        remote(ret.at[d], got2.at[me], esem.at[2], esem.at[3], **place(d)).start()
        return carry

    lax.fori_loop(1, n, send_back, 0)
    got2[me] = ret[me]
    pump(0, late)
    drain(got2, esem.at[3])

    def total(e, carry):
        s = got2[e * ten_n].astype(f32)
        for t in range(1, ten_n):
            s = s + got2[e * ten_n + t].astype(f32)
        rows_s[pl.ds(pl.multiple_of(e * 8, 8), 8), :] = s
        return carry

    lax.fori_loop(0, slots_n, total, 0)
    back = rows_s[...].astype(bf16)
    for i in range(share):
        eo_all[c, i] = mm(pick_rows(slots_n, i), back, TN).astype(bf16)

    def trade(o, ref, j, p):
        return remote(ref.at[p], ref.at[p], es.at[j, o], er.at[j, o], context=lax.rem(c + o, ctx_n))

    for o in range(1, ctx_n):
        trade(o, eo_all, 0, c).start()
        trade(o, comb_all, 1, c).start()

    def fetch(step, i, slot):
        img = seq[step] * share + i
        return (
            pltpu.make_async_copy(lo.at[img], a_buf.at[slot], obuf_sem.at[0, slot]),
            pltpu.make_async_copy(x_all.at[img], x_buf.at[slot], obuf_sem.at[1, slot]),
        )

    def put(step, i, slot):
        img = seq[step] * share + i
        return pltpu.make_async_copy(a_buf.at[slot], lo.at[img], obuf_sem.at[2, slot])

    def backward(i, carry):
        gain1, gain2 = small[0:1, :].astype(f32), small[1:2, :].astype(f32)
        g_low = g_s[i]
        res = resid[i]
        hat2, spread2 = layer_stats(res)
        second = hat2 * gain2 + small[3:4, :].astype(f32)
        tokens = second.astype(bf16)
        row_scale = lax.rsqrt(jnp.sum(second * second, axis=-1, keepdims=True) + norm_eps)
        unit = second * row_scale
        eo = eo_all[c, i]
        ds = mm(pick_rows(slots_n, i + 4), rows_s[...].astype(bf16), TN).astype(bf16)
        lg = logits[i]
        disp = soft(lg, 1)
        comb = soft(lg, 0)
        mixture = mm(comb.astype(bf16), eo, TN)
        result = res + mixture

        @pl.when(i > 1)
        def _():
            put(0, 0, 0).wait()

        a_buf[lax.rem(i, 2)] = result.astype(bf16)
        put(0, i, lax.rem(i, 2)).start()
        count = 1.0 / (length * width)
        lane = lax.broadcasted_iota(jnp.int32, (8, smalls.shape[2]), 1)
        sums = jnp.where(
            lane == 0,
            jnp.sum(result * result),
            jnp.where(lane == 1, asq[i], jnp.sum(mixture * mixture)),
        )
        at_row = lax.broadcasted_iota(jnp.int32, (8, smalls.shape[2]), 0)
        sblk[plane, :8, :] = jnp.where(at_row == i, jnp.sqrt(sums * count), sblk[plane, :8, :])
        dcomb = mm(eo, g_low, NT)
        ddisp = mm(ds, tokens, NT)
        dtok = mm(disp.astype(bf16), ds, TN)
        dlg = comb * (dcomb - jnp.sum(comb * dcomb, axis=0, keepdims=True)) + disp * (
            ddisp - jnp.sum(disp * ddisp, axis=1, keepdims=True)
        )
        dunit = logit_scale * mm(dlg, keys, TN, highest)
        dsm[4 : 4 + slots_n, :] += logit_scale * mm(dlg, unit, NN, highest)
        dsec = dtok + row_scale * (dunit - unit * jnp.sum(unit * dunit, axis=-1, keepdims=True))
        dsm[1:2, :] += jnp.sum(dsec * hat2, axis=0, keepdims=True)
        dsm[3:4, :] += jnp.sum(dsec, axis=0, keepdims=True)
        dres = g_low.astype(f32) + norm_back(dsec * gain2, hat2, spread2)
        dres_s[...] = dres
        dattn = dres.astype(bf16)
        dt_s[i] = dattn.T
        hat, spread = layer_stats(x_s[i].astype(f32))
        dn_s[...] = jnp.zeros_like(dn_s)

        @pl.when(i == 0)
        def _():
            pump(0, rest)

        def block(cb, carry):
            for j in range(1, share):

                @pl.when(jnp.logical_and(i == j, cb == ctx_n // 2))
                def _():
                    pump(1, waves[j - 1])

            proj = full[cb, :, 3 * cols :]
            dheads = mm(dattn, proj).astype(bf16)
            qkv_c = qkv[i, cb]
            grads = [[], [], []]
            for h in range(per):
                q, kk, v = head_parts(qkv_c, h, per)
                dh = dheads[:, h * HEAD_DIM : (h + 1) * HEAD_DIM]
                p = soft(mm(q, kk, NT) * 0.125, 1)
                dp = mm(dh, v, NT)
                dsc = (p * (dp - jnp.sum(p * dp, axis=1, keepdims=True))).astype(bf16)
                grads[0].append((mm(dsc, kk) * 0.125).astype(bf16))
                grads[1].append((mm(dsc, q, TN) * 0.125).astype(bf16))
                grads[2].append(mm(p.astype(bf16), dh, TN).astype(bf16))
            dqkv = jnp.concatenate(grads[0] + grads[1] + grads[2], axis=1)
            qkv[i, cb] = dqkv
            dn_s[...] += mm(dqkv, full[cb, :, : 3 * cols], NT)
            return carry

        lax.fori_loop(0, ctx_n, block, 0)
        dn = dn_s[...]
        dsm[0:1, :] += jnp.sum(dn * hat, axis=0, keepdims=True)
        dsm[2:3, :] += jnp.sum(dn, axis=0, keepdims=True)
        dx_s[i] = (dres_s[...] + norm_back(dn * gain1, hat, spread)).astype(bf16)
        launch(1, i)
        return carry

    sblk[plane] = jnp.zeros(sblk.shape[1:], f32)
    lax.fori_loop(0, share, backward, 0)
    outs = [pltpu.make_async_copy(dx_s, dxo.at[pl.ds(c * share, share)], lsem.at[1])]
    for cp in outs:
        cp.start()
    dkeys = dsm[4 : 4 + slots_n, :]
    dsm[4 : 4 + slots_n, :] = key_scale * (dkeys - keys * jnp.sum(keys * dkeys, axis=1, keepdims=True))

    def core(cc):
        return remote(part.at[cc, :, :, 1 - k], rcv1.at[cc], ksem.at[cc], krecv.at[cc], tensor=y * 2 + 1 - k)

    for cc in range(ctx_n):
        from_qkv = sum(mm(nt_s[i], qkv[i, cc]) for i in range(share)).astype(bf16)
        from_proj = sum(mm(dt_s[i], heads[i, cc]) for i in range(share)).astype(bf16)
        for j in range(plane):
            at = (cc, j // ten_n, (j // 2) % y_n, j % 2)
            part[at + (slice(None), slice(0, 3 * cols))] = from_qkv[j * rows : (j + 1) * rows]
            part[at + (slice(None), slice(3 * cols, packed))] = from_proj[j * rows : (j + 1) * rows]
        core(cc).start()
        if cc == ctx_n // 2:
            pump(1, waves[2] if len(waves) > 2 else [])
    for j in range(plane):
        sblk[j, :, :rows] = dsm[:, j * rows : (j + 1) * rows]

    def small1(o):
        j = lax.rem(mine + o, plane)
        return remote(sblk.at[j], srcv.at[o], ss.at[o], sr.at[o], wide=j // ten_n, tensor=lax.rem(j, ten_n))

    for o in range(1, plane):
        small1(o).start()

    def hop(cc, number, o):
        on_wide = (cc % 2 == 0) == (number == 2)
        ss_, rr_ = (s2, r2) if number == 2 else (s3, r3)
        if on_wide:
            p = lax.rem(w + o, wide_n)
            to = {"wide": p}
            frm = rcv1.at[cc, p] if number == 2 else rcv1.at[cc, p, y]
            into = rcv2.at[cc, pl.ds(o * y_n, y_n)] if number == 2 else rcv3.at[cc, o]
        else:
            p = lax.rem(y + o, y_n)
            to = {"tensor": p * 2 + k}
            frm = rcv1.at[cc, :, p] if number == 2 else rcv1.at[cc, w, p]
            into = rcv2.at[cc, pl.ds(o * wide_n, wide_n)] if number == 2 else rcv3.at[cc, o]
        return remote(frm, into, ss_.at[cc, o], rr_.at[cc, o], **to)

    def peers(cc, number):
        on_wide = (cc % 2 == 0) == (number == 2)
        return range(1, wide_n if on_wide else y_n)

    for cc in range(ctx_n):
        core(cc).wait_recv()
        for wi in range(wide_n):
            for yi in range(y_n):
                rcv1[cc, wi, yi] = (part[cc, wi, yi, k].astype(f32) + rcv1[cc, wi, yi].astype(f32)).astype(bf16)
        for o in peers(cc, 2):
            hop(cc, 2, o).start()
    pump(1, waves[3] if len(waves) > 3 else [])

    for o in range(1, ctx_n):
        p = lax.rem(c + ctx_n - o, ctx_n)
        trade(o, eo_all, 0, p).wait_recv()
        trade(o, comb_all, 1, p).wait_recv()

    order = [(s, i) for s in range(1, ctx_n) for i in range(share)]

    def mix_some(lo_n, hi_n):
        for j in range(lo_n, hi_n):
            step, i = order[j]
            cb = seq[step]
            slot = (j + share) % 2
            for side in (0, 1):

                @pl.when(onward(cb, side))
                def _():
                    along(0, cb, i, side, False).wait_send()

            put(step, i, slot).wait()
            for cp in fetch(step, i, slot):
                cp.start()
            for cp in fetch(step, i, slot):
                cp.wait()
            mixed = mm(comb_all[cb, i, :, :length], eo_all[cb, i], TN)
            out = x_buf[slot].astype(f32) + a_buf[slot].astype(f32) + mixed
            a_buf[slot] = out.astype(bf16)
            put(step, i, slot).start()

    third = len(order) // 3
    mix_some(0, third)
    for cc in range(ctx_n):
        on_wide = cc % 2 == 0
        for o in peers(cc, 2):
            hop(cc, 2, o).wait_recv()
        for j in range(y_n if on_wide else wide_n):
            spot_j = (cc, w, j) if on_wide else (cc, j, y)
            tot = rcv1[spot_j].astype(f32)
            for o in peers(cc, 2):
                tot = tot + rcv2[cc, o * (y_n if on_wide else wide_n) + j].astype(f32)
            rcv1[spot_j] = tot.astype(bf16)
        for o in peers(cc, 3):
            hop(cc, 3, o).start()

    tot = sblk[mine]
    for o in range(1, plane):
        small1(o).wait_recv()
        tot = tot + srcv[o]
    smalls[c, : sblk.shape[1], :] = tot
    smalls[c, sblk.shape[1] :, :] = sblk[plane, :8, :]

    def small2(o, p):
        return remote(
            smalls.at[p], smalls.at[p], ss.at[plane + o], sr.at[plane + o], context=lax.rem(c + o, ctx_n)
        )

    for o in range(1, ctx_n):
        small2(o, c).start()
    pump(1, waves[4] if len(waves) > 4 else [])
    mix_some(third, 2 * third)

    def last(cc):
        return remote(acc3.at[cc], rcv4.at[c], s4.at[cc], r4.at[c], context=cc)

    for cc in range(ctx_n):
        for o in peers(cc, 3):
            hop(cc, 3, o).wait_recv()
        tot = rcv1[cc, w, y].astype(f32)
        for o in peers(cc, 3):
            tot = tot + rcv3[cc, o].astype(f32)
        acc3[cc] = tot.astype(bf16)

        @pl.when(c != cc)
        def _():
            last(cc).start()

    mix_some(2 * third, len(order))
    for wave in waves[5:]:
        pump(1, wave)
    tot = acc3[c].astype(f32)
    for o in range(1, ctx_n):
        p = lax.rem(c + o, ctx_n)
        remote(acc3.at[0], rcv4.at[p], s4.at[p], r4.at[p], context=p).wait_recv()
        tot = tot + rcv4[p].astype(f32)
    grad[...] = tot

    for slot in (0, 1):
        put(0, 0, slot).wait()
    for j in range(4):
        expert_out(0, j).wait()
    drain(ret, esem.at[2])

    def sent(o, carry):
        pltpu.make_async_copy(send_s.at[0], send_s.at[0], esem.at[0]).wait()
        return carry

    lax.fori_loop(1, n, sent, 0)
    for o in range(1, ctx_n):
        p = lax.rem(c + ctx_n - o, ctx_n)
        small2(o, p).wait_recv()
        small2(o, c).wait_send()
        trade(o, eo_all, 0, c).wait_send()
        trade(o, comb_all, 1, c).wait_send()
        last(lax.rem(c + o, ctx_n)).wait_send()
    for o in range(1, plane):
        small1(o).wait_send()
    for cc in range(ctx_n):
        core(cc).wait_send()
        for number in (2, 3):
            for o in peers(cc, number):
                hop(cc, number, o).wait_send()
    for cp in outs:
        cp.wait()
    for a in (0, 1):
        for i in range(share):
            for side in (0, 1):

                @pl.when((c > 0) if side == 0 else (c < ctx_n - 1))
                def _():
                    along(a, c, i, side, True).wait_send()

    for step, i in order:
        for side in (0, 1):

            @pl.when(onward(seq[step], side))
            def _():
                along(1, seq[step], i, side, False).wait_send()


def run_block(x_all, g_all, full, small, up, down, rows, share):
    wide_n, ctx_n, ten_n = (lax.axis_size(a) for a in ("wide", "context", "tensor"))
    y_n = ten_n // 2
    plane = wide_n * ten_n
    n = plane * ctx_n
    most = max(wide_n, y_n)
    images, length, width = x_all.shape
    packed = full.shape[2]
    cols = packed // 4
    ff = up.shape[1]
    slots_n = small.shape[0] - 4
    par8 = 4 + slots_n + -(4 + slots_n) % 8
    lanes = rows + -rows % 128
    blk = (rows, packed)
    acts = (share, length, width)
    wide_len = length + -length % 128
    dma = pltpu.SemaphoreType.DMA
    vm = pl.BlockSpec(memory_space=pltpu.VMEM)
    hbm = pl.BlockSpec(memory_space=pl.ANY)
    V = pltpu.VMEM
    shape = jax.ShapeDtypeStruct
    return pl.pallas_call(
        functools.partial(block_kernel, share),
        out_shape=(
            shape((images, length, width), bf16),
            shape((images, length, width), bf16),
            shape(blk, f32),
            shape((ctx_n, par8 + 8, lanes), f32),
            shape((n * 8, width), bf16),
            shape((n * 8, ff), bf16),
            shape((n * 8, ff), bf16),
            shape((n * 8, width), bf16),
        ),
        in_specs=[hbm, hbm] + [vm] * 4,
        out_specs=(hbm, hbm, vm, vm) + (hbm,) * 4,
        scratch_shapes=[
            V(acts, bf16), V(acts, bf16), V(acts, bf16), V(acts, bf16),
            V((share, width, length), bf16),
            V((share, width, length), bf16),
            V((share, ctx_n, length, 3 * cols), bf16),
            V((share, ctx_n, length, cols), bf16),
            V(acts, f32),
            V((share, slots_n, length), f32),
            V((share, 8, lanes), f32),
            V((length, width), f32),
            V((length, width), f32),
            V((slots_n * 8, width), f32),
            V((slots_n, 8, width), bf16),
            V((n, 8, width), bf16),
            V((min(n, 32) * 8, width), f32),
            V((4, min(n, 32) * 8, width), bf16),
            V((n, 8, width), bf16),
            V((n, 8, width), bf16),
            V((ctx_n, share, slots_n, width), bf16),
            V((ctx_n, share, slots_n, wide_len), bf16),
            V((par8, width), f32),
            V((plane + 1, par8, lanes), f32),
            V((ctx_n, wide_n, y_n, 2) + blk, bf16),
            V((ctx_n, wide_n, y_n) + blk, bf16),
            V((ctx_n, wide_n * y_n) + blk, bf16),
            V((ctx_n, most) + blk, bf16),
            V((ctx_n,) + blk, bf16),
            V((ctx_n,) + blk, bf16),
            V((plane, par8, lanes), f32),
            V((2, length, width), bf16),
            V((2, length, width), bf16),
            dma((2,)), dma((4,)), dma((4,)),
            dma((2, 2, ctx_n, share)), dma((2, ctx_n, share)),
            dma((ctx_n,)), dma((ctx_n,)),
            dma((ctx_n, most)), dma((ctx_n, most)),
            dma((ctx_n, most)), dma((ctx_n, most)),
            dma((ctx_n,)), dma((ctx_n,)),
            dma((plane + ctx_n,)), dma((plane + ctx_n,)),
            dma((2, ctx_n)), dma((2, ctx_n)),
            dma((3, 2)),
        ],
        compiler_params=pltpu.CompilerParams(
            collective_id=2, has_side_effects=True, vmem_limit_bytes=67043328
        ),
    )(x_all, g_all, full, small, up, down)


def on_device(
    layer_input,
    qkv_weight,
    proj_weight,
    norm_gains,
    norm_biases,
    router_keys,
    up_weight,
    down_weight,
    out_cotangent,
):
    images, length, width = layer_input.shape
    wide_n, ctx_n, ten_n = (lax.axis_size(a) for a in ("wide", "context", "tensor"))
    share = images // ctx_n
    slots_n = router_keys.shape[1]
    rows, _, cols = qkv_weight.shape
    plane = wide_n * ten_n
    lanes = rows + -rows % 128

    pack = jnp.concatenate([qkv_weight.reshape(rows, 3 * cols), proj_weight.T], axis=1)
    small = jnp.concatenate([norm_gains, norm_biases, router_keys.T], axis=0)
    params = small.shape[0]
    small = jnp.pad(small, ((0, -params % 16), (0, lanes - rows)))
    weights, small = gather_weights(pack, small)
    weights = weights.reshape(ctx_n, width, 4 * cols)
    small = small.reshape((-1,) + small.shape[3:])[:, :params, :rows]
    small = small.transpose(1, 0, 2).reshape(params, width)
    layer_output, input_grad, dpack, dsmall, e_in, e_act, e_hid, e_dexp = run_block(
        layer_input, out_cotangent, weights, small, up_weight[0], down_weight[0], rows, share
    )
    up_grad = mm(e_in, e_hid, TN)
    down_grad = mm(e_act, e_dexp, TN)
    rms = dsmall[:, dsmall.shape[1] - 8 :, :3][:, :share].reshape(images, 3)
    dsmall = jnp.sum(dsmall[:, :params, :rows], axis=0)
    return (
        layer_output,
        rms,
        input_grad,
        dpack[:, : 3 * cols].reshape(rows, 3, cols),
        dpack[:, 3 * cols :].T,
        dsmall[0:2],
        dsmall[2:4],
        dsmall[4:].T,
        up_grad[None],
        down_grad[None],
    )


def solution(mesh):
    images = P(("wide", "tensor"), None, None)
    qkv = P(("wide", "tensor"), None, "context")
    proj = P("context", ("wide", "tensor"))
    lane = P(None, ("wide", "tensor"))
    rowed = P(("wide", "tensor"), None)
    up = P(("wide", "context"), None, "tensor")
    down = P(("wide", "context"), "tensor", None)
    return jax.shard_map(
        on_device,
        mesh=mesh,
        in_specs=(images, qkv, proj, lane, lane, rowed, up, down, images),
        out_specs=(images, rowed, images, qkv, proj, lane, lane, rowed, up, down),
        check_vma=False,
    )
```

```python
import functools
import math

import jax
import jax.numpy as jnp
from jax import lax
from jax.experimental import pallas as pl
from jax.experimental.pallas import tpu as pltpu
from jax.sharding import PartitionSpec as P

f32 = jnp.float32
bf16 = jnp.bfloat16

HEAD_DIM = 64
norm_eps = 1e-06
highest = lax.Precision.HIGHEST
NN = (((1,), (0,)), ((), ()))
NT = (((1,), (1,)), ((), ()))
TN = (((0,), (0,)), ((), ()))


def mm(a, b, dims=NN, precision=None):
    return lax.dot_general(a, b, dims, precision=precision, preferred_element_type=f32)


def layer_stats(values):
    center = values - jnp.mean(values, axis=-1, keepdims=True)
    spread = lax.rsqrt(jnp.mean(center * center, axis=-1, keepdims=True) + norm_eps)
    return (center * spread, spread)


def norm_back(upstream, scaled, spread):
    return spread * (
        upstream
        - jnp.mean(upstream, axis=-1, keepdims=True)
        - scaled * jnp.mean(upstream * scaled, axis=-1, keepdims=True)
    )


def soft(values, axis):
    e = jnp.exp(values - jnp.max(values, axis=axis, keepdims=True))
    return e / jnp.sum(e, axis=axis, keepdims=True)


def pick_rows(slots_n, row):
    r = lax.broadcasted_iota(jnp.int32, (slots_n * 8, slots_n), 0)
    s = lax.broadcasted_iota(jnp.int32, (slots_n * 8, slots_n), 1)
    return jnp.where(r == s * 8 + row, 1.0, 0.0).astype(bf16)


def router_unit(keys):
    scale = lax.rsqrt(jnp.sum(keys * keys, axis=1, keepdims=True) + norm_eps)
    return keys * scale, scale


def head_parts(block, h, per):
    at = [j * per * HEAD_DIM + h * HEAD_DIM for j in range(3)]
    return [block[:, a : a + HEAD_DIM] for a in at]


def remote(src, dst, ssem, rsem, **where):
    return pltpu.make_async_remote_copy(
        src_ref=src,
        dst_ref=dst,
        send_sem=ssem,
        recv_sem=rsem,
        device_id=where,
        device_id_type=pl.DeviceIdType.MESH,
    )


def spot():
    wide_n, ctx_n, ten_n = (lax.axis_size(a) for a in ("wide", "context", "tensor"))
    w, c, t = (lax.axis_index(a) for a in ("wide", "context", "tensor"))
    return wide_n, ctx_n, ten_n // 2, w, c, t // 2, lax.rem(t, 2)


def greet_plane(bar, wide_n, y_n, w, y, k):
    for o in range(1, wide_n * y_n * 2):
        j = lax.rem((w * y_n + y) * 2 + k + o, wide_n * y_n * 2)
        pl.semaphore_signal(
            bar,
            inc=1,
            device_id={"wide": j // (y_n * 2), "tensor": lax.rem(j, y_n * 2)},
            device_id_type=pl.DeviceIdType.MESH,
        )
    return wide_n * y_n * 2 - 1


def near_first(c, ctx_n):
    seq = []
    for j in range(ctx_n):
        cb = 0
        for p in range(ctx_n):
            order = sorted(range(ctx_n), key=lambda q: (abs(q - p), q))
            cb = jnp.where(c == p, order[j], cb)
        seq.append(cb)
    return seq


def gather_kernel(pack, small, full, smalls, csem, crecv, wsem, wrecv, ysem, yrecv, ksem, krecv, ssem, srecv, local):
    wide_n, ctx_n, y_n, w, c, y, k = spot()
    bar = pltpu.get_barrier_semaphore()
    met = greet_plane(bar, wide_n, y_n, w, y, k)

    @pl.when(c > 0)
    def _():
        pl.semaphore_signal(bar, inc=1, device_id={"context": c - 1}, device_id_type=pl.DeviceIdType.MESH)

    @pl.when(c < ctx_n - 1)
    def _():
        pl.semaphore_signal(bar, inc=1, device_id={"context": c + 1}, device_id_type=pl.DeviceIdType.MESH)

    mine = pltpu.make_async_copy(pack, full.at[c, w, y, k], local.at[0])
    mine_small = pltpu.make_async_copy(small, smalls.at[w, y, k], local.at[1])
    mine.start()
    mine_small.start()
    pl.semaphore_wait(bar, met + (c + ctx_n - 1) // ctx_n + (2 * ctx_n - 2 - c) // ctx_n)

    def along(cb, side, src):
        return remote(src, full.at[cb, w, y, k], csem.at[side, cb], crecv.at[cb], context=c + 2 * side - 1)

    for side in (0, 1):

        @pl.when((c > 0) if side == 0 else (c < ctx_n - 1))
        def _():
            along(c, side, pack).start()

    def small_copy(o):
        j = lax.rem((w * y_n + y) * 2 + k + o, wide_n * y_n * 2)
        return remote(
            small, smalls.at[w, y, k], ssem.at[o], srecv.at[o], wide=j // (y_n * 2), tensor=lax.rem(j, y_n * 2)
        )

    for o in range(1, wide_n * y_n * 2):
        small_copy(o).start()

    seq = near_first(c, ctx_n)

    def leg(cb, number, o, start):
        even = lax.rem(cb, 2) == 0
        for on_wide in (True, False):
            n = wide_n if on_wide else y_n
            if o >= n:
                continue
            first = number == 0
            want_even = on_wide == first

            @pl.when(even if want_even else jnp.logical_not(even))
            def _():
                if on_wide:
                    ref = full.at[cb, w, y, k] if first else full.at[cb, w, :, k]
                    to = {"wide": lax.rem(w + o, wide_n)}
                    sems = (wsem.at[cb, o], wrecv.at[cb, o])
                else:
                    ref = full.at[cb, w, y, k] if first else full.at[cb, :, y, k]
                    to = {"tensor": lax.rem(y + o, y_n) * 2 + k}
                    sems = (ysem.at[cb, o], yrecv.at[cb, o])
                cp = remote(ref, ref, *sems, **to)
                if start == "start":
                    cp.start()
                elif start == "recv":
                    cp.wait_recv()
                else:
                    cp.wait_send()

    most = max(wide_n, y_n)

    def core(cb):
        ref = full.at[cb, :, :, k]
        return remote(ref, ref, ksem.at[cb], krecv.at[cb], tensor=y * 2 + 1 - k)

    mine.wait()
    mine_small.wait()
    for step in range(ctx_n + 2):
        if step < ctx_n:
            cb = seq[step]
            if step > 0:
                along(cb, 0, pack).wait_recv()
                for side in (0, 1):
                    go = jnp.logical_and(cb > c, c > 0) if side == 0 else jnp.logical_and(cb < c, c < ctx_n - 1)

                    @pl.when(go)
                    def _():
                        along(cb, side, full.at[cb, w, y, k]).start()

            for o in range(1, most):
                leg(cb, 0, o, "start")
        if 0 < step <= ctx_n:
            cb = seq[step - 1]
            for o in range(1, most):
                leg(cb, 0, o, "recv")
            for o in range(1, most):
                leg(cb, 1, o, "start")
        if step > 1:
            cb = seq[step - 2]
            for o in range(1, most):
                leg(cb, 1, o, "recv")
            core(cb).start()
    for step in range(ctx_n):
        core(seq[step]).wait_recv()
    for o in range(1, wide_n * y_n * 2):
        cp = small_copy(o)
        cp.wait_recv()
        cp.wait_send()
    for step in range(ctx_n):
        cb = seq[step]
        for side in (0, 1):
            go = jnp.logical_and(cb >= c, c > 0) if side == 0 else jnp.logical_and(cb <= c, c < ctx_n - 1)

            @pl.when(go)
            def _():
                along(cb, side, pack).wait_send()

        for number in (0, 1):
            for o in range(1, most):
                leg(cb, number, o, "send")
        core(cb).wait_send()


def gather_weights(pack, small):
    wide_n, ctx_n, ten_n = (lax.axis_size(a) for a in ("wide", "context", "tensor"))
    y_n = ten_n // 2
    dma = pltpu.SemaphoreType.DMA
    vm = pl.BlockSpec(memory_space=pltpu.VMEM)
    return pl.pallas_call(
        gather_kernel,
        out_shape=(
            jax.ShapeDtypeStruct((ctx_n, wide_n, y_n, 2) + pack.shape, pack.dtype),
            jax.ShapeDtypeStruct((wide_n, y_n, 2) + small.shape, small.dtype),
        ),
        in_specs=[vm, vm],
        out_specs=(vm, vm),
        scratch_shapes=[
            dma((2, ctx_n)), dma((ctx_n,)),
            dma((ctx_n, wide_n)), dma((ctx_n, wide_n)),
            dma((ctx_n, y_n)), dma((ctx_n, y_n)),
            dma((ctx_n,)), dma((ctx_n,)),
            dma((wide_n * ten_n,)), dma((wide_n * ten_n,)),
            dma((2,)),
        ],
        compiler_params=pltpu.CompilerParams(collective_id=1, has_side_effects=True),
    )(pack, small)


def gelu_parts(x):
    a = 0.7978845608028654
    x2 = x * x
    th = jnp.tanh(a * x * (1.0 + 0.044715 * x2))
    val = 0.5 * x * (1.0 + th)
    der = 0.5 * (1.0 + th) + 0.5 * x * (1.0 - th * th) * (a * (1.0 + 3 * 0.044715 * x2))
    return val, der


def halves(values):
    high = values.astype(bf16).astype(f32)
    return high, values - high


def block_kernel(share, joined, *refs):
    (
        x_all, g_all, pack, small_in, up, down,
        lo, dxo, grad, smalls, e_in, e_act, e_hid, e_dexp,
        x_s, g_s, att_s, n1_s, da_s, qkv, heads, probs, resid, logits, asq, dres_s, dn_s, rows_s,
        send_s, got, r32, e_s, ret, got2, eo_all, comb_all, dsm, sblk,
        part, rcv1, rcv2, rcv3, acc3, rcv4, srcv, a_buf, x_buf,
        full_s, small_s, small_g, wsem, wrecv,
        lsem, esem, xsem, gsem, grecv, ksem, krecv, s2, r2, s3, r3, s4, r4, ss, sr, es, er, obuf_sem,
    ) = refs
    wide_n, ctx_n, y_n, w, c, y, k = spot()
    ten_n = 2 * y_n
    plane = wide_n * ten_n
    n = plane * ctx_n
    me = (w * ctx_n + c) * ten_n + y * 2 + k
    mine = (w * y_n + y) * 2 + k
    width, packed = x_s.shape[2], pack.shape[-1]
    cols = packed // 4
    per = cols // HEAD_DIM
    slots_n = rows_s.shape[0] // 8
    length = x_s.shape[1]
    small = small_s if joined else small_in

    def weight(cb, lo_col, hi_col):
        if joined:
            return full_s[cb, :, :, :, :, lo_col:hi_col].reshape(width, hi_col - lo_col)
        return pack[cb, :, lo_col:hi_col]

    rows = grad.shape[0]
    logit_scale = 1.6 * math.sqrt(width)
    seq = near_first(c, ctx_n)
    bar = pltpu.get_barrier_semaphore()

    def place(d):
        return {"wide": d // (ctx_n * ten_n), "context": lax.rem(d // ten_n, ctx_n), "tensor": lax.rem(d, ten_n)}

    def hello(o, carry):
        pl.semaphore_signal(bar, inc=1, device_id=place(lax.rem(me + o, n)), device_id_type=pl.DeviceIdType.MESH)
        return carry

    lax.fori_loop(1, n, hello, 0)
    ins = [
        pltpu.make_async_copy(x_all.at[pl.ds(c * share, share)], x_s, lsem.at[0]),
        pltpu.make_async_copy(g_all.at[pl.ds(c * share, share)], g_s, lsem.at[1]),
    ]
    for cp in ins:
        cp.start()
    rows_s[...] = jnp.zeros_like(rows_s)
    dsm[...] = jnp.zeros_like(dsm)
    tall = length + -length % 16
    gap = tall - length // 16 * 16
    for i in range(share):
        edge = pl.ds(i * tall + tall - gap, gap)
        n1_s[edge, :] = jnp.zeros((gap, width), bf16)
        da_s[edge, :] = jnp.zeros((gap, width), bf16)
        for cb in range(ctx_n):
            heads[cb, edge, :] = jnp.zeros((gap, cols), bf16)

    def of(i):
        return pl.ds(pl.multiple_of(i * tall, 16), length)


    def along(a, cb, i, side, own):
        ref = (lo, dxo)[a].at[cb * share + i]
        src = (att_s, x_s)[a].at[i] if own else ref
        return remote(src, ref, gsem.at[a, side, cb, i], grecv.at[a, cb, i], context=c + 2 * side - 1)

    def launch(a, i):
        for side in (0, 1):

            @pl.when((c > 0) if side == 0 else (c < ctx_n - 1))
            def _():
                along(a, c, i, side, True).start()

    def onward(cb, side):
        if side == 0:
            return jnp.logical_and(cb > c, c > 0)
        return jnp.logical_and(cb < c, c < ctx_n - 1)

    def pump(a, todo):
        for step, i in todo:
            cb = seq[step]
            along(a, cb, i, 0, False).wait_recv()
            for side in (0, 1):

                @pl.when(onward(cb, side))
                def _():
                    along(a, cb, i, side, False).start()

    pairs = [(s, i) for s in range(1, ctx_n) for i in range(share)]
    pairs.sort(key=lambda p: (p[0] + p[1], p[1]))
    middle, late, rest = pairs[:1], pairs[1:4], pairs[4:]
    waves = [[p for p in pairs if p[0] + p[1] == d] for d in range(1, ctx_n + share - 1)]
    half = rows // 2

    def w_ctx(cb, side, own):
        ref = full_s.at[cb, w, y, k]
        return remote(pack if own else ref, ref, wsem.at[0, cb, side], wrecv.at[0, cb, 0], context=c + 2 * side - 1)

    def w_leg(cb, number, h, o):
        at = pl.ds(h * half, half)
        slot = number * 2 + h
        if (number == 0) == (h == 0):
            ref = full_s.at[cb, w, y, k, at] if number == 0 else full_s.at[cb, w, :, k, at]
            to = {"wide": lax.rem(w + o, wide_n)}
        else:
            ref = full_s.at[cb, w, y, k, at] if number == 0 else full_s.at[cb, :, y, k, at]
            to = {"tensor": lax.rem(y + o, y_n) * 2 + k}
        return remote(ref, ref, wsem.at[1 + slot, cb, o], wrecv.at[1 + slot, cb, o], **to)

    def w_legs(cb, number):
        out = []
        for h in (0, 1):
            on_wide = (number == 0) == (h == 0)
            out += [w_leg(cb, number, h, o) for o in range(1, wide_n if on_wide else y_n)]
        return out

    def w_core(cb):
        ref = full_s.at[cb, :, :, k]
        return remote(ref, ref, wsem.at[5, cb, 0], wrecv.at[5, cb, 0], tensor=y * 2 + 1 - k)

    def w_small(o):
        j = lax.rem(mine + o, plane)
        to = {"wide": j // ten_n, "tensor": lax.rem(j, ten_n)}
        return remote(small_in, small_g.at[w, y, k], wsem.at[6, 0, o], wrecv.at[6, 0, o], **to)

    def w_arrive(j):
        cb = seq[j]
        if j > 0:
            w_ctx(cb, 0, False).wait_recv()
            for side in (0, 1):

                @pl.when(onward(cb, side))
                def _():
                    w_ctx(cb, side, False).start()

        for cp in w_legs(cb, 0):
            cp.start()

    def w_second(j):
        for cp in w_legs(seq[j], 0):
            cp.wait_recv()
        for cp in w_legs(seq[j], 1):
            cp.start()

    def w_third(j):
        for cp in w_legs(seq[j], 1):
            cp.wait_recv()
        w_core(seq[j]).start()

    def w_ready(j):
        if joined:
            w_core(seq[j]).wait_recv()

    if joined:
        full_s[c, w, y, k] = pack[...]
        small_g[w, y, k] = small_in[...]
    pl.semaphore_wait(bar, n - 1)
    if joined:
        for side in (0, 1):

            @pl.when((c > 0) if side == 0 else (c < ctx_n - 1))
            def _():
                w_ctx(c, side, True).start()

        w_arrive(0)
        for o in range(1, plane):
            w_small(o).start()
        for o in range(1, plane):
            w_small(o).wait_recv()
        pieces = [small_g[j // ten_n, (j // 2) % y_n, j % 2][:, :rows] for j in range(plane)]
        small_s[...] = jnp.concatenate([p.astype(f32) for p in pieces], axis=1)
    keys, key_scale = router_unit(small[4 : 4 + slots_n, :].astype(f32))
    keys_hi, keys_lo = halves(keys)
    keys_two = jnp.concatenate([keys_hi, keys_lo], axis=0).astype(bf16)
    keys_three = jnp.concatenate([keys_hi, keys_lo, keys_hi], axis=0).astype(bf16)
    for cp in ins:
        cp.wait()

    def norm_first(i, carry):
        hat, _ = layer_stats(x_s[i].astype(f32))
        n1_s[of(i), :] = (hat * small[0:1, :].astype(f32) + small[2:3, :].astype(f32)).astype(bf16)
        return carry

    lax.fori_loop(0, share, norm_first, 0)

    def between(j, i):
        todo = {}
        if joined:
            todo = {
                (0, 0): lambda: w_third(1),
                (0, 1): lambda: w_second(2),
                (0, 2): lambda: w_arrive(3),
                (1, 0): lambda: w_third(2),
                (1, 1): lambda: w_second(3),
                (2, 0): lambda: w_third(3),
            }
        return todo.get((j, i))

    if joined:
        w_second(0)
        w_arrive(1)
        w_third(0)
        w_second(1)
        w_arrive(2)
    for j in range(ctx_n):
        w_ready(j)
        cb = seq[j]
        qkv_f = mm(n1_s[...], weight(cb, 0, 3 * cols))
        qkv[cb] = jnp.concatenate([qkv_f[:, :cols] * 0.125, qkv_f[:, cols:]], axis=1).astype(bf16)

        def attend(i, carry):
            for at in range(share):
                if between(j, at) is not None:
                    pl.when(i == at)(between(j, at))
            qkv_c = qkv[cb, of(i), :]
            mixed = []
            for h in range(per):
                q, kk, v = head_parts(qkv_c, h, per)
                s = mm(q, kk, NT)
                e = jnp.exp(s - jnp.max(s, axis=1, keepdims=True))
                p = (e * (1.0 / jnp.sum(e, axis=1, keepdims=True))).astype(bf16)
                probs[i, cb, h] = p
                mixed.append(mm(p, v).astype(bf16))
            heads[cb, of(i), :] = jnp.concatenate(mixed, axis=1)
            return carry

        lax.fori_loop(0, share, attend, 0)
        add = mm(heads[cb], weight(cb, 3 * cols, packed), NT)
        if j == 0:
            resid[...] = add
        else:
            resid[...] += add

    def attention_out(i, carry):
        att_s[i] = resid[of(i), :].astype(bf16)
        launch(0, i)
        return carry

    lax.fori_loop(0, share, attention_out, 0)

    def route(i, carry):
        att = resid[of(i), :]
        asq[i] = jnp.full(asq.shape[1:], jnp.sum(att * att), f32)
        res = x_s[i].astype(f32) + att
        resid[of(i), :] = res
        hat2, _ = layer_stats(res)
        second = hat2 * small[1:2, :].astype(f32) + small[3:4, :].astype(f32)
        unit = second * lax.rsqrt(jnp.sum(second * second, axis=-1, keepdims=True) + norm_eps)
        unit_hi, unit_lo = halves(unit)
        lg = mm(keys_two, unit_hi.astype(bf16), NT)
        lg = lg[:slots_n] + lg[slots_n:] + mm(keys_two[:slots_n], unit_lo.astype(bf16), NT)
        lg = logit_scale * lg
        logits[i] = lg
        disp = soft(lg, 1).astype(bf16)
        comb = soft(lg, 0).astype(bf16)
        comb_all[c, i, :, :length] = comb
        slots = mm(disp, second.astype(bf16)).astype(bf16)
        dexp = mm(comb, g_s[i]).astype(bf16)
        rows_s[...] += mm(pick_rows(slots_n, i), slots) + mm(pick_rows(slots_n, i + 4), dexp)
        return carry

    lax.fori_loop(0, share, route, 0)

    for e in range(slots_n):
        send_s[e] = rows_s[e * 8 : e * 8 + 8, :].astype(bf16)
    got[me] = send_s[w * ctx_n + c]

    def send_out(o, carry):
        d = lax.rem(me + o, n)
        remote(send_s.at[d // ten_n], got.at[me], esem.at[0], esem.at[1], **place(d)).start()
        return carry

    lax.fori_loop(1, n, send_out, 0)

    def drain(ref, sem):
        some = ref.at[pl.ds(0, n - 1)]
        pltpu.make_async_copy(some, some, sem).wait()

    pump(0, middle)
    drain(got, esem.at[1])

    group = min(n, 32)
    chunk = group * 8
    first = lax.rem(lax.broadcasted_iota(jnp.int32, (chunk, 1), 0), 8) < 4

    def expert_out(b, j):
        dst = (e_in, e_act, e_hid, e_dexp)[j]
        at = pl.ds(pl.multiple_of(b * chunk, chunk), chunk)
        return pltpu.make_async_copy(e_s.at[j], dst.at[at, :], xsem.at[j])

    def experts(b, carry):
        def widen(j, carry):
            r32[pl.ds(pl.multiple_of(j * 8, 8), 8), :] = got[b * group + j].astype(f32)
            return carry

        lax.fori_loop(0, group, widen, 0)

        @pl.when(b > 0)
        def _():
            for j in range(4):
                expert_out(b, j).wait()

        low = r32[...].astype(bf16)
        e_s[0] = low
        e_s[3] = pltpu.roll(r32[...], chunk - 4, 0).astype(bf16)
        hidden = mm(low, up[...])
        act_g = pltpu.roll(mm(low, down[...], NT), chunk - 4, 0)
        val, der = gelu_parts(hidden)
        active = jnp.where(first, val, 0.0).astype(bf16)
        hid_g = jnp.where(first, act_g * der, 0.0).astype(bf16)
        e_s[1] = active
        e_s[2] = hid_g
        part_o = mm(active, down[...])
        part_s = mm(hid_g, up[...], NT)
        r32[...] = jnp.where(first, part_o, pltpu.roll(part_s, 4, 0))
        for j in range(4):
            expert_out(b, j).start()

        def narrow(j, carry):
            ret[b * group + j] = r32[pl.ds(pl.multiple_of(j * 8, 8), 8), :].astype(bf16)
            return carry

        lax.fori_loop(0, group, narrow, 0)
        return carry

    lax.fori_loop(0, n // group, experts, 0)

    def send_back(o, carry):
        d = lax.rem(me + o, n)
        remote(ret.at[d], got2.at[me], esem.at[2], esem.at[3], **place(d)).start()
        return carry

    lax.fori_loop(1, n, send_back, 0)
    got2[me] = ret[me]
    pump(0, late)
    drain(got2, esem.at[3])

    def total(e, carry):
        s = got2[e * ten_n].astype(f32)
        for t in range(1, ten_n):
            s = s + got2[e * ten_n + t].astype(f32)
        rows_s[pl.ds(pl.multiple_of(e * 8, 8), 8), :] = s
        return carry

    lax.fori_loop(0, slots_n, total, 0)
    back = rows_s[...].astype(bf16)
    for i in range(share):
        eo_all[c, i] = mm(pick_rows(slots_n, i), back, TN).astype(bf16)

    def trade(o, ref, j, p):
        return remote(ref.at[p], ref.at[p], es.at[j, o], er.at[j, o], context=lax.rem(c + o, ctx_n))

    for o in range(1, ctx_n):
        trade(o, eo_all, 0, c).start()
        trade(o, comb_all, 1, c).start()

    def fetch(step, i, slot):
        img = seq[step] * share + i
        return (
            pltpu.make_async_copy(lo.at[img], a_buf.at[slot], obuf_sem.at[0, slot]),
            pltpu.make_async_copy(x_all.at[img], x_buf.at[slot], obuf_sem.at[1, slot]),
        )

    def put(step, i, slot):
        img = seq[step] * share + i
        return pltpu.make_async_copy(a_buf.at[slot], lo.at[img], obuf_sem.at[2, slot])

    def backward(i, carry):
        gain1, gain2 = small[0:1, :].astype(f32), small[1:2, :].astype(f32)
        g_low = g_s[i]
        res = resid[of(i), :]
        hat2, spread2 = layer_stats(res)
        second = hat2 * gain2 + small[3:4, :].astype(f32)
        tokens = second.astype(bf16)
        row_scale = lax.rsqrt(jnp.sum(second * second, axis=-1, keepdims=True) + norm_eps)
        unit = second * row_scale
        eo = eo_all[c, i]
        ds = mm(pick_rows(slots_n, i + 4), rows_s[...].astype(bf16), TN).astype(bf16)
        lg = logits[i]
        disp = soft(lg, 1)
        comb = soft(lg, 0)
        mixture = mm(comb.astype(bf16), eo, TN)
        result = res + mixture

        @pl.when(i > 1)
        def _():
            put(0, 0, 0).wait()

        a_buf[lax.rem(i, 2)] = result.astype(bf16)
        put(0, i, lax.rem(i, 2)).start()
        count = 1.0 / (length * width)
        lane = lax.broadcasted_iota(jnp.int32, (8, smalls.shape[2]), 1)
        sums = jnp.where(
            lane == 0,
            jnp.sum(result * result),
            jnp.where(lane == 1, asq[i], jnp.sum(mixture * mixture)),
        )
        at_row = lax.broadcasted_iota(jnp.int32, (8, smalls.shape[2]), 0)
        sblk[plane, :8, :] = jnp.where(at_row == i, jnp.sqrt(sums * count), sblk[plane, :8, :])
        dcomb = mm(eo, g_low, NT)
        ddisp = mm(ds, tokens, NT)
        dtok = mm(disp.astype(bf16), ds, TN)
        dlg = comb * (dcomb - jnp.sum(comb * dcomb, axis=0, keepdims=True)) + disp * (
            ddisp - jnp.sum(disp * ddisp, axis=1, keepdims=True)
        )
        dlg_hi, dlg_lo = halves(dlg)
        dlg_two = jnp.concatenate([dlg_hi, dlg_lo], axis=0).astype(bf16)
        dlg_three = jnp.concatenate([dlg_hi, dlg_hi, dlg_lo], axis=0).astype(bf16)
        dunit = logit_scale * mm(dlg_three, keys_three, TN)
        unit_hi, unit_lo = halves(unit)
        dk_part = mm(dlg_two, unit_hi.astype(bf16))
        dk_part = dk_part[:slots_n] + dk_part[slots_n:] + mm(dlg_two[:slots_n], unit_lo.astype(bf16))
        dsm[4 : 4 + slots_n, :] += logit_scale * dk_part
        dsec = dtok + row_scale * (dunit - unit * jnp.sum(unit * dunit, axis=-1, keepdims=True))
        dsm[1:2, :] += jnp.sum(dsec * hat2, axis=0, keepdims=True)
        dsm[3:4, :] += jnp.sum(dsec, axis=0, keepdims=True)
        dres = g_low.astype(f32) + norm_back(dsec * gain2, hat2, spread2)
        dres_s[...] = dres
        dattn = dres.astype(bf16)
        da_s[of(i), :] = dattn
        hat, spread = layer_stats(x_s[i].astype(f32))
        dn_s[...] = jnp.zeros_like(dn_s)

        @pl.when(i == 0)
        def _():
            pump(0, rest)

        def block(cb, carry):
            for j in range(1, share):

                @pl.when(jnp.logical_and(i == j, cb == ctx_n // 2))
                def _():
                    pump(1, waves[j - 1])

            dheads = mm(dattn, weight(cb, 3 * cols, packed)).astype(bf16)
            qkv_c = qkv[cb, of(i), :]
            along_heads = dheads.astype(f32) * heads[cb, of(i), :].astype(f32)
            grads = [[], [], []]
            for h in range(per):
                q, kk, v = head_parts(qkv_c, h, per)
                at = slice(h * HEAD_DIM, (h + 1) * HEAD_DIM)
                dh = dheads[:, at]
                p = probs[i, cb, h]
                dp = mm(dh, v, NT) - jnp.sum(along_heads[:, at], axis=1, keepdims=True)
                dsc = (p.astype(f32) * dp).astype(bf16)
                grads[0].append((mm(dsc, kk) * 0.125).astype(bf16))
                grads[1].append(mm(dsc, q, TN).astype(bf16))
                grads[2].append(mm(p, dh, TN).astype(bf16))
            dqkv = jnp.concatenate(grads[0] + grads[1] + grads[2], axis=1)
            qkv[cb, of(i), :] = dqkv
            dn_s[...] += mm(dqkv, weight(cb, 0, 3 * cols), NT)
            return carry

        lax.fori_loop(0, ctx_n, block, 0)
        dn = dn_s[...]
        dsm[0:1, :] += jnp.sum(dn * hat, axis=0, keepdims=True)
        dsm[2:3, :] += jnp.sum(dn, axis=0, keepdims=True)
        x_s[i] = (dres_s[...] + norm_back(dn * gain1, hat, spread)).astype(bf16)
        launch(1, i)
        return carry

    sblk[plane] = jnp.zeros(sblk.shape[1:], f32)
    lax.fori_loop(0, share, backward, 0)
    outs = [pltpu.make_async_copy(x_s, dxo.at[pl.ds(c * share, share)], lsem.at[1])]
    for cp in outs:
        cp.start()
    dkeys = dsm[4 : 4 + slots_n, :]
    dsm[4 : 4 + slots_n, :] = key_scale * (dkeys - keys * jnp.sum(keys * dkeys, axis=1, keepdims=True))

    def core(cc):
        return remote(part.at[cc, :, :, 1 - k], rcv1.at[cc], ksem.at[cc], krecv.at[cc], tensor=y * 2 + 1 - k)

    normed_t = n1_s[...].T
    dattn_t = da_s[...].T
    for cc in range(ctx_n):
        from_qkv = mm(normed_t, qkv[cc]).astype(bf16)
        from_proj = mm(dattn_t, heads[cc]).astype(bf16)
        for j in range(plane):
            at = (cc, j // ten_n, (j // 2) % y_n, j % 2)
            part[at + (slice(None), slice(0, 3 * cols))] = from_qkv[j * rows : (j + 1) * rows]
            part[at + (slice(None), slice(3 * cols, packed))] = from_proj[j * rows : (j + 1) * rows]
        core(cc).start()
        if cc == ctx_n // 2:
            pump(1, waves[2] if len(waves) > 2 else [])
    for j in range(plane):
        sblk[j, :, :rows] = dsm[:, j * rows : (j + 1) * rows]

    def small1(o):
        j = lax.rem(mine + o, plane)
        return remote(sblk.at[j], srcv.at[o], ss.at[o], sr.at[o], wide=j // ten_n, tensor=lax.rem(j, ten_n))

    for o in range(1, plane):
        small1(o).start()

    def hop(cc, number, o):
        on_wide = (cc % 2 == 0) == (number == 2)
        ss_, rr_ = (s2, r2) if number == 2 else (s3, r3)
        if on_wide:
            p = lax.rem(w + o, wide_n)
            to = {"wide": p}
            frm = rcv1.at[cc, p] if number == 2 else rcv1.at[cc, p, y]
            into = rcv2.at[cc, pl.ds(o * y_n, y_n)] if number == 2 else rcv3.at[cc, o]
        else:
            p = lax.rem(y + o, y_n)
            to = {"tensor": p * 2 + k}
            frm = rcv1.at[cc, :, p] if number == 2 else rcv1.at[cc, w, p]
            into = rcv2.at[cc, pl.ds(o * wide_n, wide_n)] if number == 2 else rcv3.at[cc, o]
        return remote(frm, into, ss_.at[cc, o], rr_.at[cc, o], **to)

    def peers(cc, number):
        on_wide = (cc % 2 == 0) == (number == 2)
        return range(1, wide_n if on_wide else y_n)

    for cc in range(ctx_n):
        core(cc).wait_recv()
        for wi in range(wide_n):
            for yi in range(y_n):
                rcv1[cc, wi, yi] = (part[cc, wi, yi, k].astype(f32) + rcv1[cc, wi, yi].astype(f32)).astype(bf16)
        for o in peers(cc, 2):
            hop(cc, 2, o).start()
    pump(1, waves[3] if len(waves) > 3 else [])

    for o in range(1, ctx_n):
        p = lax.rem(c + ctx_n - o, ctx_n)
        trade(o, eo_all, 0, p).wait_recv()
        trade(o, comb_all, 1, p).wait_recv()

    order = [(s, i) for s in range(1, ctx_n) for i in range(share)]

    def mix_some(lo_n, hi_n):
        for j in range(lo_n, hi_n):
            step, i = order[j]
            cb = seq[step]
            slot = (j + share) % 2
            for side in (0, 1):

                @pl.when(onward(cb, side))
                def _():
                    along(0, cb, i, side, False).wait_send()

            put(step, i, slot).wait()
            for cp in fetch(step, i, slot):
                cp.start()
            for cp in fetch(step, i, slot):
                cp.wait()
            mixed = mm(comb_all[cb, i, :, :length], eo_all[cb, i], TN)
            out = x_buf[slot].astype(f32) + a_buf[slot].astype(f32) + mixed
            a_buf[slot] = out.astype(bf16)
            put(step, i, slot).start()

    third = len(order) // 3
    mix_some(0, third)
    for cc in range(ctx_n):
        on_wide = cc % 2 == 0
        for o in peers(cc, 2):
            hop(cc, 2, o).wait_recv()
        for j in range(y_n if on_wide else wide_n):
            spot_j = (cc, w, j) if on_wide else (cc, j, y)
            tot = rcv1[spot_j].astype(f32)
            for o in peers(cc, 2):
                tot = tot + rcv2[cc, o * (y_n if on_wide else wide_n) + j].astype(f32)
            rcv1[spot_j] = tot.astype(bf16)
        for o in peers(cc, 3):
            hop(cc, 3, o).start()

    tot = sblk[mine]
    for o in range(1, plane):
        small1(o).wait_recv()
        tot = tot + srcv[o]
    smalls[c, : sblk.shape[1], :] = tot
    smalls[c, sblk.shape[1] :, :] = sblk[plane, :8, :]

    def small2(o, p):
        return remote(
            smalls.at[p], smalls.at[p], ss.at[plane + o], sr.at[plane + o], context=lax.rem(c + o, ctx_n)
        )

    for o in range(1, ctx_n):
        small2(o, c).start()
    pump(1, waves[4] if len(waves) > 4 else [])
    mix_some(third, 2 * third)

    def last(cc):
        return remote(acc3.at[cc], rcv4.at[c], s4.at[cc], r4.at[c], context=cc)

    for cc in range(ctx_n):
        for o in peers(cc, 3):
            hop(cc, 3, o).wait_recv()
        tot = rcv1[cc, w, y].astype(f32)
        for o in peers(cc, 3):
            tot = tot + rcv3[cc, o].astype(f32)
        acc3[cc] = tot.astype(bf16)

        @pl.when(c != cc)
        def _():
            last(cc).start()

    mix_some(2 * third, len(order))
    for wave in waves[5:]:
        pump(1, wave)
    tot = acc3[c].astype(f32)
    for o in range(1, ctx_n):
        p = lax.rem(c + o, ctx_n)
        remote(acc3.at[0], rcv4.at[p], s4.at[p], r4.at[p], context=p).wait_recv()
        tot = tot + rcv4[p].astype(f32)
    grad[...] = tot

    for slot in (0, 1):
        put(0, 0, slot).wait()
    for j in range(4):
        expert_out(0, j).wait()
    drain(ret, esem.at[2])

    def sent(o, carry):
        pltpu.make_async_copy(send_s.at[0], send_s.at[0], esem.at[0]).wait()
        return carry

    lax.fori_loop(1, n, sent, 0)
    for o in range(1, ctx_n):
        p = lax.rem(c + ctx_n - o, ctx_n)
        small2(o, p).wait_recv()
        small2(o, c).wait_send()
        trade(o, eo_all, 0, c).wait_send()
        trade(o, comb_all, 1, c).wait_send()
        last(lax.rem(c + o, ctx_n)).wait_send()
    for o in range(1, plane):
        small1(o).wait_send()
    for cc in range(ctx_n):
        core(cc).wait_send()
        for number in (2, 3):
            for o in peers(cc, number):
                hop(cc, number, o).wait_send()
    for cp in outs:
        cp.wait()
    if joined:
        for o in range(1, plane):
            w_small(o).wait_send()
        for cb in range(ctx_n):
            for number in (0, 1):
                for cp in w_legs(cb, number):
                    cp.wait_send()
            w_core(cb).wait_send()
            for side in (0, 1):
                go = (cb >= c, c > 0) if side == 0 else (cb <= c, c < ctx_n - 1)

                @pl.when(jnp.logical_and(*go))
                def _():
                    w_ctx(cb, side, True).wait_send()

    for a in (0, 1):
        for i in range(share):
            for side in (0, 1):

                @pl.when((c > 0) if side == 0 else (c < ctx_n - 1))
                def _():
                    along(a, c, i, side, True).wait_send()

    for step, i in order:
        for side in (0, 1):

            @pl.when(onward(seq[step], side))
            def _():
                along(1, seq[step], i, side, False).wait_send()


def run_block(x_all, g_all, pack, small, slots_n, up, down, rows, share):
    wide_n, ctx_n, ten_n = (lax.axis_size(a) for a in ("wide", "context", "tensor"))
    y_n = ten_n // 2
    plane = wide_n * ten_n
    n = plane * ctx_n
    most = max(wide_n, y_n)
    images, length, width = x_all.shape
    packed = pack.shape[-1]
    joined = pack.ndim == 2
    cols = packed // 4
    ff = up.shape[1]
    par8 = 4 + slots_n + -(4 + slots_n) % 8
    lanes = rows + -rows % 128
    blk = (rows, packed)
    acts = (share, length, width)
    wide_len = length + -length % 128
    tall = length + -length % 16
    dma = pltpu.SemaphoreType.DMA
    vm = pl.BlockSpec(memory_space=pltpu.VMEM)
    hbm = pl.BlockSpec(memory_space=pl.ANY)
    V = pltpu.VMEM
    shape = jax.ShapeDtypeStruct
    return pl.pallas_call(
        functools.partial(block_kernel, share, joined),
        out_shape=(
            shape((images, length, width), bf16),
            shape((images, length, width), bf16),
            shape(blk, f32),
            shape((ctx_n, par8 + 8, lanes), f32),
            shape((n * 8, width), bf16),
            shape((n * 8, ff), bf16),
            shape((n * 8, ff), bf16),
            shape((n * 8, width), bf16),
        ),
        in_specs=[hbm, hbm] + [vm] * 4,
        out_specs=(hbm, hbm, vm, vm) + (hbm,) * 4,
        scratch_shapes=[
            V(acts, bf16), V(acts, bf16), V(acts, bf16),
            V((share * tall, width), bf16),
            V((share * tall, width), bf16),
            V((ctx_n, share * tall, 3 * cols), bf16),
            V((ctx_n, share * tall, cols), bf16),
            V((share, ctx_n, cols // HEAD_DIM, length, length), bf16),
            V((share * tall, width), f32),
            V((share, slots_n, length), f32),
            V((share, 8, lanes), f32),
            V((length, width), f32),
            V((length, width), f32),
            V((slots_n * 8, width), f32),
            V((slots_n, 8, width), bf16),
            V((n, 8, width), bf16),
            V((min(n, 32) * 8, width), f32),
            V((4, min(n, 32) * 8, width), bf16),
            V((n, 8, width), bf16),
            V((n, 8, width), bf16),
            V((ctx_n, share, slots_n, width), bf16),
            V((ctx_n, share, slots_n, wide_len), bf16),
            V((par8, width), f32),
            V((plane + 1, par8, lanes), f32),
            V((ctx_n, wide_n, y_n, 2) + blk, bf16),
            V((ctx_n, wide_n, y_n) + blk, bf16),
            V((ctx_n, wide_n * y_n) + blk, bf16),
            V((ctx_n, most) + blk, bf16),
            V((ctx_n,) + blk, bf16),
            V((ctx_n,) + blk, bf16),
            V((plane, par8, lanes), f32),
            V((2, length, width), bf16),
            V((2, length, width), bf16),
            V((ctx_n, wide_n, y_n, 2) + blk if joined else (8, 128), bf16),
            V((small.shape[0], width) if joined else (8, 128), f32),
            V((wide_n, y_n, 2) + small.shape if joined else (8, 128), bf16),
            dma((7, ctx_n, plane) if joined else (1,)), dma((7, ctx_n, plane) if joined else (1,)),
            dma((2,)), dma((4,)), dma((4,)),
            dma((2, 2, ctx_n, share)), dma((2, ctx_n, share)),
            dma((ctx_n,)), dma((ctx_n,)),
            dma((ctx_n, most)), dma((ctx_n, most)),
            dma((ctx_n, most)), dma((ctx_n, most)),
            dma((ctx_n,)), dma((ctx_n,)),
            dma((plane + ctx_n,)), dma((plane + ctx_n,)),
            dma((2, ctx_n)), dma((2, ctx_n)),
            dma((3, 2)),
        ],
        compiler_params=pltpu.CompilerParams(
            collective_id=2, has_side_effects=True, vmem_limit_bytes=67043328
        ),
    )(x_all, g_all, pack, small, up, down)


def on_device(
    layer_input,
    qkv_weight,
    proj_weight,
    norm_gains,
    norm_biases,
    router_keys,
    up_weight,
    down_weight,
    out_cotangent,
):
    images, length, width = layer_input.shape
    wide_n, ctx_n, ten_n = (lax.axis_size(a) for a in ("wide", "context", "tensor"))
    share = images // ctx_n
    slots_n = router_keys.shape[1]
    rows, _, cols = qkv_weight.shape
    plane = wide_n * ten_n
    lanes = rows + -rows % 128

    pack = jnp.concatenate([qkv_weight.reshape(rows, 3 * cols), proj_weight.T], axis=1)
    small = jnp.concatenate([norm_gains, norm_biases, router_keys.T], axis=0)
    params = small.shape[0]
    small = jnp.pad(small, ((0, -params % 16), (0, lanes - rows)))
    if rows % 32 == 0:
        weights = pack
    else:
        weights, small = gather_weights(pack, small)
        weights = weights.reshape(ctx_n, width, 4 * cols)
        small = small.reshape((-1,) + small.shape[3:])[:, :params, :rows]
        small = small.transpose(1, 0, 2).reshape(params, width)
    layer_output, input_grad, dpack, dsmall, e_in, e_act, e_hid, e_dexp = run_block(
        layer_input, out_cotangent, weights, small, slots_n, up_weight[0], down_weight[0], rows, share
    )
    up_grad = mm(e_in, e_hid, TN)
    down_grad = mm(e_act, e_dexp, TN)
    rms = dsmall[:, dsmall.shape[1] - 8 :, :3][:, :share].reshape(images, 3)
    dsmall = jnp.sum(dsmall[:, :params, :rows], axis=0)
    return (
        layer_output,
        rms,
        input_grad,
        dpack[:, : 3 * cols].reshape(rows, 3, cols),
        dpack[:, 3 * cols :].T,
        dsmall[0:2],
        dsmall[2:4],
        dsmall[4:].T,
        up_grad[None],
        down_grad[None],
    )


def solution(mesh):
    images = P(("wide", "tensor"), None, None)
    qkv = P(("wide", "tensor"), None, "context")
    proj = P("context", ("wide", "tensor"))
    lane = P(None, ("wide", "tensor"))
    rowed = P(("wide", "tensor"), None)
    up = P(("wide", "context"), None, "tensor")
    down = P(("wide", "context"), "tensor", None)
    return jax.shard_map(
        on_device,
        mesh=mesh,
        in_specs=(images, qkv, proj, lane, lane, rowed, up, down, images),
        out_specs=(images, rowed, images, qkv, proj, lane, lane, rowed, up, down),
        check_vma=False,
    )
```

```python
import functools
import math

import jax
import jax.numpy as jnp
from jax import lax
from jax.experimental import pallas as pl
from jax.experimental.pallas import tpu as pltpu
from jax.sharding import PartitionSpec as P

f32 = jnp.float32
bf16 = jnp.bfloat16

HEAD_DIM = 64
norm_eps = 1e-06
highest = lax.Precision.HIGHEST
NN = (((1,), (0,)), ((), ()))
NT = (((1,), (1,)), ((), ()))
TN = (((0,), (0,)), ((), ()))


def mm(a, b, dims=NN, precision=None):
    return lax.dot_general(a, b, dims, precision=precision, preferred_element_type=f32)


def layer_stats(values):
    center = values - jnp.mean(values, axis=-1, keepdims=True)
    spread = lax.rsqrt(jnp.mean(center * center, axis=-1, keepdims=True) + norm_eps)
    return (center * spread, spread)


def norm_back(upstream, scaled, spread):
    return spread * (
        upstream
        - jnp.mean(upstream, axis=-1, keepdims=True)
        - scaled * jnp.mean(upstream * scaled, axis=-1, keepdims=True)
    )


def soft(values, axis):
    e = jnp.exp(values - jnp.max(values, axis=axis, keepdims=True))
    return e / jnp.sum(e, axis=axis, keepdims=True)


def pick_rows(slots_n, row):
    r = lax.broadcasted_iota(jnp.int32, (slots_n * 8, slots_n), 0)
    s = lax.broadcasted_iota(jnp.int32, (slots_n * 8, slots_n), 1)
    return jnp.where(r == s * 8 + row, 1.0, 0.0).astype(bf16)


def router_unit(keys):
    scale = lax.rsqrt(jnp.sum(keys * keys, axis=1, keepdims=True) + norm_eps)
    return keys * scale, scale


def head_parts(block, h, per):
    at = [j * per * HEAD_DIM + h * HEAD_DIM for j in range(3)]
    return [block[:, a : a + HEAD_DIM] for a in at]


def remote(src, dst, ssem, rsem, **where):
    return pltpu.make_async_remote_copy(
        src_ref=src,
        dst_ref=dst,
        send_sem=ssem,
        recv_sem=rsem,
        device_id=where,
        device_id_type=pl.DeviceIdType.MESH,
    )


def spot():
    wide_n, ctx_n, ten_n = (lax.axis_size(a) for a in ("wide", "context", "tensor"))
    w, c, t = (lax.axis_index(a) for a in ("wide", "context", "tensor"))
    return wide_n, ctx_n, ten_n // 2, w, c, t // 2, lax.rem(t, 2)


def greet_plane(bar, wide_n, y_n, w, y, k):
    for o in range(1, wide_n * y_n * 2):
        j = lax.rem((w * y_n + y) * 2 + k + o, wide_n * y_n * 2)
        pl.semaphore_signal(
            bar,
            inc=1,
            device_id={"wide": j // (y_n * 2), "tensor": lax.rem(j, y_n * 2)},
            device_id_type=pl.DeviceIdType.MESH,
        )
    return wide_n * y_n * 2 - 1


def near_first(c, ctx_n):
    seq = []
    for j in range(ctx_n):
        cb = 0
        for p in range(ctx_n):
            order = sorted(range(ctx_n), key=lambda q: (abs(q - p), q))
            cb = jnp.where(c == p, order[j], cb)
        seq.append(cb)
    return seq


def gather_kernel(pack, small, full, smalls, csem, crecv, wsem, wrecv, ysem, yrecv, ksem, krecv, ssem, srecv, local):
    wide_n, ctx_n, y_n, w, c, y, k = spot()
    bar = pltpu.get_barrier_semaphore()
    met = greet_plane(bar, wide_n, y_n, w, y, k)

    @pl.when(c > 0)
    def _():
        pl.semaphore_signal(bar, inc=1, device_id={"context": c - 1}, device_id_type=pl.DeviceIdType.MESH)

    @pl.when(c < ctx_n - 1)
    def _():
        pl.semaphore_signal(bar, inc=1, device_id={"context": c + 1}, device_id_type=pl.DeviceIdType.MESH)

    mine = pltpu.make_async_copy(pack, full.at[c, w, y, k], local.at[0])
    mine_small = pltpu.make_async_copy(small, smalls.at[w, y, k], local.at[1])
    mine.start()
    mine_small.start()
    pl.semaphore_wait(bar, met + (c + ctx_n - 1) // ctx_n + (2 * ctx_n - 2 - c) // ctx_n)

    def along(cb, side, src):
        return remote(src, full.at[cb, w, y, k], csem.at[side, cb], crecv.at[cb], context=c + 2 * side - 1)

    for side in (0, 1):

        @pl.when((c > 0) if side == 0 else (c < ctx_n - 1))
        def _():
            along(c, side, pack).start()

    def small_copy(o):
        j = lax.rem((w * y_n + y) * 2 + k + o, wide_n * y_n * 2)
        return remote(
            small, smalls.at[w, y, k], ssem.at[o], srecv.at[o], wide=j // (y_n * 2), tensor=lax.rem(j, y_n * 2)
        )

    for o in range(1, wide_n * y_n * 2):
        small_copy(o).start()

    seq = near_first(c, ctx_n)

    def leg(cb, number, o, start):
        even = lax.rem(cb, 2) == 0
        for on_wide in (True, False):
            n = wide_n if on_wide else y_n
            if o >= n:
                continue
            first = number == 0
            want_even = on_wide == first

            @pl.when(even if want_even else jnp.logical_not(even))
            def _():
                if on_wide:
                    ref = full.at[cb, w, y, k] if first else full.at[cb, w, :, k]
                    to = {"wide": lax.rem(w + o, wide_n)}
                    sems = (wsem.at[cb, o], wrecv.at[cb, o])
                else:
                    ref = full.at[cb, w, y, k] if first else full.at[cb, :, y, k]
                    to = {"tensor": lax.rem(y + o, y_n) * 2 + k}
                    sems = (ysem.at[cb, o], yrecv.at[cb, o])
                cp = remote(ref, ref, *sems, **to)
                if start == "start":
                    cp.start()
                elif start == "recv":
                    cp.wait_recv()
                else:
                    cp.wait_send()

    most = max(wide_n, y_n)

    def core(cb):
        ref = full.at[cb, :, :, k]
        return remote(ref, ref, ksem.at[cb], krecv.at[cb], tensor=y * 2 + 1 - k)

    mine.wait()
    mine_small.wait()
    for step in range(ctx_n + 2):
        if step < ctx_n:
            cb = seq[step]
            if step > 0:
                along(cb, 0, pack).wait_recv()
                for side in (0, 1):
                    go = jnp.logical_and(cb > c, c > 0) if side == 0 else jnp.logical_and(cb < c, c < ctx_n - 1)

                    @pl.when(go)
                    def _():
                        along(cb, side, full.at[cb, w, y, k]).start()

            for o in range(1, most):
                leg(cb, 0, o, "start")
        if 0 < step <= ctx_n:
            cb = seq[step - 1]
            for o in range(1, most):
                leg(cb, 0, o, "recv")
            for o in range(1, most):
                leg(cb, 1, o, "start")
        if step > 1:
            cb = seq[step - 2]
            for o in range(1, most):
                leg(cb, 1, o, "recv")
            core(cb).start()
    for step in range(ctx_n):
        core(seq[step]).wait_recv()
    for o in range(1, wide_n * y_n * 2):
        cp = small_copy(o)
        cp.wait_recv()
        cp.wait_send()
    for step in range(ctx_n):
        cb = seq[step]
        for side in (0, 1):
            go = jnp.logical_and(cb >= c, c > 0) if side == 0 else jnp.logical_and(cb <= c, c < ctx_n - 1)

            @pl.when(go)
            def _():
                along(cb, side, pack).wait_send()

        for number in (0, 1):
            for o in range(1, most):
                leg(cb, number, o, "send")
        core(cb).wait_send()


def gather_weights(pack, small):
    wide_n, ctx_n, ten_n = (lax.axis_size(a) for a in ("wide", "context", "tensor"))
    y_n = ten_n // 2
    dma = pltpu.SemaphoreType.DMA
    vm = pl.BlockSpec(memory_space=pltpu.VMEM)
    return pl.pallas_call(
        gather_kernel,
        out_shape=(
            jax.ShapeDtypeStruct((ctx_n, wide_n, y_n, 2) + pack.shape, pack.dtype),
            jax.ShapeDtypeStruct((wide_n, y_n, 2) + small.shape, small.dtype),
        ),
        in_specs=[vm, vm],
        out_specs=(vm, vm),
        scratch_shapes=[
            dma((2, ctx_n)), dma((ctx_n,)),
            dma((ctx_n, wide_n)), dma((ctx_n, wide_n)),
            dma((ctx_n, y_n)), dma((ctx_n, y_n)),
            dma((ctx_n,)), dma((ctx_n,)),
            dma((wide_n * ten_n,)), dma((wide_n * ten_n,)),
            dma((2,)),
        ],
        compiler_params=pltpu.CompilerParams(collective_id=1, has_side_effects=True),
    )(pack, small)


def gelu_parts(x):
    a = 0.7978845608028654
    x2 = x * x
    th = jnp.tanh(a * x * (1.0 + 0.044715 * x2))
    val = 0.5 * x * (1.0 + th)
    der = 0.5 * (1.0 + th) + 0.5 * x * (1.0 - th * th) * (a * (1.0 + 3 * 0.044715 * x2))
    return val, der


def halves(values):
    high = values.astype(bf16).astype(f32)
    return high, values - high


def block_kernel(share, joined, *refs):
    (
        x_all, g_all, pack, small_in, up, down,
        lo, dxo, grad, smalls, e_in, e_act, e_hid, e_dexp,
        x_s, g_s, att_s, n1_s, da_s, qkv, heads, probs, resid, logits, asq, dres_s, dn_s, rows_s,
        send_s, got, r32, e_s, ret, got2, back_g, eo_all, comb_all, dsm, sblk,
        part, rcv1, rcv2, rcv3, acc3, rcv4, srcv, a_buf, x_buf,
        full_s, small_s, small_g, wsem, wrecv,
        lsem, esem, xsem, gsem, grecv, ksem, krecv, s2, r2, s3, r3, s4, r4, ss, sr, es, er, obuf_sem,
    ) = refs
    wide_n, ctx_n, y_n, w, c, y, k = spot()
    ten_n = 2 * y_n
    plane = wide_n * ten_n
    n = plane * ctx_n
    me = (w * ctx_n + c) * ten_n + y * 2 + k
    mine = (w * y_n + y) * 2 + k
    width, packed = x_s.shape[2], pack.shape[-1]
    cols = packed // 4
    per = cols // HEAD_DIM
    slots_n = rows_s.shape[0] // 8
    length = x_s.shape[1]
    small = small_s if joined else small_in

    def weight(cb, lo_col, hi_col):
        if joined:
            return full_s[cb, :, :, :, :, lo_col:hi_col].reshape(width, hi_col - lo_col)
        return pack[cb, :, lo_col:hi_col]

    rows = grad.shape[0]
    logit_scale = 1.6 * math.sqrt(width)
    seq = near_first(c, ctx_n)
    bar = pltpu.get_barrier_semaphore()

    def place(d):
        return {"wide": d // (ctx_n * ten_n), "context": lax.rem(d // ten_n, ctx_n), "tensor": lax.rem(d, ten_n)}

    def hello(o, carry):
        pl.semaphore_signal(bar, inc=1, device_id=place(lax.rem(me + o, n)), device_id_type=pl.DeviceIdType.MESH)
        return carry

    lax.fori_loop(1, n, hello, 0)
    ins = [
        pltpu.make_async_copy(x_all.at[pl.ds(c * share, share)], x_s, lsem.at[0]),
        pltpu.make_async_copy(g_all.at[pl.ds(c * share, share)], g_s, lsem.at[1]),
    ]
    for cp in ins:
        cp.start()
    rows_s[...] = jnp.zeros_like(rows_s)
    dsm[...] = jnp.zeros_like(dsm)
    tall = length + -length % 16
    gap = tall - length // 16 * 16
    for i in range(share):
        edge = pl.ds(i * tall + tall - gap, gap)
        n1_s[edge, :] = jnp.zeros((gap, width), bf16)
        da_s[edge, :] = jnp.zeros((gap, width), bf16)
        for cb in range(ctx_n):
            heads[cb, edge, :] = jnp.zeros((gap, cols), bf16)

    def of(i):
        return pl.ds(pl.multiple_of(i * tall, 16), length)


    def along(a, cb, i, side, own):
        ref = (lo, dxo)[a].at[cb * share + i]
        src = (att_s, x_s)[a].at[i] if own else ref
        return remote(src, ref, gsem.at[a, side, cb, i], grecv.at[a, cb, i], context=c + 2 * side - 1)

    def launch(a, i):
        for side in (0, 1):

            @pl.when((c > 0) if side == 0 else (c < ctx_n - 1))
            def _():
                along(a, c, i, side, True).start()

    def onward(cb, side):
        if side == 0:
            return jnp.logical_and(cb > c, c > 0)
        return jnp.logical_and(cb < c, c < ctx_n - 1)

    def pump(a, steps, i):
        for step in steps:
            cb = seq[step]
            for side in (0, 1):

                @pl.when(onward(cb, side))
                def _():
                    along(a, cb, i, 0, False).wait_recv()
                    along(a, cb, i, side, False).start()

    def arrived(a, step, i):
        cb = seq[step]

        @pl.when(jnp.logical_not(jnp.logical_or(onward(cb, 0), onward(cb, 1))))
        def _():
            along(a, cb, i, 0, False).wait_recv()

    near, far = list(range(1, min(3, ctx_n))), list(range(3, ctx_n))

    half = rows // 2

    def w_ctx(cb, side, own):
        ref = full_s.at[cb, w, y, k]
        return remote(pack if own else ref, ref, wsem.at[0, cb, side], wrecv.at[0, cb, 0], context=c + 2 * side - 1)

    def w_leg(cb, number, h, o):
        at = pl.ds(h * half, half)
        slot = number * 2 + h
        if (number == 0) == (h == 0):
            ref = full_s.at[cb, w, y, k, at] if number == 0 else full_s.at[cb, w, :, k, at]
            to = {"wide": lax.rem(w + o, wide_n)}
        else:
            ref = full_s.at[cb, w, y, k, at] if number == 0 else full_s.at[cb, :, y, k, at]
            to = {"tensor": lax.rem(y + o, y_n) * 2 + k}
        return remote(ref, ref, wsem.at[1 + slot, cb, o], wrecv.at[1 + slot, cb, o], **to)

    def w_legs(cb, number):
        out = []
        for h in (0, 1):
            on_wide = (number == 0) == (h == 0)
            out += [w_leg(cb, number, h, o) for o in range(1, wide_n if on_wide else y_n)]
        return out

    def w_core(cb):
        ref = full_s.at[cb, :, :, k]
        return remote(ref, ref, wsem.at[5, cb, 0], wrecv.at[5, cb, 0], tensor=y * 2 + 1 - k)

    def w_small(o):
        j = lax.rem(mine + o, plane)
        to = {"wide": j // ten_n, "tensor": lax.rem(j, ten_n)}
        return remote(small_in, small_g.at[w, y, k], wsem.at[6, 0, o], wrecv.at[6, 0, o], **to)

    def w_arrive(j):
        cb = seq[j]
        if j > 0:
            w_ctx(cb, 0, False).wait_recv()
            for side in (0, 1):

                @pl.when(onward(cb, side))
                def _():
                    w_ctx(cb, side, False).start()

        for cp in w_legs(cb, 0):
            cp.start()

    def w_second(j):
        for cp in w_legs(seq[j], 0):
            cp.wait_recv()
        for cp in w_legs(seq[j], 1):
            cp.start()

    def w_third(j):
        for cp in w_legs(seq[j], 1):
            cp.wait_recv()
        w_core(seq[j]).start()

    def w_ready(j):
        if joined:
            w_core(seq[j]).wait_recv()

    if joined:
        full_s[c, w, y, k] = pack[...]
        small_g[w, y, k] = small_in[...]
    pl.semaphore_wait(bar, n - 1)
    if joined:
        for side in (0, 1):

            @pl.when((c > 0) if side == 0 else (c < ctx_n - 1))
            def _():
                w_ctx(c, side, True).start()

        w_arrive(0)
        for o in range(1, plane):
            w_small(o).start()
        for o in range(1, plane):
            w_small(o).wait_recv()
        pieces = [small_g[j // ten_n, (j // 2) % y_n, j % 2][:, :rows] for j in range(plane)]
        small_s[...] = jnp.concatenate([p.astype(f32) for p in pieces], axis=1)
    keys, key_scale = router_unit(small[4 : 4 + slots_n, :].astype(f32))
    keys_hi, keys_lo = halves(keys)
    keys_two = jnp.concatenate([keys_hi, keys_lo], axis=0).astype(bf16)
    keys_three = jnp.concatenate([keys_hi, keys_lo, keys_hi], axis=0).astype(bf16)
    for cp in ins:
        cp.wait()

    def norm_first(i, carry):
        hat, _ = layer_stats(x_s[i].astype(f32))
        n1_s[of(i), :] = (hat * small[0:1, :].astype(f32) + small[2:3, :].astype(f32)).astype(bf16)
        return carry

    lax.fori_loop(0, share, norm_first, 0)

    def between(j, i):
        todo = {}
        if joined:
            todo = {
                (0, 0): lambda: w_third(1),
                (0, 1): lambda: w_second(2),
                (0, 2): lambda: w_arrive(3),
                (1, 0): lambda: w_third(2),
                (1, 1): lambda: w_second(3),
                (2, 0): lambda: w_third(3),
            }
        return todo.get((j, i))

    if joined:
        w_second(0)
        w_arrive(1)
        w_third(0)
        w_second(1)
        w_arrive(2)
    for j in range(ctx_n):
        w_ready(j)
        cb = seq[j]
        qkv_f = mm(n1_s[...], weight(cb, 0, 3 * cols))
        qkv[cb] = jnp.concatenate([qkv_f[:, :cols] * 0.125, qkv_f[:, cols:]], axis=1).astype(bf16)

        def attend(i, carry):
            for at in range(share):
                if between(j, at) is not None:
                    pl.when(i == at)(between(j, at))
            qkv_c = qkv[cb, of(i), :]
            mixed = []
            for h in range(per):
                q, kk, v = head_parts(qkv_c, h, per)
                s = mm(q, kk, NT)
                e = jnp.exp(s - jnp.max(s, axis=1, keepdims=True))
                p = (e * (1.0 / jnp.sum(e, axis=1, keepdims=True))).astype(bf16)
                probs[i, cb, h] = p
                mixed.append(mm(p, v).astype(bf16))
            heads[cb, of(i), :] = jnp.concatenate(mixed, axis=1)
            return carry

        lax.fori_loop(0, share, attend, 0)
        add = mm(heads[cb], weight(cb, 3 * cols, packed), NT)
        if j == 0:
            resid[...] = add
        else:
            resid[...] += add

    def attention_out(i, carry):
        att_s[i] = resid[of(i), :].astype(bf16)
        return carry

    lax.fori_loop(0, share, attention_out, 0)

    def route(i, carry):
        att = resid[of(i), :]
        asq[i] = jnp.full(asq.shape[1:], jnp.sum(att * att), f32)
        res = x_s[i].astype(f32) + att
        resid[of(i), :] = res
        hat2, _ = layer_stats(res)
        second = hat2 * small[1:2, :].astype(f32) + small[3:4, :].astype(f32)
        unit = second * lax.rsqrt(jnp.sum(second * second, axis=-1, keepdims=True) + norm_eps)
        unit_hi, unit_lo = halves(unit)
        lg = mm(keys_two, unit_hi.astype(bf16), NT)
        lg = lg[:slots_n] + lg[slots_n:] + mm(keys_two[:slots_n], unit_lo.astype(bf16), NT)
        lg = logit_scale * lg
        logits[i] = lg
        disp = soft(lg, 1).astype(bf16)
        comb = soft(lg, 0).astype(bf16)
        comb_all[c, i, :, :length] = comb
        slots = mm(disp, second.astype(bf16)).astype(bf16)
        dexp = mm(comb, g_s[i]).astype(bf16)
        rows_s[...] += mm(pick_rows(slots_n, i), slots) + mm(pick_rows(slots_n, i + 4), dexp)
        return carry

    lax.fori_loop(0, share, route, 0)

    for e in range(slots_n):
        send_s[e] = rows_s[e * 8 : e * 8 + 8, :].astype(bf16)
    spot_e = w * ctx_n + c
    spot_t = y * 2 + k
    pairs_n = wide_n * ctx_n

    def expert_at(o):
        p = lax.rem(spot_e + o, pairs_n)
        return p, {"wide": p // ctx_n, "context": lax.rem(p, ctx_n)}

    def drain(ref, count, sem):
        some = ref.at[pl.ds(0, count)]
        pltpu.make_async_copy(some, some, sem).wait()

    for o in range(1, pairs_n):
        p, to = expert_at(o)
        remote(send_s.at[p], got.at[spot_t, spot_e], esem.at[0], esem.at[1], **to).start()
    got[spot_t, spot_e] = send_s[spot_e]
    for i in range(share):
        launch(0, i)
    drain(got.at[spot_t], pairs_n - 1, esem.at[1])
    for o in range(1, ten_n):
        mine_in = got.at[spot_t]
        remote(mine_in, mine_in, esem.at[2], esem.at[3], tensor=lax.rem(spot_t + o, ten_n)).start()
    drain(got, ten_n - 1, esem.at[3])

    group = min(n, 32)
    chunk = group * 8
    first = lax.rem(lax.broadcasted_iota(jnp.int32, (chunk, 1), 0), 8) < 4

    def expert_out(b, j):
        dst = (e_in, e_act, e_hid, e_dexp)[j]
        at = pl.ds(pl.multiple_of(b * chunk, chunk), chunk)
        return pltpu.make_async_copy(e_s.at[j], dst.at[at, :], xsem.at[j])

    def experts(b, carry):
        def widen(j, carry):
            r32[pl.ds(pl.multiple_of(j * 8, 8), 8), :] = got[(b * group + j) // pairs_n, lax.rem(b * group + j, pairs_n)].astype(f32)
            return carry

        lax.fori_loop(0, group, widen, 0)

        @pl.when(b > 0)
        def _():
            for j in range(4):
                expert_out(b, j).wait()

        low = r32[...].astype(bf16)
        e_s[0] = low
        e_s[3] = pltpu.roll(r32[...], chunk - 4, 0).astype(bf16)
        hidden = mm(low, up[...])
        act_g = pltpu.roll(mm(low, down[...], NT), chunk - 4, 0)
        val, der = gelu_parts(hidden)
        active = jnp.where(first, val, 0.0).astype(bf16)
        hid_g = jnp.where(first, act_g * der, 0.0).astype(bf16)
        e_s[1] = active
        e_s[2] = hid_g
        part_o = mm(active, down[...])
        part_s = mm(hid_g, up[...], NT)
        r32[...] = jnp.where(first, part_o, pltpu.roll(part_s, 4, 0))
        for j in range(4):
            expert_out(b, j).start()

        def narrow(j, carry):
            ret[(b * group + j) // pairs_n, lax.rem(b * group + j, pairs_n)] = r32[pl.ds(pl.multiple_of(j * 8, 8), 8), :].astype(bf16)
            return carry

        lax.fori_loop(0, group, narrow, 0)
        return carry

    lax.fori_loop(0, n // group, experts, 0)

    for o in range(1, ten_n):
        p = lax.rem(spot_t + o, ten_n)
        remote(ret.at[p], got2.at[spot_t], esem.at[4], esem.at[5], tensor=p).start()
    got2[spot_t] = ret[spot_t]
    drain(got2, ten_n - 1, esem.at[5])
    drain(send_s, pairs_n - 1, esem.at[0])

    def total(e, carry):
        s = got2[0, e].astype(f32)
        for t in range(1, ten_n):
            s = s + got2[t, e].astype(f32)
        send_s[e] = s.astype(bf16)
        return carry

    lax.fori_loop(0, pairs_n, total, 0)
    for o in range(1, pairs_n):
        p, to = expert_at(o)
        remote(send_s.at[p], back_g.at[spot_e], esem.at[6], esem.at[7], **to).start()
    back_g[spot_e] = send_s[spot_e]
    for i in range(share):
        pump(0, near, i)
    drain(back_g, pairs_n - 1, esem.at[7])

    def spread(e, carry):
        rows_s[pl.ds(pl.multiple_of(e * 8, 8), 8), :] = back_g[e].astype(f32)
        return carry

    lax.fori_loop(0, slots_n, spread, 0)
    back = rows_s[...].astype(bf16)
    for i in range(share):
        eo_all[c, i] = mm(pick_rows(slots_n, i), back, TN).astype(bf16)

    def trade(o, ref, j, p):
        return remote(ref.at[p], ref.at[p], es.at[j, o], er.at[j, o], context=lax.rem(c + o, ctx_n))

    for o in range(1, ctx_n):
        trade(o, eo_all, 0, c).start()
        trade(o, comb_all, 1, c).start()

    def fetch(step, i, slot):
        img = seq[step] * share + i
        return (
            pltpu.make_async_copy(lo.at[img], a_buf.at[slot], obuf_sem.at[0, slot]),
            pltpu.make_async_copy(x_all.at[img], x_buf, obuf_sem.at[1, slot]),
        )

    def put(step, i, slot):
        img = seq[step] * share + i
        return pltpu.make_async_copy(a_buf.at[slot], lo.at[img], obuf_sem.at[2, slot])

    def backward(i, carry):
        gain1, gain2 = small[0:1, :].astype(f32), small[1:2, :].astype(f32)
        g_low = g_s[i]
        res = resid[of(i), :]
        hat2, spread2 = layer_stats(res)
        second = hat2 * gain2 + small[3:4, :].astype(f32)
        tokens = second.astype(bf16)
        row_scale = lax.rsqrt(jnp.sum(second * second, axis=-1, keepdims=True) + norm_eps)
        unit = second * row_scale
        eo = eo_all[c, i]
        ds = mm(pick_rows(slots_n, i + 4), rows_s[...].astype(bf16), TN).astype(bf16)
        lg = logits[i]
        disp = soft(lg, 1)
        comb = soft(lg, 0)
        mixture = mm(comb.astype(bf16), eo, TN)
        result = res + mixture

        @pl.when(i > 1)
        def _():
            put(0, 0, 0).wait()

        a_buf[lax.rem(i, 2)] = result.astype(bf16)
        put(0, i, lax.rem(i, 2)).start()
        count = 1.0 / (length * width)
        lane = lax.broadcasted_iota(jnp.int32, (8, smalls.shape[2]), 1)
        sums = jnp.where(
            lane == 0,
            jnp.sum(result * result),
            jnp.where(lane == 1, asq[i], jnp.sum(mixture * mixture)),
        )
        at_row = lax.broadcasted_iota(jnp.int32, (8, smalls.shape[2]), 0)
        sblk[plane, :8, :] = jnp.where(at_row == i, jnp.sqrt(sums * count), sblk[plane, :8, :])
        dcomb = mm(eo, g_low, NT)
        ddisp = mm(ds, tokens, NT)
        dtok = mm(disp.astype(bf16), ds, TN)
        dlg = comb * (dcomb - jnp.sum(comb * dcomb, axis=0, keepdims=True)) + disp * (
            ddisp - jnp.sum(disp * ddisp, axis=1, keepdims=True)
        )
        dlg_hi, dlg_lo = halves(dlg)
        dlg_two = jnp.concatenate([dlg_hi, dlg_lo], axis=0).astype(bf16)
        dlg_three = jnp.concatenate([dlg_hi, dlg_hi, dlg_lo], axis=0).astype(bf16)
        dunit = logit_scale * mm(dlg_three, keys_three, TN)
        unit_hi, unit_lo = halves(unit)
        dk_part = mm(dlg_two, unit_hi.astype(bf16))
        dk_part = dk_part[:slots_n] + dk_part[slots_n:] + mm(dlg_two[:slots_n], unit_lo.astype(bf16))
        dsm[4 : 4 + slots_n, :] += logit_scale * dk_part
        dsec = dtok + row_scale * (dunit - unit * jnp.sum(unit * dunit, axis=-1, keepdims=True))
        dsm[1:2, :] += jnp.sum(dsec * hat2, axis=0, keepdims=True)
        dsm[3:4, :] += jnp.sum(dsec, axis=0, keepdims=True)
        dres = g_low.astype(f32) + norm_back(dsec * gain2, hat2, spread2)
        dres_s[...] = dres
        dattn = dres.astype(bf16)
        da_s[of(i), :] = dattn
        hat, spread = layer_stats(x_s[i].astype(f32))
        dn_s[...] = jnp.zeros_like(dn_s)

        def block(cb, carry):
            for at, a, steps, img in (
                ((0, 1), 0, far, 0),
                ((0, 3), 0, far, 1),
                ((1, 0), 0, far, 2),
                ((1, 3), 1, near, 0),
                ((2, 2), 1, far, 0),
                ((2, 3), 1, near, 1),
            ):

                @pl.when(jnp.logical_and(i == at[0], cb == at[1]))
                def _():
                    pump(a, steps, img)

            dheads = mm(dattn, weight(cb, 3 * cols, packed)).astype(bf16)
            qkv_c = qkv[cb, of(i), :]
            along_heads = dheads.astype(f32) * heads[cb, of(i), :].astype(f32)
            grads = [[], [], []]
            for h in range(per):
                q, kk, v = head_parts(qkv_c, h, per)
                at = slice(h * HEAD_DIM, (h + 1) * HEAD_DIM)
                dh = dheads[:, at]
                p = probs[i, cb, h]
                dp = mm(dh, v, NT) - jnp.sum(along_heads[:, at], axis=1, keepdims=True)
                dsc = (p.astype(f32) * dp).astype(bf16)
                grads[0].append((mm(dsc, kk) * 0.125).astype(bf16))
                grads[1].append(mm(dsc, q, TN).astype(bf16))
                grads[2].append(mm(p, dh, TN).astype(bf16))
            dqkv = jnp.concatenate(grads[0] + grads[1] + grads[2], axis=1)
            qkv[cb, of(i), :] = dqkv
            dn_s[...] += mm(dqkv, weight(cb, 0, 3 * cols), NT)
            return carry

        lax.fori_loop(0, ctx_n, block, 0)
        dn = dn_s[...]
        dsm[0:1, :] += jnp.sum(dn * hat, axis=0, keepdims=True)
        dsm[2:3, :] += jnp.sum(dn, axis=0, keepdims=True)
        x_s[i] = (dres_s[...] + norm_back(dn * gain1, hat, spread)).astype(bf16)
        launch(1, i)
        return carry

    sblk[plane] = jnp.zeros(sblk.shape[1:], f32)
    lax.fori_loop(0, share, backward, 0)
    outs = [pltpu.make_async_copy(x_s, dxo.at[pl.ds(c * share, share)], lsem.at[1])]
    for cp in outs:
        cp.start()
    dkeys = dsm[4 : 4 + slots_n, :]
    dsm[4 : 4 + slots_n, :] = key_scale * (dkeys - keys * jnp.sum(keys * dkeys, axis=1, keepdims=True))

    def core(cc):
        return remote(part.at[cc, :, :, 1 - k], rcv1.at[cc], ksem.at[cc], krecv.at[cc], tensor=y * 2 + 1 - k)

    normed_t = n1_s[...].T
    dattn_t = da_s[...].T
    for cc in range(ctx_n):
        from_qkv = mm(normed_t, qkv[cc]).astype(bf16)
        from_proj = mm(dattn_t, heads[cc]).astype(bf16)
        for j in range(plane):
            at = (cc, j // ten_n, (j // 2) % y_n, j % 2)
            part[at + (slice(None), slice(0, 3 * cols))] = from_qkv[j * rows : (j + 1) * rows]
            part[at + (slice(None), slice(3 * cols, packed))] = from_proj[j * rows : (j + 1) * rows]
        core(cc).start()
        if cc == ctx_n - 1:
            pump(1, far, 1)
            pump(1, near, 2)
    for j in range(plane):
        sblk[j, :, :rows] = dsm[:, j * rows : (j + 1) * rows]

    def small1(o):
        j = lax.rem(mine + o, plane)
        return remote(sblk.at[j], srcv.at[o], ss.at[o], sr.at[o], wide=j // ten_n, tensor=lax.rem(j, ten_n))

    for o in range(1, plane):
        small1(o).start()

    def hop(cc, number, o):
        on_wide = (cc % 2 == 0) == (number == 2)
        ss_, rr_ = (s2, r2) if number == 2 else (s3, r3)
        if on_wide:
            p = lax.rem(w + o, wide_n)
            to = {"wide": p}
            frm = rcv1.at[cc, p] if number == 2 else rcv1.at[cc, p, y]
            into = rcv2.at[cc, pl.ds(o * y_n, y_n)] if number == 2 else rcv3.at[cc, o]
        else:
            p = lax.rem(y + o, y_n)
            to = {"tensor": p * 2 + k}
            frm = rcv1.at[cc, :, p] if number == 2 else rcv1.at[cc, w, p]
            into = rcv2.at[cc, pl.ds(o * wide_n, wide_n)] if number == 2 else rcv3.at[cc, o]
        return remote(frm, into, ss_.at[cc, o], rr_.at[cc, o], **to)

    def peers(cc, number):
        on_wide = (cc % 2 == 0) == (number == 2)
        return range(1, wide_n if on_wide else y_n)

    for cc in range(ctx_n):
        core(cc).wait_recv()
        for wi in range(wide_n):
            for yi in range(y_n):
                rcv1[cc, wi, yi] = (part[cc, wi, yi, k].astype(f32) + rcv1[cc, wi, yi].astype(f32)).astype(bf16)
        for o in peers(cc, 2):
            hop(cc, 2, o).start()

    for o in range(1, ctx_n):
        p = lax.rem(c + ctx_n - o, ctx_n)
        trade(o, eo_all, 0, p).wait_recv()
        trade(o, comb_all, 1, p).wait_recv()

    order = [(s, i) for s in range(1, ctx_n) for i in range(share)]

    def mix_some(lo_n, hi_n):
        for j in range(lo_n, hi_n):
            step, i = order[j]
            cb = seq[step]
            slot = (j + share) % 2
            for side in (0, 1):

                @pl.when(onward(cb, side))
                def _():
                    along(0, cb, i, side, False).wait_send()

            arrived(0, step, i)
            put(step, i, slot).wait()
            for cp in fetch(step, i, slot):
                cp.start()
            for cp in fetch(step, i, slot):
                cp.wait()
            mixed = mm(comb_all[cb, i, :, :length], eo_all[cb, i], TN)
            out = x_buf[...].astype(f32) + a_buf[slot].astype(f32) + mixed
            a_buf[slot] = out.astype(bf16)
            put(step, i, slot).start()

    third = len(order) // 3
    mix_some(0, third)
    for cc in range(ctx_n):
        on_wide = cc % 2 == 0
        for o in peers(cc, 2):
            hop(cc, 2, o).wait_recv()
        for j in range(y_n if on_wide else wide_n):
            spot_j = (cc, w, j) if on_wide else (cc, j, y)
            tot = rcv1[spot_j].astype(f32)
            for o in peers(cc, 2):
                tot = tot + rcv2[cc, o * (y_n if on_wide else wide_n) + j].astype(f32)
            rcv1[spot_j] = tot.astype(bf16)
        for o in peers(cc, 3):
            hop(cc, 3, o).start()

    tot = sblk[mine]
    for o in range(1, plane):
        small1(o).wait_recv()
        tot = tot + srcv[o]
    smalls[c, : sblk.shape[1], :] = tot
    smalls[c, sblk.shape[1] :, :] = sblk[plane, :8, :]

    def small2(o, p):
        return remote(
            smalls.at[p], smalls.at[p], ss.at[plane + o], sr.at[plane + o], context=lax.rem(c + o, ctx_n)
        )

    for o in range(1, ctx_n):
        small2(o, c).start()
    pump(1, far, 2)
    mix_some(third, 2 * third)

    def last(cc):
        return remote(acc3.at[cc], rcv4.at[c], s4.at[cc], r4.at[c], context=cc)

    for cc in range(ctx_n):
        for o in peers(cc, 3):
            hop(cc, 3, o).wait_recv()
        tot = rcv1[cc, w, y].astype(f32)
        for o in peers(cc, 3):
            tot = tot + rcv3[cc, o].astype(f32)
        acc3[cc] = tot.astype(bf16)

        @pl.when(c != cc)
        def _():
            last(cc).start()

    mix_some(2 * third, len(order))
    for step, i in order:
        arrived(1, step, i)
    tot = acc3[c].astype(f32)
    for o in range(1, ctx_n):
        p = lax.rem(c + o, ctx_n)
        remote(acc3.at[0], rcv4.at[p], s4.at[p], r4.at[p], context=p).wait_recv()
        tot = tot + rcv4[p].astype(f32)
    grad[...] = tot

    for slot in (0, 1):
        put(0, 0, slot).wait()
    for j in range(4):
        expert_out(0, j).wait()
    drain(got, ten_n - 1, esem.at[2])
    drain(ret, ten_n - 1, esem.at[4])
    drain(send_s, pairs_n - 1, esem.at[6])
    for o in range(1, ctx_n):
        p = lax.rem(c + ctx_n - o, ctx_n)
        small2(o, p).wait_recv()
        small2(o, c).wait_send()
        trade(o, eo_all, 0, c).wait_send()
        trade(o, comb_all, 1, c).wait_send()
        last(lax.rem(c + o, ctx_n)).wait_send()
    for o in range(1, plane):
        small1(o).wait_send()
    for cc in range(ctx_n):
        core(cc).wait_send()
        for number in (2, 3):
            for o in peers(cc, number):
                hop(cc, number, o).wait_send()
    for cp in outs:
        cp.wait()
    if joined:
        for o in range(1, plane):
            w_small(o).wait_send()
        for cb in range(ctx_n):
            for number in (0, 1):
                for cp in w_legs(cb, number):
                    cp.wait_send()
            w_core(cb).wait_send()
            for side in (0, 1):
                go = (cb >= c, c > 0) if side == 0 else (cb <= c, c < ctx_n - 1)

                @pl.when(jnp.logical_and(*go))
                def _():
                    w_ctx(cb, side, True).wait_send()

    for a in (0, 1):
        for i in range(share):
            for side in (0, 1):

                @pl.when((c > 0) if side == 0 else (c < ctx_n - 1))
                def _():
                    along(a, c, i, side, True).wait_send()

    for step, i in order:
        for side in (0, 1):

            @pl.when(onward(seq[step], side))
            def _():
                along(1, seq[step], i, side, False).wait_send()


def run_block(x_all, g_all, pack, small, slots_n, up, down, rows, share):
    wide_n, ctx_n, ten_n = (lax.axis_size(a) for a in ("wide", "context", "tensor"))
    y_n = ten_n // 2
    plane = wide_n * ten_n
    n = plane * ctx_n
    most = max(wide_n, y_n)
    images, length, width = x_all.shape
    packed = pack.shape[-1]
    joined = pack.ndim == 2
    cols = packed // 4
    ff = up.shape[1]
    par8 = 4 + slots_n + -(4 + slots_n) % 8
    lanes = rows + -rows % 128
    blk = (rows, packed)
    acts = (share, length, width)
    wide_len = length + -length % 128
    tall = length + -length % 16
    dma = pltpu.SemaphoreType.DMA
    vm = pl.BlockSpec(memory_space=pltpu.VMEM)
    hbm = pl.BlockSpec(memory_space=pl.ANY)
    V = pltpu.VMEM
    shape = jax.ShapeDtypeStruct
    return pl.pallas_call(
        functools.partial(block_kernel, share, joined),
        out_shape=(
            shape((images, length, width), bf16),
            shape((images, length, width), bf16),
            shape(blk, f32),
            shape((ctx_n, par8 + 8, lanes), f32),
            shape((n * 8, width), bf16),
            shape((n * 8, ff), bf16),
            shape((n * 8, ff), bf16),
            shape((n * 8, width), bf16),
        ),
        in_specs=[hbm, hbm] + [vm] * 4,
        out_specs=(hbm, hbm, vm, vm) + (hbm,) * 4,
        scratch_shapes=[
            V(acts, bf16), V(acts, bf16), V(acts, bf16),
            V((share * tall, width), bf16),
            V((share * tall, width), bf16),
            V((ctx_n, share * tall, 3 * cols), bf16),
            V((ctx_n, share * tall, cols), bf16),
            V((share, ctx_n, cols // HEAD_DIM, length, length), bf16),
            V((share * tall, width), f32),
            V((share, slots_n, length), f32),
            V((share, 8, lanes), f32),
            V((length, width), f32),
            V((length, width), f32),
            V((slots_n * 8, width), f32),
            V((slots_n, 8, width), bf16),
            V((ten_n, slots_n, 8, width), bf16),
            V((min(n, 32) * 8, width), f32),
            V((4, min(n, 32) * 8, width), bf16),
            V((ten_n, slots_n, 8, width), bf16),
            V((ten_n, slots_n, 8, width), bf16),
            V((slots_n, 8, width), bf16),
            V((ctx_n, share, slots_n, width), bf16),
            V((ctx_n, share, slots_n, wide_len), bf16),
            V((par8, width), f32),
            V((plane + 1, par8, lanes), f32),
            V((ctx_n, wide_n, y_n, 2) + blk, bf16),
            V((ctx_n, wide_n, y_n) + blk, bf16),
            V((ctx_n, wide_n * y_n) + blk, bf16),
            V((ctx_n, most) + blk, bf16),
            V((ctx_n,) + blk, bf16),
            V((ctx_n,) + blk, bf16),
            V((plane, par8, lanes), f32),
            V((2, length, width), bf16),
            V((length, width), bf16),
            V((ctx_n, wide_n, y_n, 2) + blk if joined else (8, 128), bf16),
            V((small.shape[0], width) if joined else (8, 128), f32),
            V((wide_n, y_n, 2) + small.shape if joined else (8, 128), bf16),
            dma((7, ctx_n, plane) if joined else (1,)), dma((7, ctx_n, plane) if joined else (1,)),
            dma((2,)), dma((8,)), dma((4,)),
            dma((2, 2, ctx_n, share)), dma((2, ctx_n, share)),
            dma((ctx_n,)), dma((ctx_n,)),
            dma((ctx_n, most)), dma((ctx_n, most)),
            dma((ctx_n, most)), dma((ctx_n, most)),
            dma((ctx_n,)), dma((ctx_n,)),
            dma((plane + ctx_n,)), dma((plane + ctx_n,)),
            dma((2, ctx_n)), dma((2, ctx_n)),
            dma((3, 2)),
        ],
        compiler_params=pltpu.CompilerParams(
            collective_id=2, has_side_effects=True, vmem_limit_bytes=67043328
        ),
    )(x_all, g_all, pack, small, up, down)


def on_device(
    layer_input,
    qkv_weight,
    proj_weight,
    norm_gains,
    norm_biases,
    router_keys,
    up_weight,
    down_weight,
    out_cotangent,
):
    images, length, width = layer_input.shape
    wide_n, ctx_n, ten_n = (lax.axis_size(a) for a in ("wide", "context", "tensor"))
    share = images // ctx_n
    slots_n = router_keys.shape[1]
    rows, _, cols = qkv_weight.shape
    plane = wide_n * ten_n
    lanes = rows + -rows % 128

    pack = jnp.concatenate([qkv_weight.reshape(rows, 3 * cols), proj_weight.T], axis=1)
    small = jnp.concatenate([norm_gains, norm_biases, router_keys.T], axis=0)
    params = small.shape[0]
    small = jnp.pad(small, ((0, -params % 16), (0, lanes - rows)))
    if rows % 32 == 0:
        weights = pack
    else:
        weights, small = gather_weights(pack, small)
        weights = weights.reshape(ctx_n, width, 4 * cols)
        small = small.reshape((-1,) + small.shape[3:])[:, :params, :rows]
        small = small.transpose(1, 0, 2).reshape(params, width)
    layer_output, input_grad, dpack, dsmall, e_in, e_act, e_hid, e_dexp = run_block(
        layer_input, out_cotangent, weights, small, slots_n, up_weight[0], down_weight[0], rows, share
    )
    up_grad = mm(e_in, e_hid, TN)
    down_grad = mm(e_act, e_dexp, TN)
    rms = dsmall[:, dsmall.shape[1] - 8 :, :3][:, :share].reshape(images, 3)
    dsmall = jnp.sum(dsmall[:, :params, :rows], axis=0)
    return (
        layer_output,
        rms,
        input_grad,
        dpack[:, : 3 * cols].reshape(rows, 3, cols),
        dpack[:, 3 * cols :].T,
        dsmall[0:2],
        dsmall[2:4],
        dsmall[4:].T,
        up_grad[None],
        down_grad[None],
    )


def solution(mesh):
    images = P(("wide", "tensor"), None, None)
    qkv = P(("wide", "tensor"), None, "context")
    proj = P("context", ("wide", "tensor"))
    lane = P(None, ("wide", "tensor"))
    rowed = P(("wide", "tensor"), None)
    up = P(("wide", "context"), None, "tensor")
    down = P(("wide", "context"), "tensor", None)
    return jax.shard_map(
        on_device,
        mesh=mesh,
        in_specs=(images, qkv, proj, lane, lane, rowed, up, down, images),
        out_specs=(images, rowed, images, qkv, proj, lane, lane, rowed, up, down),
        check_vma=False,
    )
```

```python
import functools
import math

import jax
import jax.numpy as jnp
from jax import lax
from jax.experimental import pallas as pl
from jax.experimental.pallas import tpu as pltpu
from jax.sharding import PartitionSpec as P

f32 = jnp.float32
bf16 = jnp.bfloat16

HEAD_DIM = 64
norm_eps = 1e-06
highest = lax.Precision.HIGHEST
NN = (((1,), (0,)), ((), ()))
NT = (((1,), (1,)), ((), ()))
TN = (((0,), (0,)), ((), ()))


def mm(a, b, dims=NN, precision=None):
    return lax.dot_general(a, b, dims, precision=precision, preferred_element_type=f32)


def layer_stats(values):
    center = values - jnp.mean(values, axis=-1, keepdims=True)
    spread = lax.rsqrt(jnp.mean(center * center, axis=-1, keepdims=True) + norm_eps)
    return (center * spread, spread)


def norm_back(upstream, scaled, spread):
    return spread * (
        upstream
        - jnp.mean(upstream, axis=-1, keepdims=True)
        - scaled * jnp.mean(upstream * scaled, axis=-1, keepdims=True)
    )


def soft(values, axis):
    e = jnp.exp(values - jnp.max(values, axis=axis, keepdims=True))
    return e / jnp.sum(e, axis=axis, keepdims=True)


def pick_rows(slots_n, row):
    r = lax.broadcasted_iota(jnp.int32, (slots_n * 8, slots_n), 0)
    s = lax.broadcasted_iota(jnp.int32, (slots_n * 8, slots_n), 1)
    return jnp.where(r == s * 8 + row, 1.0, 0.0).astype(bf16)


def router_unit(keys):
    scale = lax.rsqrt(jnp.sum(keys * keys, axis=1, keepdims=True) + norm_eps)
    return keys * scale, scale


def head_parts(block, h, per):
    at = [j * per * HEAD_DIM + h * HEAD_DIM for j in range(3)]
    return [block[:, a : a + HEAD_DIM] for a in at]


def remote(src, dst, ssem, rsem, **where):
    return pltpu.make_async_remote_copy(
        src_ref=src,
        dst_ref=dst,
        send_sem=ssem,
        recv_sem=rsem,
        device_id=where,
        device_id_type=pl.DeviceIdType.MESH,
    )


def spot():
    wide_n, ctx_n, ten_n = (lax.axis_size(a) for a in ("wide", "context", "tensor"))
    w, c, t = (lax.axis_index(a) for a in ("wide", "context", "tensor"))
    return wide_n, ctx_n, ten_n // 2, w, c, t // 2, lax.rem(t, 2)


def greet_plane(bar, wide_n, y_n, w, y, k):
    for o in range(1, wide_n * y_n * 2):
        j = lax.rem((w * y_n + y) * 2 + k + o, wide_n * y_n * 2)
        pl.semaphore_signal(
            bar,
            inc=1,
            device_id={"wide": j // (y_n * 2), "tensor": lax.rem(j, y_n * 2)},
            device_id_type=pl.DeviceIdType.MESH,
        )
    return wide_n * y_n * 2 - 1


def near_first(c, ctx_n):
    seq = []
    for j in range(ctx_n):
        cb = 0
        for p in range(ctx_n):
            order = sorted(range(ctx_n), key=lambda q: (abs(q - p), q))
            cb = jnp.where(c == p, order[j], cb)
        seq.append(cb)
    return seq


def gather_kernel(pack, small, full, smalls, csem, crecv, wsem, wrecv, ysem, yrecv, ksem, krecv, ssem, srecv, local):
    wide_n, ctx_n, y_n, w, c, y, k = spot()
    bar = pltpu.get_barrier_semaphore()
    met = greet_plane(bar, wide_n, y_n, w, y, k)

    @pl.when(c > 0)
    def _():
        pl.semaphore_signal(bar, inc=1, device_id={"context": c - 1}, device_id_type=pl.DeviceIdType.MESH)

    @pl.when(c < ctx_n - 1)
    def _():
        pl.semaphore_signal(bar, inc=1, device_id={"context": c + 1}, device_id_type=pl.DeviceIdType.MESH)

    mine = pltpu.make_async_copy(pack, full.at[c, w, y, k], local.at[0])
    mine_small = pltpu.make_async_copy(small, smalls.at[w, y, k], local.at[1])
    mine.start()
    mine_small.start()
    pl.semaphore_wait(bar, met + (c + ctx_n - 1) // ctx_n + (2 * ctx_n - 2 - c) // ctx_n)

    def along(cb, side, src):
        return remote(src, full.at[cb, w, y, k], csem.at[side, cb], crecv.at[cb], context=c + 2 * side - 1)

    for side in (0, 1):

        @pl.when((c > 0) if side == 0 else (c < ctx_n - 1))
        def _():
            along(c, side, pack).start()

    def small_copy(o):
        j = lax.rem((w * y_n + y) * 2 + k + o, wide_n * y_n * 2)
        return remote(
            small, smalls.at[w, y, k], ssem.at[o], srecv.at[o], wide=j // (y_n * 2), tensor=lax.rem(j, y_n * 2)
        )

    for o in range(1, wide_n * y_n * 2):
        small_copy(o).start()

    seq = near_first(c, ctx_n)

    def leg(cb, number, o, start):
        even = lax.rem(cb, 2) == 0
        for on_wide in (True, False):
            n = wide_n if on_wide else y_n
            if o >= n:
                continue
            first = number == 0
            want_even = on_wide == first

            @pl.when(even if want_even else jnp.logical_not(even))
            def _():
                if on_wide:
                    ref = full.at[cb, w, y, k] if first else full.at[cb, w, :, k]
                    to = {"wide": lax.rem(w + o, wide_n)}
                    sems = (wsem.at[cb, o], wrecv.at[cb, o])
                else:
                    ref = full.at[cb, w, y, k] if first else full.at[cb, :, y, k]
                    to = {"tensor": lax.rem(y + o, y_n) * 2 + k}
                    sems = (ysem.at[cb, o], yrecv.at[cb, o])
                cp = remote(ref, ref, *sems, **to)
                if start == "start":
                    cp.start()
                elif start == "recv":
                    cp.wait_recv()
                else:
                    cp.wait_send()

    most = max(wide_n, y_n)

    def core(cb):
        ref = full.at[cb, :, :, k]
        return remote(ref, ref, ksem.at[cb], krecv.at[cb], tensor=y * 2 + 1 - k)

    mine.wait()
    mine_small.wait()
    for step in range(ctx_n + 2):
        if step < ctx_n:
            cb = seq[step]
            if step > 0:
                along(cb, 0, pack).wait_recv()
                for side in (0, 1):
                    go = jnp.logical_and(cb > c, c > 0) if side == 0 else jnp.logical_and(cb < c, c < ctx_n - 1)

                    @pl.when(go)
                    def _():
                        along(cb, side, full.at[cb, w, y, k]).start()

            for o in range(1, most):
                leg(cb, 0, o, "start")
        if 0 < step <= ctx_n:
            cb = seq[step - 1]
            for o in range(1, most):
                leg(cb, 0, o, "recv")
            for o in range(1, most):
                leg(cb, 1, o, "start")
        if step > 1:
            cb = seq[step - 2]
            for o in range(1, most):
                leg(cb, 1, o, "recv")
            core(cb).start()
    for step in range(ctx_n):
        core(seq[step]).wait_recv()
    for o in range(1, wide_n * y_n * 2):
        cp = small_copy(o)
        cp.wait_recv()
        cp.wait_send()
    for step in range(ctx_n):
        cb = seq[step]
        for side in (0, 1):
            go = jnp.logical_and(cb >= c, c > 0) if side == 0 else jnp.logical_and(cb <= c, c < ctx_n - 1)

            @pl.when(go)
            def _():
                along(cb, side, pack).wait_send()

        for number in (0, 1):
            for o in range(1, most):
                leg(cb, number, o, "send")
        core(cb).wait_send()


def gather_weights(pack, small):
    wide_n, ctx_n, ten_n = (lax.axis_size(a) for a in ("wide", "context", "tensor"))
    y_n = ten_n // 2
    dma = pltpu.SemaphoreType.DMA
    vm = pl.BlockSpec(memory_space=pltpu.VMEM)
    return pl.pallas_call(
        gather_kernel,
        out_shape=(
            jax.ShapeDtypeStruct((ctx_n, wide_n, y_n, 2) + pack.shape, pack.dtype),
            jax.ShapeDtypeStruct((wide_n, y_n, 2) + small.shape, small.dtype),
        ),
        in_specs=[vm, vm],
        out_specs=(vm, vm),
        scratch_shapes=[
            dma((2, ctx_n)), dma((ctx_n,)),
            dma((ctx_n, wide_n)), dma((ctx_n, wide_n)),
            dma((ctx_n, y_n)), dma((ctx_n, y_n)),
            dma((ctx_n,)), dma((ctx_n,)),
            dma((wide_n * ten_n,)), dma((wide_n * ten_n,)),
            dma((2,)),
        ],
        compiler_params=pltpu.CompilerParams(collective_id=1, has_side_effects=True),
    )(pack, small)


def gelu_parts(x):
    a = 0.7978845608028654
    x2 = x * x
    th = jnp.tanh(a * x * (1.0 + 0.044715 * x2))
    val = 0.5 * x * (1.0 + th)
    der = 0.5 * (1.0 + th) + 0.5 * x * (1.0 - th * th) * (a * (1.0 + 3 * 0.044715 * x2))
    return val, der


def halves(values):
    high = values.astype(bf16).astype(f32)
    return high, values - high


def block_kernel(share, joined, *refs):
    (
        x_all, g_all, qkv_w, proj_w, gains_w, biases_w, router_w, up, down,
        lo, dxo, grad, smalls, e_in, e_act, e_hid, e_dexp,
        x_s, g_s, att_s, n1_s, da_s, qkv, heads, probs, resid, logits, asq, dres_s, dn_s, rows_s,
        send_s, got, r32, e_s, ret, got2, back_g, eo_all, comb_all, dsm, sblk,
        part, rcv1, rcv2, rcv3, acc3, rcv4, srcv, a_buf, x_buf,
        full_s, small_s, small_g, pack_s, small_p, turn, wsem, wrecv,
        lsem, esem, xsem, gsem, grecv, ksem, krecv, s2, r2, s3, r3, s4, r4, ss, sr, es, er, obuf_sem,
    ) = refs
    wide_n, ctx_n, y_n, w, c, y, k = spot()
    ten_n = 2 * y_n
    plane = wide_n * ten_n
    n = plane * ctx_n
    me = (w * ctx_n + c) * ten_n + y * 2 + k
    mine = (w * y_n + y) * 2 + k
    width, packed = x_s.shape[2], grad.shape[1]
    pack, small_in = (pack_s, small_p) if joined else (qkv_w, proj_w)
    cols = packed // 4
    per = cols // HEAD_DIM
    slots_n = rows_s.shape[0] // 8
    length = x_s.shape[1]
    small = small_s if joined else small_in

    def weight(cb, lo_col, hi_col):
        if joined:
            return full_s[cb, :, :, :, :, lo_col:hi_col].reshape(width, hi_col - lo_col)
        return pack[cb, :, lo_col:hi_col]

    rows = grad.shape[0]
    logit_scale = 1.6 * math.sqrt(width)
    seq = near_first(c, ctx_n)
    bar = pltpu.get_barrier_semaphore()

    def place(d):
        return {"wide": d // (ctx_n * ten_n), "context": lax.rem(d // ten_n, ctx_n), "tensor": lax.rem(d, ten_n)}

    def hello(o, carry):
        pl.semaphore_signal(bar, inc=1, device_id=place(lax.rem(me + o, n)), device_id_type=pl.DeviceIdType.MESH)
        return carry

    lax.fori_loop(1, n, hello, 0)
    ins = [
        pltpu.make_async_copy(x_all.at[pl.ds(c * share, share)], x_s, lsem.at[0]),
        pltpu.make_async_copy(g_all.at[pl.ds(c * share, share)], g_s, lsem.at[1]),
    ]
    for cp in ins:
        cp.start()
    rows_s[...] = jnp.zeros_like(rows_s)
    dsm[...] = jnp.zeros_like(dsm)
    tall = length + -length % 16
    gap = tall - length // 16 * 16
    for i in range(share):
        edge = pl.ds(i * tall + tall - gap, gap)
        n1_s[edge, :] = jnp.zeros((gap, width), bf16)
        da_s[edge, :] = jnp.zeros((gap, width), bf16)
        for cb in range(ctx_n):
            heads[cb, edge, :] = jnp.zeros((gap, cols), bf16)

    def of(i):
        return pl.ds(pl.multiple_of(i * tall, 16), length)


    def along(a, cb, i, side, own):
        ref = (lo, dxo)[a].at[cb * share + i]
        src = (att_s, x_s)[a].at[i] if own else ref
        return remote(src, ref, gsem.at[a, side, cb, i], grecv.at[a, cb, i], context=c + 2 * side - 1)

    def launch(a, i):
        for side in (0, 1):

            @pl.when((c > 0) if side == 0 else (c < ctx_n - 1))
            def _():
                along(a, c, i, side, True).start()

    def onward(cb, side):
        if side == 0:
            return jnp.logical_and(cb > c, c > 0)
        return jnp.logical_and(cb < c, c < ctx_n - 1)

    def pump(a, steps, i):
        for step in steps:
            cb = seq[step]
            for side in (0, 1):

                @pl.when(onward(cb, side))
                def _():
                    along(a, cb, i, 0, False).wait_recv()
                    along(a, cb, i, side, False).start()

    def arrived(a, step, i):
        cb = seq[step]

        @pl.when(jnp.logical_not(jnp.logical_or(onward(cb, 0), onward(cb, 1))))
        def _():
            along(a, cb, i, 0, False).wait_recv()

    near, far = list(range(1, min(3, ctx_n))), list(range(3, ctx_n))

    half = rows // 2

    def w_ctx(cb, side, own):
        ref = full_s.at[cb, w, y, k]
        return remote(pack if own else ref, ref, wsem.at[0, cb, side], wrecv.at[0, cb, 0], context=c + 2 * side - 1)

    def w_leg(cb, number, h, o):
        at = pl.ds(h * half, half)
        slot = number * 2 + h
        if (number == 0) == (h == 0):
            ref = full_s.at[cb, w, y, k, at] if number == 0 else full_s.at[cb, w, :, k, at]
            to = {"wide": lax.rem(w + o, wide_n)}
        else:
            ref = full_s.at[cb, w, y, k, at] if number == 0 else full_s.at[cb, :, y, k, at]
            to = {"tensor": lax.rem(y + o, y_n) * 2 + k}
        return remote(ref, ref, wsem.at[1 + slot, cb, o], wrecv.at[1 + slot, cb, o], **to)

    def w_legs(cb, number):
        out = []
        for h in (0, 1):
            on_wide = (number == 0) == (h == 0)
            out += [w_leg(cb, number, h, o) for o in range(1, wide_n if on_wide else y_n)]
        return out

    def w_core(cb):
        ref = full_s.at[cb, :, :, k]
        return remote(ref, ref, wsem.at[5, cb, 0], wrecv.at[5, cb, 0], tensor=y * 2 + 1 - k)

    def w_small(o):
        j = lax.rem(mine + o, plane)
        to = {"wide": j // ten_n, "tensor": lax.rem(j, ten_n)}
        return remote(small_in, small_g.at[w, y, k], wsem.at[6, 0, o], wrecv.at[6, 0, o], **to)

    def w_arrive(j):
        cb = seq[j]
        if j > 0:
            w_ctx(cb, 0, False).wait_recv()
            for side in (0, 1):

                @pl.when(onward(cb, side))
                def _():
                    w_ctx(cb, side, False).start()

        for cp in w_legs(cb, 0):
            cp.start()

    def w_second(j):
        for cp in w_legs(seq[j], 0):
            cp.wait_recv()
        for cp in w_legs(seq[j], 1):
            cp.start()

    def w_third(j):
        for cp in w_legs(seq[j], 1):
            cp.wait_recv()
        w_core(seq[j]).start()

    def w_ready(j):
        if joined:
            w_core(seq[j]).wait_recv()

    if joined:
        turn[:cols, :rows] = proj_w[...].astype(f32)
        pieces = [qkv_w[j] for j in range(3)] + [turn[...].T[:rows, :cols].astype(bf16)]
        pack_s[...] = jnp.concatenate(pieces, axis=1)
        lines = jnp.concatenate([r[...].astype(f32) for r in (gains_w, biases_w, router_w)], axis=0)
        turn[: lines.shape[0], :rows] = lines
        small_p[...] = turn[: small_p.shape[0], : small_p.shape[1]].astype(bf16)
        full_s[c, w, y, k] = pack[...]
        small_g[w, y, k] = small_in[...]
    pl.semaphore_wait(bar, n - 1)
    if joined:
        for side in (0, 1):

            @pl.when((c > 0) if side == 0 else (c < ctx_n - 1))
            def _():
                w_ctx(c, side, True).start()

        w_arrive(0)
        for o in range(1, plane):
            w_small(o).start()
        for o in range(1, plane):
            w_small(o).wait_recv()
        pieces = [small_g[j // ten_n, (j // 2) % y_n, j % 2][:, :rows] for j in range(plane)]
        small_s[...] = jnp.concatenate([p.astype(f32) for p in pieces], axis=1)
    keys, key_scale = router_unit(small[4 : 4 + slots_n, :].astype(f32))
    keys_hi, keys_lo = halves(keys)
    keys_two = jnp.concatenate([keys_hi, keys_lo], axis=0).astype(bf16)
    keys_three = jnp.concatenate([keys_hi, keys_lo, keys_hi], axis=0).astype(bf16)
    for cp in ins:
        cp.wait()

    def norm_first(i, carry):
        hat, _ = layer_stats(x_s[i].astype(f32))
        n1_s[of(i), :] = (hat * small[0:1, :].astype(f32) + small[2:3, :].astype(f32)).astype(bf16)
        return carry

    lax.fori_loop(0, share, norm_first, 0)

    def between(j, i):
        todo = {}
        if joined:
            todo = {
                (0, 0): lambda: w_third(1),
                (0, 1): lambda: w_second(2),
                (0, 2): lambda: w_arrive(3),
                (1, 0): lambda: w_third(2),
                (1, 1): lambda: w_second(3),
                (2, 0): lambda: w_third(3),
            }
        return todo.get((j, i))

    if joined:
        w_second(0)
        w_arrive(1)
        w_third(0)
        w_second(1)
        w_arrive(2)
    for j in range(ctx_n):
        w_ready(j)
        cb = seq[j]
        qkv_f = mm(n1_s[...], weight(cb, 0, 3 * cols))
        qkv[cb] = jnp.concatenate([qkv_f[:, :cols] * 0.125, qkv_f[:, cols:]], axis=1).astype(bf16)

        def attend(i, carry):
            for at in range(share):
                if between(j, at) is not None:
                    pl.when(i == at)(between(j, at))
            qkv_c = qkv[cb, of(i), :]
            mixed = []
            for h in range(per):
                q, kk, v = head_parts(qkv_c, h, per)
                s = mm(q, kk, NT)
                e = jnp.exp(s - jnp.max(s, axis=1, keepdims=True))
                p = (e * (1.0 / jnp.sum(e, axis=1, keepdims=True))).astype(bf16)
                probs[i, cb, h] = p
                mixed.append(mm(p, v).astype(bf16))
            heads[cb, of(i), :] = jnp.concatenate(mixed, axis=1)
            return carry

        lax.fori_loop(0, share, attend, 0)
        add = mm(heads[cb], weight(cb, 3 * cols, packed), NT)
        if j == 0:
            resid[...] = add
        else:
            resid[...] += add

    def attention_out(i, carry):
        att_s[i] = resid[of(i), :].astype(bf16)
        return carry

    lax.fori_loop(0, share, attention_out, 0)

    def route(i, carry):
        att = resid[of(i), :]
        asq[i] = jnp.full(asq.shape[1:], jnp.sum(att * att), f32)
        res = x_s[i].astype(f32) + att
        resid[of(i), :] = res
        hat2, _ = layer_stats(res)
        second = hat2 * small[1:2, :].astype(f32) + small[3:4, :].astype(f32)
        unit = second * lax.rsqrt(jnp.sum(second * second, axis=-1, keepdims=True) + norm_eps)
        unit_hi, unit_lo = halves(unit)
        lg = mm(keys_two, unit_hi.astype(bf16), NT)
        lg = lg[:slots_n] + lg[slots_n:] + mm(keys_two[:slots_n], unit_lo.astype(bf16), NT)
        lg = logit_scale * lg
        logits[i] = lg
        disp = soft(lg, 1).astype(bf16)
        comb = soft(lg, 0).astype(bf16)
        comb_all[c, i, :, :length] = comb
        slots = mm(disp, second.astype(bf16)).astype(bf16)
        dexp = mm(comb, g_s[i]).astype(bf16)
        rows_s[...] += mm(pick_rows(slots_n, i), slots) + mm(pick_rows(slots_n, i + 4), dexp)
        return carry

    lax.fori_loop(0, share, route, 0)

    for e in range(slots_n):
        send_s[e] = rows_s[e * 8 : e * 8 + 8, :].astype(bf16)
    spot_e = w * ctx_n + c
    spot_t = y * 2 + k
    pairs_n = wide_n * ctx_n

    def expert_at(o):
        p = lax.rem(spot_e + o, pairs_n)
        return p, {"wide": p // ctx_n, "context": lax.rem(p, ctx_n)}

    def drain(ref, count, sem):
        some = ref.at[pl.ds(0, count)]
        pltpu.make_async_copy(some, some, sem).wait()

    for o in range(1, pairs_n):
        p, to = expert_at(o)
        remote(send_s.at[p], got.at[spot_t, spot_e], esem.at[0], esem.at[1], **to).start()
    got[spot_t, spot_e] = send_s[spot_e]
    for i in range(share):
        launch(0, i)
    drain(got.at[spot_t], pairs_n - 1, esem.at[1])
    for o in range(1, ten_n):
        mine_in = got.at[spot_t]
        remote(mine_in, mine_in, esem.at[2], esem.at[3], tensor=lax.rem(spot_t + o, ten_n)).start()
    drain(got, ten_n - 1, esem.at[3])

    group = min(n, 32)
    chunk = group * 8
    first = lax.rem(lax.broadcasted_iota(jnp.int32, (chunk, 1), 0), 8) < 4

    def expert_out(b, j):
        dst = (e_in, e_act, e_hid, e_dexp)[j]
        at = pl.ds(pl.multiple_of(b * chunk, chunk), chunk)
        return pltpu.make_async_copy(e_s.at[j], dst.at[at, :], xsem.at[j])

    def experts(b, carry):
        def widen(j, carry):
            r32[pl.ds(pl.multiple_of(j * 8, 8), 8), :] = got[(b * group + j) // pairs_n, lax.rem(b * group + j, pairs_n)].astype(f32)
            return carry

        lax.fori_loop(0, group, widen, 0)

        @pl.when(b > 0)
        def _():
            for j in range(4):
                expert_out(b, j).wait()

        low = r32[...].astype(bf16)
        e_s[0] = low
        e_s[3] = pltpu.roll(r32[...], chunk - 4, 0).astype(bf16)
        hidden = mm(low, up[...])
        act_g = pltpu.roll(mm(low, down[...], NT), chunk - 4, 0)
        val, der = gelu_parts(hidden)
        active = jnp.where(first, val, 0.0).astype(bf16)
        hid_g = jnp.where(first, act_g * der, 0.0).astype(bf16)
        e_s[1] = active
        e_s[2] = hid_g
        part_o = mm(active, down[...])
        part_s = mm(hid_g, up[...], NT)
        r32[...] = jnp.where(first, part_o, pltpu.roll(part_s, 4, 0))
        for j in range(4):
            expert_out(b, j).start()

        def narrow(j, carry):
            ret[(b * group + j) // pairs_n, lax.rem(b * group + j, pairs_n)] = r32[pl.ds(pl.multiple_of(j * 8, 8), 8), :].astype(bf16)
            return carry

        lax.fori_loop(0, group, narrow, 0)
        return carry

    lax.fori_loop(0, n // group, experts, 0)

    for o in range(1, ten_n):
        p = lax.rem(spot_t + o, ten_n)
        remote(ret.at[p], got2.at[spot_t], esem.at[4], esem.at[5], tensor=p).start()
    got2[spot_t] = ret[spot_t]
    drain(got2, ten_n - 1, esem.at[5])
    drain(send_s, pairs_n - 1, esem.at[0])

    def total(e, carry):
        s = got2[0, e].astype(f32)
        for t in range(1, ten_n):
            s = s + got2[t, e].astype(f32)
        send_s[e] = s.astype(bf16)
        return carry

    lax.fori_loop(0, pairs_n, total, 0)
    for o in range(1, pairs_n):
        p, to = expert_at(o)
        remote(send_s.at[p], back_g.at[spot_e], esem.at[6], esem.at[7], **to).start()
    back_g[spot_e] = send_s[spot_e]
    for i in range(share):
        pump(0, near, i)
    drain(back_g, pairs_n - 1, esem.at[7])

    def spread(e, carry):
        rows_s[pl.ds(pl.multiple_of(e * 8, 8), 8), :] = back_g[e].astype(f32)
        return carry

    lax.fori_loop(0, slots_n, spread, 0)
    back = rows_s[...].astype(bf16)
    for i in range(share):
        eo_all[c, i] = mm(pick_rows(slots_n, i), back, TN).astype(bf16)

    def trade(o, ref, j, p):
        return remote(ref.at[p], ref.at[p], es.at[j, o], er.at[j, o], context=lax.rem(c + o, ctx_n))

    for o in range(1, ctx_n):
        trade(o, eo_all, 0, c).start()
        trade(o, comb_all, 1, c).start()

    def fetch(step, i, slot):
        img = seq[step] * share + i
        return (
            pltpu.make_async_copy(lo.at[img], a_buf.at[slot], obuf_sem.at[0, slot]),
            pltpu.make_async_copy(x_all.at[img], x_buf, obuf_sem.at[1, slot]),
        )

    def put(step, i, slot):
        img = seq[step] * share + i
        return pltpu.make_async_copy(a_buf.at[slot], lo.at[img], obuf_sem.at[2, slot])

    def backward(i, carry):
        gain1, gain2 = small[0:1, :].astype(f32), small[1:2, :].astype(f32)
        g_low = g_s[i]
        res = resid[of(i), :]
        hat2, spread2 = layer_stats(res)
        second = hat2 * gain2 + small[3:4, :].astype(f32)
        tokens = second.astype(bf16)
        row_scale = lax.rsqrt(jnp.sum(second * second, axis=-1, keepdims=True) + norm_eps)
        unit = second * row_scale
        eo = eo_all[c, i]
        ds = mm(pick_rows(slots_n, i + 4), rows_s[...].astype(bf16), TN).astype(bf16)
        lg = logits[i]
        disp = soft(lg, 1)
        comb = soft(lg, 0)
        mixture = mm(comb.astype(bf16), eo, TN)
        result = res + mixture

        @pl.when(i > 1)
        def _():
            put(0, 0, 0).wait()

        a_buf[lax.rem(i, 2)] = result.astype(bf16)
        put(0, i, lax.rem(i, 2)).start()
        count = 1.0 / (length * width)
        lane = lax.broadcasted_iota(jnp.int32, (8, smalls.shape[2]), 1)
        sums = jnp.where(
            lane == 0,
            jnp.sum(result * result),
            jnp.where(lane == 1, asq[i], jnp.sum(mixture * mixture)),
        )
        at_row = lax.broadcasted_iota(jnp.int32, (8, smalls.shape[2]), 0)
        sblk[plane, :8, :] = jnp.where(at_row == i, jnp.sqrt(sums * count), sblk[plane, :8, :])
        dcomb = mm(eo, g_low, NT)
        ddisp = mm(ds, tokens, NT)
        dtok = mm(disp.astype(bf16), ds, TN)
        dlg = comb * (dcomb - jnp.sum(comb * dcomb, axis=0, keepdims=True)) + disp * (
            ddisp - jnp.sum(disp * ddisp, axis=1, keepdims=True)
        )
        dlg_hi, dlg_lo = halves(dlg)
        dlg_two = jnp.concatenate([dlg_hi, dlg_lo], axis=0).astype(bf16)
        dlg_three = jnp.concatenate([dlg_hi, dlg_hi, dlg_lo], axis=0).astype(bf16)
        dunit = logit_scale * mm(dlg_three, keys_three, TN)
        unit_hi, unit_lo = halves(unit)
        dk_part = mm(dlg_two, unit_hi.astype(bf16))
        dk_part = dk_part[:slots_n] + dk_part[slots_n:] + mm(dlg_two[:slots_n], unit_lo.astype(bf16))
        dsm[4 : 4 + slots_n, :] += logit_scale * dk_part
        dsec = dtok + row_scale * (dunit - unit * jnp.sum(unit * dunit, axis=-1, keepdims=True))
        dsm[1:2, :] += jnp.sum(dsec * hat2, axis=0, keepdims=True)
        dsm[3:4, :] += jnp.sum(dsec, axis=0, keepdims=True)
        dres = g_low.astype(f32) + norm_back(dsec * gain2, hat2, spread2)
        dres_s[...] = dres
        dattn = dres.astype(bf16)
        da_s[of(i), :] = dattn
        hat, spread = layer_stats(x_s[i].astype(f32))
        dn_s[...] = jnp.zeros_like(dn_s)

        def block(cb, carry):
            for at, a, steps, img in (
                ((0, 1), 0, far, 0),
                ((0, 3), 0, far, 1),
                ((1, 0), 0, far, 2),
                ((1, 3), 1, near, 0),
                ((2, 2), 1, far, 0),
                ((2, 3), 1, near, 1),
            ):

                @pl.when(jnp.logical_and(i == at[0], cb == at[1]))
                def _():
                    pump(a, steps, img)

            dheads = mm(dattn, weight(cb, 3 * cols, packed)).astype(bf16)
            qkv_c = qkv[cb, of(i), :]
            along_heads = dheads.astype(f32) * heads[cb, of(i), :].astype(f32)
            grads = [[], [], []]
            for h in range(per):
                q, kk, v = head_parts(qkv_c, h, per)
                at = slice(h * HEAD_DIM, (h + 1) * HEAD_DIM)
                dh = dheads[:, at]
                p = probs[i, cb, h]
                dp = mm(dh, v, NT) - jnp.sum(along_heads[:, at], axis=1, keepdims=True)
                dsc = (p.astype(f32) * dp).astype(bf16)
                grads[0].append((mm(dsc, kk) * 0.125).astype(bf16))
                grads[1].append(mm(dsc, q, TN).astype(bf16))
                grads[2].append(mm(p, dh, TN).astype(bf16))
            dqkv = jnp.concatenate(grads[0] + grads[1] + grads[2], axis=1)
            qkv[cb, of(i), :] = dqkv
            dn_s[...] += mm(dqkv, weight(cb, 0, 3 * cols), NT)
            return carry

        lax.fori_loop(0, ctx_n, block, 0)
        dn = dn_s[...]
        dsm[0:1, :] += jnp.sum(dn * hat, axis=0, keepdims=True)
        dsm[2:3, :] += jnp.sum(dn, axis=0, keepdims=True)
        x_s[i] = (dres_s[...] + norm_back(dn * gain1, hat, spread)).astype(bf16)
        launch(1, i)
        return carry

    sblk[plane] = jnp.zeros(sblk.shape[1:], f32)
    lax.fori_loop(0, share, backward, 0)
    outs = [pltpu.make_async_copy(x_s, dxo.at[pl.ds(c * share, share)], lsem.at[1])]
    for cp in outs:
        cp.start()
    dkeys = dsm[4 : 4 + slots_n, :]
    dsm[4 : 4 + slots_n, :] = key_scale * (dkeys - keys * jnp.sum(keys * dkeys, axis=1, keepdims=True))

    def core(cc):
        return remote(part.at[cc, :, :, 1 - k], rcv1.at[cc], ksem.at[cc], krecv.at[cc], tensor=y * 2 + 1 - k)

    normed_t = n1_s[...].T
    dattn_t = da_s[...].T
    for cc in range(ctx_n):
        from_qkv = mm(normed_t, qkv[cc]).astype(bf16)
        from_proj = mm(dattn_t, heads[cc]).astype(bf16)
        for j in range(plane):
            at = (cc, j // ten_n, (j // 2) % y_n, j % 2)
            part[at + (slice(None), slice(0, 3 * cols))] = from_qkv[j * rows : (j + 1) * rows]
            part[at + (slice(None), slice(3 * cols, packed))] = from_proj[j * rows : (j + 1) * rows]
        core(cc).start()
        if cc == ctx_n - 1:
            pump(1, far, 1)
            pump(1, near, 2)
    for j in range(plane):
        sblk[j, :, :rows] = dsm[:, j * rows : (j + 1) * rows]

    def small1(o):
        j = lax.rem(mine + o, plane)
        return remote(sblk.at[j], srcv.at[o], ss.at[o], sr.at[o], wide=j // ten_n, tensor=lax.rem(j, ten_n))

    for o in range(1, plane):
        small1(o).start()

    def hop(cc, number, o):
        on_wide = (cc % 2 == 0) == (number == 2)
        ss_, rr_ = (s2, r2) if number == 2 else (s3, r3)
        if on_wide:
            p = lax.rem(w + o, wide_n)
            to = {"wide": p}
            frm = rcv1.at[cc, p] if number == 2 else rcv1.at[cc, p, y]
            into = rcv2.at[cc, pl.ds(o * y_n, y_n)] if number == 2 else rcv3.at[cc, o]
        else:
            p = lax.rem(y + o, y_n)
            to = {"tensor": p * 2 + k}
            frm = rcv1.at[cc, :, p] if number == 2 else rcv1.at[cc, w, p]
            into = rcv2.at[cc, pl.ds(o * wide_n, wide_n)] if number == 2 else rcv3.at[cc, o]
        return remote(frm, into, ss_.at[cc, o], rr_.at[cc, o], **to)

    def peers(cc, number):
        on_wide = (cc % 2 == 0) == (number == 2)
        return range(1, wide_n if on_wide else y_n)

    for cc in range(ctx_n):
        core(cc).wait_recv()
        for wi in range(wide_n):
            for yi in range(y_n):
                rcv1[cc, wi, yi] = (part[cc, wi, yi, k].astype(f32) + rcv1[cc, wi, yi].astype(f32)).astype(bf16)
        for o in peers(cc, 2):
            hop(cc, 2, o).start()

    for o in range(1, ctx_n):
        p = lax.rem(c + ctx_n - o, ctx_n)
        trade(o, eo_all, 0, p).wait_recv()
        trade(o, comb_all, 1, p).wait_recv()

    order = [(s, i) for s in range(1, ctx_n) for i in range(share)]

    def mix_some(lo_n, hi_n):
        for j in range(lo_n, hi_n):
            step, i = order[j]
            cb = seq[step]
            slot = (j + share) % 2
            for side in (0, 1):

                @pl.when(onward(cb, side))
                def _():
                    along(0, cb, i, side, False).wait_send()

            arrived(0, step, i)
            put(step, i, slot).wait()
            for cp in fetch(step, i, slot):
                cp.start()
            for cp in fetch(step, i, slot):
                cp.wait()
            mixed = mm(comb_all[cb, i, :, :length], eo_all[cb, i], TN)
            out = x_buf[...].astype(f32) + a_buf[slot].astype(f32) + mixed
            a_buf[slot] = out.astype(bf16)
            put(step, i, slot).start()

    third = len(order) // 3
    mix_some(0, third)
    for cc in range(ctx_n):
        on_wide = cc % 2 == 0
        for o in peers(cc, 2):
            hop(cc, 2, o).wait_recv()
        for j in range(y_n if on_wide else wide_n):
            spot_j = (cc, w, j) if on_wide else (cc, j, y)
            tot = rcv1[spot_j].astype(f32)
            for o in peers(cc, 2):
                tot = tot + rcv2[cc, o * (y_n if on_wide else wide_n) + j].astype(f32)
            rcv1[spot_j] = tot.astype(bf16)
        for o in peers(cc, 3):
            hop(cc, 3, o).start()

    tot = sblk[mine]
    for o in range(1, plane):
        small1(o).wait_recv()
        tot = tot + srcv[o]
    smalls[c, : sblk.shape[1], :] = tot
    smalls[c, sblk.shape[1] :, :] = sblk[plane, :8, :]

    def small2(o, p):
        return remote(
            smalls.at[p], smalls.at[p], ss.at[plane + o], sr.at[plane + o], context=lax.rem(c + o, ctx_n)
        )

    for o in range(1, ctx_n):
        small2(o, c).start()
    pump(1, far, 2)
    mix_some(third, 2 * third)

    def last(cc):
        return remote(acc3.at[cc], rcv4.at[c], s4.at[cc], r4.at[c], context=cc)

    for cc in range(ctx_n):
        for o in peers(cc, 3):
            hop(cc, 3, o).wait_recv()
        tot = rcv1[cc, w, y].astype(f32)
        for o in peers(cc, 3):
            tot = tot + rcv3[cc, o].astype(f32)
        acc3[cc] = tot.astype(bf16)

        @pl.when(c != cc)
        def _():
            last(cc).start()

    mix_some(2 * third, len(order))
    for step, i in order:
        arrived(1, step, i)
    tot = acc3[c].astype(f32)
    for o in range(1, ctx_n):
        p = lax.rem(c + o, ctx_n)
        remote(acc3.at[0], rcv4.at[p], s4.at[p], r4.at[p], context=p).wait_recv()
        tot = tot + rcv4[p].astype(f32)
    grad[...] = tot

    for slot in (0, 1):
        put(0, 0, slot).wait()
    for j in range(4):
        expert_out(0, j).wait()
    drain(got, ten_n - 1, esem.at[2])
    drain(ret, ten_n - 1, esem.at[4])
    drain(send_s, pairs_n - 1, esem.at[6])
    for o in range(1, ctx_n):
        p = lax.rem(c + ctx_n - o, ctx_n)
        small2(o, p).wait_recv()
        small2(o, c).wait_send()
        trade(o, eo_all, 0, c).wait_send()
        trade(o, comb_all, 1, c).wait_send()
        last(lax.rem(c + o, ctx_n)).wait_send()
    for o in range(1, plane):
        small1(o).wait_send()
    for cc in range(ctx_n):
        core(cc).wait_send()
        for number in (2, 3):
            for o in peers(cc, number):
                hop(cc, number, o).wait_send()
    for cp in outs:
        cp.wait()
    if joined:
        for o in range(1, plane):
            w_small(o).wait_send()
        for cb in range(ctx_n):
            for number in (0, 1):
                for cp in w_legs(cb, number):
                    cp.wait_send()
            w_core(cb).wait_send()
            for side in (0, 1):
                go = (cb >= c, c > 0) if side == 0 else (cb <= c, c < ctx_n - 1)

                @pl.when(jnp.logical_and(*go))
                def _():
                    w_ctx(cb, side, True).wait_send()

    for a in (0, 1):
        for i in range(share):
            for side in (0, 1):

                @pl.when((c > 0) if side == 0 else (c < ctx_n - 1))
                def _():
                    along(a, c, i, side, True).wait_send()

    for step, i in order:
        for side in (0, 1):

            @pl.when(onward(seq[step], side))
            def _():
                along(1, seq[step], i, side, False).wait_send()


def run_block(x_all, g_all, given, slots_n, up, down, rows, share):
    wide_n, ctx_n, ten_n = (lax.axis_size(a) for a in ("wide", "context", "tensor"))
    y_n = ten_n // 2
    plane = wide_n * ten_n
    n = plane * ctx_n
    most = max(wide_n, y_n)
    images, length, width = x_all.shape
    packed = 4 * (width // ctx_n)
    joined = len(given) == 5
    small_rows = 4 + slots_n + -(4 + slots_n) % 16
    if not joined:
        given = tuple(given) + (given[1],) * 3
    up8 = lambda v, m: v + -v % m
    cols = packed // 4
    ff = up.shape[1]
    par8 = 4 + slots_n + -(4 + slots_n) % 8
    lanes = rows + -rows % 128
    blk = (rows, packed)
    acts = (share, length, width)
    wide_len = length + -length % 128
    tall = length + -length % 16
    dma = pltpu.SemaphoreType.DMA
    vm = pl.BlockSpec(memory_space=pltpu.VMEM)
    hbm = pl.BlockSpec(memory_space=pl.ANY)
    V = pltpu.VMEM
    shape = jax.ShapeDtypeStruct
    return pl.pallas_call(
        functools.partial(block_kernel, share, joined),
        out_shape=(
            shape((images, length, width), bf16),
            shape((images, length, width), bf16),
            shape(blk, f32),
            shape((ctx_n, par8 + 8, lanes), f32),
            shape((n * 8, width), bf16),
            shape((n * 8, ff), bf16),
            shape((n * 8, ff), bf16),
            shape((n * 8, width), bf16),
        ),
        in_specs=[hbm, hbm] + [vm] * 2 + [vm if joined else hbm] * 3 + [vm] * 2,
        out_specs=(hbm, hbm, vm, vm) + (hbm,) * 4,
        scratch_shapes=[
            V(acts, bf16), V(acts, bf16), V(acts, bf16),
            V((share * tall, width), bf16),
            V((share * tall, width), bf16),
            V((ctx_n, share * tall, 3 * cols), bf16),
            V((ctx_n, share * tall, cols), bf16),
            V((share, ctx_n, cols // HEAD_DIM, length, length), bf16),
            V((share * tall, width), f32),
            V((share, slots_n, length), f32),
            V((share, 8, lanes), f32),
            V((length, width), f32),
            V((length, width), f32),
            V((slots_n * 8, width), f32),
            V((slots_n, 8, width), bf16),
            V((ten_n, slots_n, 8, width), bf16),
            V((min(n, 32) * 8, width), f32),
            V((4, min(n, 32) * 8, width), bf16),
            V((ten_n, slots_n, 8, width), bf16),
            V((ten_n, slots_n, 8, width), bf16),
            V((slots_n, 8, width), bf16),
            V((ctx_n, share, slots_n, width), bf16),
            V((ctx_n, share, slots_n, wide_len), bf16),
            V((par8, width), f32),
            V((plane + 1, par8, lanes), f32),
            V((ctx_n, wide_n, y_n, 2) + blk, bf16),
            V((ctx_n, wide_n, y_n) + blk, bf16),
            V((ctx_n, wide_n * y_n) + blk, bf16),
            V((ctx_n, most) + blk, bf16),
            V((ctx_n,) + blk, bf16),
            V((ctx_n,) + blk, bf16),
            V((plane, par8, lanes), f32),
            V((2, length, width), bf16),
            V((length, width), bf16),
            V((ctx_n, wide_n, y_n, 2) + blk if joined else (8, 128), bf16),
            V((small_rows, width) if joined else (8, 128), f32),
            V((wide_n, y_n, 2, small_rows, lanes) if joined else (8, 128), bf16),
            V(blk if joined else (8, 128), bf16),
            V((small_rows, lanes) if joined else (8, 128), bf16),
            V((up8(cols, 128), up8(rows, 128)) if joined else (8, 128), f32),
            dma((7, ctx_n, plane) if joined else (1,)), dma((7, ctx_n, plane) if joined else (1,)),
            dma((2,)), dma((8,)), dma((4,)),
            dma((2, 2, ctx_n, share)), dma((2, ctx_n, share)),
            dma((ctx_n,)), dma((ctx_n,)),
            dma((ctx_n, most)), dma((ctx_n, most)),
            dma((ctx_n, most)), dma((ctx_n, most)),
            dma((ctx_n,)), dma((ctx_n,)),
            dma((plane + ctx_n,)), dma((plane + ctx_n,)),
            dma((2, ctx_n)), dma((2, ctx_n)),
            dma((3, 2)),
        ],
        compiler_params=pltpu.CompilerParams(
            collective_id=2, has_side_effects=True, vmem_limit_bytes=67043328
        ),
    )(x_all, g_all, *given, up, down)


def last_kernel(share, params, *refs):
    (
        lo_in, dx_in, e_in, e_act, e_hid, e_dexp, grad, smalls,
        lo, dx, up_grad, down_grad, qkv_grad, proj_grad, gains, biases, router, rms,
        hold, turn, lines, isem, osem, usem,
    ) = refs
    groups = lo_in.shape[0] // share
    moves = [(a, b) for b in range(groups) for a in (0, 1)]

    def take(a, b):
        at = pl.ds(b * share, share)
        return pltpu.make_async_copy((lo_in, dx_in)[a].at[at], hold.at[a, at], isem.at[a, b])

    def give(a, b):
        at = pl.ds(b * share, share)
        return pltpu.make_async_copy(hold.at[a, at], (lo, dx)[a].at[at], osem.at[a, b])

    for m in moves:
        take(*m).start()
    up_grad[...] = mm(e_in[...], e_hid[...], TN)
    for m in moves[: len(moves) // 2]:
        take(*m).wait()
        give(*m).start()
    down_grad[...] = mm(e_act[...], e_dexp[...], TN)
    for m in moves[len(moves) // 2 :]:
        take(*m).wait()
        give(*m).start()
    rows, packed = grad.shape
    cols = packed // 4
    for j in range(3):
        qkv_grad[j] = grad[:, j * cols : (j + 1) * cols]
    turn[:rows, :cols] = grad[:, 3 * cols :]
    proj_grad[...] = turn[...].T[:cols, :rows]
    total = smalls[0]
    for b in range(1, groups):
        total = total + smalls[b]
    gains[...] = total[0:2, :rows]
    biases[...] = total[2:4, :rows]
    router[...] = total[4:params, :rows]
    mark = smalls.shape[1] - 8
    for b in range(groups):
        lines[b * share : (b + 1) * share, :] = smalls[b, mark : mark + share, :]
    rms[...] = lines[...].T[:3, : groups * share]
    for m in moves:
        give(*m).wait()


def run_last(lo, dx, e_in, e_act, e_hid, e_dexp, grad, smalls, share, params):
    rows, packed = grad.shape
    cols = packed // 4
    width, ff = e_in.shape[1], e_act.shape[1]
    images = lo.shape[0]
    groups = images // share
    vm = pl.BlockSpec(memory_space=pltpu.VMEM)
    hbm = pl.BlockSpec(memory_space=pl.ANY)
    shape = jax.ShapeDtypeStruct
    V = pltpu.VMEM
    up8 = lambda v, m: v + -v % m
    dma = pltpu.SemaphoreType.DMA
    return pl.pallas_call(
        functools.partial(last_kernel, share, params),
        out_shape=(
            shape(lo.shape, bf16), shape(dx.shape, bf16),
            shape((width, ff), f32), shape((ff, width), f32),
            shape((3, rows, cols), f32), shape((cols, rows), f32),
            shape((2, rows), f32), shape((2, rows), f32), shape((params - 4, rows), f32),
            shape((3, images), f32),
        ),
        in_specs=[hbm, hbm] + [vm] * 6,
        out_specs=(hbm, hbm) + (vm,) * 8,
        scratch_shapes=[
            V((2,) + lo.shape, bf16),
            V((up8(rows, 128), up8(cols, 128)), f32),
            V((128, 128), f32),
            dma((2, groups)), dma((2, groups)), dma((2,)),
        ],
    )(lo, dx, e_in, e_act, e_hid, e_dexp, grad, smalls)


def on_device(
    layer_input,
    qkv_weight,
    proj_weight,
    norm_gains,
    norm_biases,
    router_keys,
    up_weight,
    down_weight,
    out_cotangent,
):
    images, length, width = layer_input.shape
    wide_n, ctx_n, ten_n = (lax.axis_size(a) for a in ("wide", "context", "tensor"))
    share = images // ctx_n
    slots_n = router_keys.shape[1]
    rows, _, cols = qkv_weight.shape
    lanes = rows + -rows % 128

    params = 4 + slots_n
    if rows % 32 == 0:
        given = (qkv_weight.transpose(1, 0, 2), proj_weight, norm_gains, norm_biases, router_keys.T)
    else:
        pack = jnp.concatenate([qkv_weight.reshape(rows, 3 * cols), proj_weight.T], axis=1)
        small = jnp.concatenate([norm_gains, norm_biases, router_keys.T], axis=0)
        small = jnp.pad(small, ((0, -params % 16), (0, lanes - rows)))
        weights, small = gather_weights(pack, small)
        weights = weights.reshape(ctx_n, width, 4 * cols)
        small = small.reshape((-1,) + small.shape[3:])[:, :params, :rows]
        small = small.transpose(1, 0, 2).reshape(params, width)
        given = (weights, small)
    lo, dx, dpack, dsmall, *sides = run_block(
        layer_input, out_cotangent, given, slots_n, up_weight[0], down_weight[0], rows, share
    )
    lo, dx, up_grad, down_grad, qkv_grad, proj_grad, gains, biases, router, rms = run_last(
        lo, dx, *sides, dpack, dsmall, share, params
    )
    return (
        lo,
        rms.T,
        dx,
        qkv_grad.transpose(1, 0, 2),
        proj_grad,
        gains,
        biases,
        router.T,
        up_grad[None],
        down_grad[None],
    )


def solution(mesh):
    images = P(("wide", "tensor"), None, None)
    qkv = P(("wide", "tensor"), None, "context")
    proj = P("context", ("wide", "tensor"))
    lane = P(None, ("wide", "tensor"))
    rowed = P(("wide", "tensor"), None)
    up = P(("wide", "context"), None, "tensor")
    down = P(("wide", "context"), "tensor", None)
    return jax.shard_map(
        on_device,
        mesh=mesh,
        in_specs=(images, qkv, proj, lane, lane, rowed, up, down, images),
        out_specs=(images, rowed, images, qkv, proj, lane, lane, rowed, up, down),
        check_vma=False,
    )
```

```python
import functools
import math

import jax
import jax.numpy as jnp
from jax import lax
from jax.experimental import pallas as pl
from jax.experimental.pallas import tpu as pltpu
from jax.sharding import PartitionSpec as P

f32 = jnp.float32
bf16 = jnp.bfloat16

HEAD_DIM = 64
norm_eps = 1e-06
highest = lax.Precision.HIGHEST
NN = (((1,), (0,)), ((), ()))
NT = (((1,), (1,)), ((), ()))
TN = (((0,), (0,)), ((), ()))


def mm(a, b, dims=NN, precision=None):
    return lax.dot_general(a, b, dims, precision=precision, preferred_element_type=f32)


def layer_stats(values):
    center = values - jnp.mean(values, axis=-1, keepdims=True)
    spread = lax.rsqrt(jnp.mean(center * center, axis=-1, keepdims=True) + norm_eps)
    return (center * spread, spread)


def norm_back(upstream, scaled, spread):
    return spread * (
        upstream
        - jnp.mean(upstream, axis=-1, keepdims=True)
        - scaled * jnp.mean(upstream * scaled, axis=-1, keepdims=True)
    )


def soft(values, axis):
    e = jnp.exp(values - jnp.max(values, axis=axis, keepdims=True))
    return e / jnp.sum(e, axis=axis, keepdims=True)


def pick_rows(slots_n, row):
    r = lax.broadcasted_iota(jnp.int32, (slots_n * 8, slots_n), 0)
    s = lax.broadcasted_iota(jnp.int32, (slots_n * 8, slots_n), 1)
    return jnp.where(r == s * 8 + row, 1.0, 0.0).astype(bf16)


def router_unit(keys):
    scale = lax.rsqrt(jnp.sum(keys * keys, axis=1, keepdims=True) + norm_eps)
    return keys * scale, scale


def head_parts(block, h, per):
    at = [j * per * HEAD_DIM + h * HEAD_DIM for j in range(3)]
    return [block[:, a : a + HEAD_DIM] for a in at]


def remote(src, dst, ssem, rsem, **where):
    return pltpu.make_async_remote_copy(
        src_ref=src,
        dst_ref=dst,
        send_sem=ssem,
        recv_sem=rsem,
        device_id=where,
        device_id_type=pl.DeviceIdType.MESH,
    )


def spot():
    wide_n, ctx_n, ten_n = (lax.axis_size(a) for a in ("wide", "context", "tensor"))
    w, c, t = (lax.axis_index(a) for a in ("wide", "context", "tensor"))
    return wide_n, ctx_n, ten_n // 2, w, c, t // 2, lax.rem(t, 2)


def greet_plane(bar, wide_n, y_n, w, y, k):
    for o in range(1, wide_n * y_n * 2):
        j = lax.rem((w * y_n + y) * 2 + k + o, wide_n * y_n * 2)
        pl.semaphore_signal(
            bar,
            inc=1,
            device_id={"wide": j // (y_n * 2), "tensor": lax.rem(j, y_n * 2)},
            device_id_type=pl.DeviceIdType.MESH,
        )
    return wide_n * y_n * 2 - 1


def near_first(c, ctx_n):
    seq = []
    for j in range(ctx_n):
        cb = 0
        for p in range(ctx_n):
            order = sorted(range(ctx_n), key=lambda q: (abs(q - p), q))
            cb = jnp.where(c == p, order[j], cb)
        seq.append(cb)
    return seq


def gather_kernel(pack, small, full, smalls, csem, crecv, wsem, wrecv, ysem, yrecv, ksem, krecv, ssem, srecv, local):
    wide_n, ctx_n, y_n, w, c, y, k = spot()
    bar = pltpu.get_barrier_semaphore()
    met = greet_plane(bar, wide_n, y_n, w, y, k)

    @pl.when(c > 0)
    def _():
        pl.semaphore_signal(bar, inc=1, device_id={"context": c - 1}, device_id_type=pl.DeviceIdType.MESH)

    @pl.when(c < ctx_n - 1)
    def _():
        pl.semaphore_signal(bar, inc=1, device_id={"context": c + 1}, device_id_type=pl.DeviceIdType.MESH)

    mine = pltpu.make_async_copy(pack, full.at[c, w, y, k], local.at[0])
    mine_small = pltpu.make_async_copy(small, smalls.at[w, y, k], local.at[1])
    mine.start()
    mine_small.start()
    pl.semaphore_wait(bar, met + (c + ctx_n - 1) // ctx_n + (2 * ctx_n - 2 - c) // ctx_n)

    def along(cb, side, src):
        return remote(src, full.at[cb, w, y, k], csem.at[side, cb], crecv.at[cb], context=c + 2 * side - 1)

    for side in (0, 1):

        @pl.when((c > 0) if side == 0 else (c < ctx_n - 1))
        def _():
            along(c, side, pack).start()

    def small_copy(o):
        j = lax.rem((w * y_n + y) * 2 + k + o, wide_n * y_n * 2)
        return remote(
            small, smalls.at[w, y, k], ssem.at[o], srecv.at[o], wide=j // (y_n * 2), tensor=lax.rem(j, y_n * 2)
        )

    for o in range(1, wide_n * y_n * 2):
        small_copy(o).start()

    seq = near_first(c, ctx_n)

    def leg(cb, number, o, start):
        even = lax.rem(cb, 2) == 0
        for on_wide in (True, False):
            n = wide_n if on_wide else y_n
            if o >= n:
                continue
            first = number == 0
            want_even = on_wide == first

            @pl.when(even if want_even else jnp.logical_not(even))
            def _():
                if on_wide:
                    ref = full.at[cb, w, y, k] if first else full.at[cb, w, :, k]
                    to = {"wide": lax.rem(w + o, wide_n)}
                    sems = (wsem.at[cb, o], wrecv.at[cb, o])
                else:
                    ref = full.at[cb, w, y, k] if first else full.at[cb, :, y, k]
                    to = {"tensor": lax.rem(y + o, y_n) * 2 + k}
                    sems = (ysem.at[cb, o], yrecv.at[cb, o])
                cp = remote(ref, ref, *sems, **to)
                if start == "start":
                    cp.start()
                elif start == "recv":
                    cp.wait_recv()
                else:
                    cp.wait_send()

    most = max(wide_n, y_n)

    def core(cb):
        ref = full.at[cb, :, :, k]
        return remote(ref, ref, ksem.at[cb], krecv.at[cb], tensor=y * 2 + 1 - k)

    mine.wait()
    mine_small.wait()
    for step in range(ctx_n + 2):
        if step < ctx_n:
            cb = seq[step]
            if step > 0:
                along(cb, 0, pack).wait_recv()
                for side in (0, 1):
                    go = jnp.logical_and(cb > c, c > 0) if side == 0 else jnp.logical_and(cb < c, c < ctx_n - 1)

                    @pl.when(go)
                    def _():
                        along(cb, side, full.at[cb, w, y, k]).start()

            for o in range(1, most):
                leg(cb, 0, o, "start")
        if 0 < step <= ctx_n:
            cb = seq[step - 1]
            for o in range(1, most):
                leg(cb, 0, o, "recv")
            for o in range(1, most):
                leg(cb, 1, o, "start")
        if step > 1:
            cb = seq[step - 2]
            for o in range(1, most):
                leg(cb, 1, o, "recv")
            core(cb).start()
    for step in range(ctx_n):
        core(seq[step]).wait_recv()
    for o in range(1, wide_n * y_n * 2):
        cp = small_copy(o)
        cp.wait_recv()
        cp.wait_send()
    for step in range(ctx_n):
        cb = seq[step]
        for side in (0, 1):
            go = jnp.logical_and(cb >= c, c > 0) if side == 0 else jnp.logical_and(cb <= c, c < ctx_n - 1)

            @pl.when(go)
            def _():
                along(cb, side, pack).wait_send()

        for number in (0, 1):
            for o in range(1, most):
                leg(cb, number, o, "send")
        core(cb).wait_send()


def gather_weights(pack, small):
    wide_n, ctx_n, ten_n = (lax.axis_size(a) for a in ("wide", "context", "tensor"))
    y_n = ten_n // 2
    dma = pltpu.SemaphoreType.DMA
    vm = pl.BlockSpec(memory_space=pltpu.VMEM)
    return pl.pallas_call(
        gather_kernel,
        out_shape=(
            jax.ShapeDtypeStruct((ctx_n, wide_n, y_n, 2) + pack.shape, pack.dtype),
            jax.ShapeDtypeStruct((wide_n, y_n, 2) + small.shape, small.dtype),
        ),
        in_specs=[vm, vm],
        out_specs=(vm, vm),
        scratch_shapes=[
            dma((2, ctx_n)), dma((ctx_n,)),
            dma((ctx_n, wide_n)), dma((ctx_n, wide_n)),
            dma((ctx_n, y_n)), dma((ctx_n, y_n)),
            dma((ctx_n,)), dma((ctx_n,)),
            dma((wide_n * ten_n,)), dma((wide_n * ten_n,)),
            dma((2,)),
        ],
        compiler_params=pltpu.CompilerParams(collective_id=1, has_side_effects=True),
    )(pack, small)


def gelu_parts(x):
    a = 0.7978845608028654
    x2 = x * x
    th = jnp.tanh(a * x * (1.0 + 0.044715 * x2))
    val = 0.5 * x * (1.0 + th)
    der = 0.5 * (1.0 + th) + 0.5 * x * (1.0 - th * th) * (a * (1.0 + 3 * 0.044715 * x2))
    return val, der


def halves(values):
    high = values.astype(bf16).astype(f32)
    return high, values - high


def block_kernel(share, joined, *refs):
    (
        x_all, g_all, qkv_w, proj_w, gains_w, biases_w, router_w, up, down,
        lo, dxo, grad, smalls, e_in, e_act, e_hid, e_dexp,
        x_s, g_s, att_s, n1_s, da_s, qkv, heads, probs, resid, logits, asq, dres_s, dn_s, rows_s,
        send_s, got, r32, e_s, ret, got2, back_g, eo_all, comb_all, dsm, sblk,
        part, rcv1, rcv2, rcv3, acc3, rcv4, srcv, a_buf, x_buf,
        full_s, small_s, small_g, pack_s, small_p, turn, wsem, wrecv,
        lsem, esem, xsem, gsem, grecv, ksem, krecv, s2, r2, s3, r3, s4, r4, ss, sr, es, er, obuf_sem,
    ) = refs
    wide_n, ctx_n, y_n, w, c, y, k = spot()
    ten_n = 2 * y_n
    plane = wide_n * ten_n
    n = plane * ctx_n
    me = (w * ctx_n + c) * ten_n + y * 2 + k
    mine = (w * y_n + y) * 2 + k
    width, packed = x_s.shape[2], grad.shape[1]
    pack, small_in = (pack_s, small_p) if joined else (qkv_w, proj_w)
    cols = packed // 4
    per = cols // HEAD_DIM
    slots_n = rows_s.shape[0] // 8
    length = x_s.shape[1]
    small = small_s if joined else small_in

    def weight(cb, lo_col, hi_col):
        if joined:
            return full_s[cb, :, :, :, :, lo_col:hi_col].reshape(width, hi_col - lo_col)
        return pack[cb, :, lo_col:hi_col]

    rows = grad.shape[0]
    logit_scale = 1.6 * math.sqrt(width)
    seq = near_first(c, ctx_n)
    bar = pltpu.get_barrier_semaphore()

    def place(d):
        return {"wide": d // (ctx_n * ten_n), "context": lax.rem(d // ten_n, ctx_n), "tensor": lax.rem(d, ten_n)}

    def hello(o, carry):
        pl.semaphore_signal(bar, inc=1, device_id=place(lax.rem(me + o, n)), device_id_type=pl.DeviceIdType.MESH)
        return carry

    lax.fori_loop(1, n, hello, 0)
    ins = [
        pltpu.make_async_copy(x_all.at[pl.ds(c * share, share)], x_s, lsem.at[0]),
        pltpu.make_async_copy(g_all.at[pl.ds(c * share, share)], g_s, lsem.at[1]),
    ]
    for cp in ins:
        cp.start()
    rows_s[...] = jnp.zeros_like(rows_s)
    dsm[...] = jnp.zeros_like(dsm)
    tall = length + -length % 16
    gap = tall - length // 16 * 16
    for i in range(share):
        edge = pl.ds(i * tall + tall - gap, gap)
        n1_s[edge, :] = jnp.zeros((gap, width), bf16)
        da_s[edge, :] = jnp.zeros((gap, width), bf16)
        for cb in range(ctx_n):
            heads[cb, edge, :] = jnp.zeros((gap, cols), bf16)

    def of(i):
        return pl.ds(pl.multiple_of(i * tall, 16), length)


    def along(a, cb, i, side, own):
        ref = (lo, dxo)[a].at[cb * share + i]
        src = (att_s, x_s)[a].at[i] if own else ref
        return remote(src, ref, gsem.at[a, side, cb, i], grecv.at[a, cb, i], context=c + 2 * side - 1)

    def launch(a, i):
        for side in (0, 1):

            @pl.when((c > 0) if side == 0 else (c < ctx_n - 1))
            def _():
                along(a, c, i, side, True).start()

    spare = ctx_n > 2

    def onward(cb, side, a=1):
        if side == 0:
            go, end = jnp.logical_and(cb > c, c > 0), jnp.logical_and(c == 1, cb == ctx_n - 1)
        else:
            go, end = jnp.logical_and(cb < c, c < ctx_n - 1), jnp.logical_and(c == ctx_n - 2, cb == 0)
        return jnp.logical_and(go, jnp.logical_not(end)) if a == 0 and spare else go

    def at_end(cb):
        return jnp.logical_or(
            jnp.logical_and(c == 0, cb == ctx_n - 1), jnp.logical_and(c == ctx_n - 1, cb == 0)
        )

    def pump(a, steps, i):
        for step in steps:
            cb = seq[step]
            for side in (0, 1):

                @pl.when(onward(cb, side, a))
                def _():
                    along(a, cb, i, 0, False).wait_recv()
                    along(a, cb, i, side, False).start()

    def arrived(a, step, i):
        cb = seq[step]
        passed = jnp.logical_or(onward(cb, 0, a), onward(cb, 1, a))
        if a == 0 and spare:
            passed = jnp.logical_or(passed, at_end(cb))

        @pl.when(jnp.logical_not(passed))
        def _():
            along(a, cb, i, 0, False).wait_recv()

    near, far = list(range(1, min(3, ctx_n))), list(range(3, ctx_n))

    half = rows // 2

    def w_ctx(cb, side, own):
        ref = full_s.at[cb, w, y, k]
        return remote(pack if own else ref, ref, wsem.at[0, cb, side], wrecv.at[0, cb, 0], context=c + 2 * side - 1)

    def w_leg(cb, number, h, o):
        at = pl.ds(h * half, half)
        slot = number * 2 + h
        if (number == 0) == (h == 0):
            ref = full_s.at[cb, w, y, k, at] if number == 0 else full_s.at[cb, w, :, k, at]
            to = {"wide": lax.rem(w + o, wide_n)}
        else:
            ref = full_s.at[cb, w, y, k, at] if number == 0 else full_s.at[cb, :, y, k, at]
            to = {"tensor": lax.rem(y + o, y_n) * 2 + k}
        return remote(ref, ref, wsem.at[1 + slot, cb, o], wrecv.at[1 + slot, cb, o], **to)

    def w_legs(cb, number):
        out = []
        for h in (0, 1):
            on_wide = (number == 0) == (h == 0)
            out += [w_leg(cb, number, h, o) for o in range(1, wide_n if on_wide else y_n)]
        return out

    def w_core(cb):
        ref = full_s.at[cb, :, :, k]
        return remote(ref, ref, wsem.at[5, cb, 0], wrecv.at[5, cb, 0], tensor=y * 2 + 1 - k)

    def w_small(o):
        j = lax.rem(mine + o, plane)
        to = {"wide": j // ten_n, "tensor": lax.rem(j, ten_n)}
        return remote(small_in, small_g.at[w, y, k], wsem.at[6, 0, o], wrecv.at[6, 0, o], **to)

    def w_arrive(j):
        cb = seq[j]
        if j > 0:
            w_ctx(cb, 0, False).wait_recv()
            for side in (0, 1):

                @pl.when(onward(cb, side))
                def _():
                    w_ctx(cb, side, False).start()

        for cp in w_legs(cb, 0):
            cp.start()

    def w_second(j):
        for cp in w_legs(seq[j], 0):
            cp.wait_recv()
        for cp in w_legs(seq[j], 1):
            cp.start()

    def w_third(j):
        for cp in w_legs(seq[j], 1):
            cp.wait_recv()
        w_core(seq[j]).start()

    def w_ready(j):
        if joined:
            w_core(seq[j]).wait_recv()

    if joined:
        turn[:cols, :rows] = proj_w[...].astype(f32)
        pieces = [qkv_w[j] for j in range(3)] + [turn[...].T[:rows, :cols].astype(bf16)]
        pack_s[...] = jnp.concatenate(pieces, axis=1)
        lines = jnp.concatenate([r[...].astype(f32) for r in (gains_w, biases_w, router_w)], axis=0)
        turn[: lines.shape[0], :rows] = lines
        small_p[...] = turn[: small_p.shape[0], : small_p.shape[1]].astype(bf16)
        full_s[c, w, y, k] = pack[...]
        small_g[w, y, k] = small_in[...]
    pl.semaphore_wait(bar, n - 1)
    if joined:
        for side in (0, 1):

            @pl.when((c > 0) if side == 0 else (c < ctx_n - 1))
            def _():
                w_ctx(c, side, True).start()

        w_arrive(0)
        for o in range(1, plane):
            w_small(o).start()
        for o in range(1, plane):
            w_small(o).wait_recv()
        pieces = [small_g[j // ten_n, (j // 2) % y_n, j % 2][:, :rows] for j in range(plane)]
        small_s[...] = jnp.concatenate([p.astype(f32) for p in pieces], axis=1)
    keys, key_scale = router_unit(small[4 : 4 + slots_n, :].astype(f32))
    keys_hi, keys_lo = halves(keys)
    keys_two = jnp.concatenate([keys_hi, keys_lo], axis=0).astype(bf16)
    keys_three = jnp.concatenate([keys_hi, keys_lo, keys_hi], axis=0).astype(bf16)
    for cp in ins:
        cp.wait()

    def norm_first(i, carry):
        hat, _ = layer_stats(x_s[i].astype(f32))
        n1_s[of(i), :] = (hat * small[0:1, :].astype(f32) + small[2:3, :].astype(f32)).astype(bf16)
        return carry

    lax.fori_loop(0, share, norm_first, 0)

    def between(j, i):
        todo = {}
        if joined:
            todo = {
                (0, 0): lambda: w_third(1),
                (0, 1): lambda: w_second(2),
                (0, 2): lambda: w_arrive(3),
                (1, 0): lambda: w_third(2),
                (1, 1): lambda: w_second(3),
                (2, 0): lambda: w_third(3),
            }
        return todo.get((j, i))

    if joined:
        w_second(0)
        w_arrive(1)
        w_third(0)
        w_second(1)
        w_arrive(2)
    for j in range(ctx_n):
        w_ready(j)
        cb = seq[j]
        qkv_f = mm(n1_s[...], weight(cb, 0, 3 * cols))
        qkv[cb] = jnp.concatenate([qkv_f[:, :cols] * 0.125, qkv_f[:, cols:]], axis=1).astype(bf16)

        def attend(i, carry):
            for at in range(share):
                if between(j, at) is not None:
                    pl.when(i == at)(between(j, at))
            qkv_c = qkv[cb, of(i), :]
            mixed = []
            for h in range(per):
                q, kk, v = head_parts(qkv_c, h, per)
                s = mm(q, kk, NT)
                e = jnp.exp(s - jnp.max(s, axis=1, keepdims=True))
                p = (e * (1.0 / jnp.sum(e, axis=1, keepdims=True))).astype(bf16)
                probs[i, cb, h] = p
                mixed.append(mm(p, v).astype(bf16))
            heads[cb, of(i), :] = jnp.concatenate(mixed, axis=1)
            return carry

        lax.fori_loop(0, share, attend, 0)
        add = mm(heads[cb], weight(cb, 3 * cols, packed), NT)
        if j == 0:
            resid[...] = add
        else:
            resid[...] += add

    def attention_out(i, carry):
        att_s[i] = resid[of(i), :].astype(bf16)
        return carry

    lax.fori_loop(0, share, attention_out, 0)

    def route(i, carry):
        att = resid[of(i), :]
        asq[i] = jnp.full(asq.shape[1:], jnp.sum(att * att), f32)
        res = x_s[i].astype(f32) + att
        resid[of(i), :] = res
        hat2, _ = layer_stats(res)
        second = hat2 * small[1:2, :].astype(f32) + small[3:4, :].astype(f32)
        unit = second * lax.rsqrt(jnp.sum(second * second, axis=-1, keepdims=True) + norm_eps)
        unit_hi, unit_lo = halves(unit)
        lg = mm(keys_two, unit_hi.astype(bf16), NT)
        lg = lg[:slots_n] + lg[slots_n:] + mm(keys_two[:slots_n], unit_lo.astype(bf16), NT)
        lg = logit_scale * lg
        logits[i] = lg
        disp = soft(lg, 1).astype(bf16)
        comb = soft(lg, 0).astype(bf16)
        comb_all[c, i, :, :length] = comb
        slots = mm(disp, second.astype(bf16)).astype(bf16)
        dexp = mm(comb, g_s[i]).astype(bf16)
        rows_s[...] += mm(pick_rows(slots_n, i), slots) + mm(pick_rows(slots_n, i + 4), dexp)
        return carry

    lax.fori_loop(0, share, route, 0)

    for e in range(slots_n):
        send_s[e] = rows_s[e * 8 : e * 8 + 8, :].astype(bf16)
    spot_e = w * ctx_n + c
    spot_t = y * 2 + k
    pairs_n = wide_n * ctx_n

    def expert_at(o):
        p = lax.rem(spot_e + o, pairs_n)
        return p, {"wide": p // ctx_n, "context": lax.rem(p, ctx_n)}

    def drain(ref, count, sem):
        some = ref.at[pl.ds(0, count)]
        pltpu.make_async_copy(some, some, sem).wait()

    for o in range(1, pairs_n):
        p, to = expert_at(o)
        remote(send_s.at[p], got.at[spot_t, spot_e], esem.at[0], esem.at[1], **to).start()
    got[spot_t, spot_e] = send_s[spot_e]
    for i in range(share):
        launch(0, i)
    drain(got.at[spot_t], pairs_n - 1, esem.at[1])
    for o in range(1, ten_n):
        mine_in = got.at[spot_t]
        remote(mine_in, mine_in, esem.at[2], esem.at[3], tensor=lax.rem(spot_t + o, ten_n)).start()
    drain(got, ten_n - 1, esem.at[3])

    group = min(n, 32)
    chunk = group * 8
    first = lax.rem(lax.broadcasted_iota(jnp.int32, (chunk, 1), 0), 8) < 4

    def expert_out(b, j):
        dst = (e_in, e_act, e_hid, e_dexp)[j]
        at = pl.ds(pl.multiple_of(b * chunk, chunk), chunk)
        return pltpu.make_async_copy(e_s.at[j], dst.at[at, :], xsem.at[j])

    def experts(b, carry):
        def widen(j, carry):
            r32[pl.ds(pl.multiple_of(j * 8, 8), 8), :] = got[(b * group + j) // pairs_n, lax.rem(b * group + j, pairs_n)].astype(f32)
            return carry

        lax.fori_loop(0, group, widen, 0)

        @pl.when(b > 0)
        def _():
            for j in range(4):
                expert_out(b, j).wait()

        low = r32[...].astype(bf16)
        e_s[0] = low
        e_s[3] = pltpu.roll(r32[...], chunk - 4, 0).astype(bf16)
        hidden = mm(low, up[...])
        act_g = pltpu.roll(mm(low, down[...], NT), chunk - 4, 0)
        val, der = gelu_parts(hidden)
        active = jnp.where(first, val, 0.0).astype(bf16)
        hid_g = jnp.where(first, act_g * der, 0.0).astype(bf16)
        e_s[1] = active
        e_s[2] = hid_g
        part_o = mm(active, down[...])
        part_s = mm(hid_g, up[...], NT)
        r32[...] = jnp.where(first, part_o, pltpu.roll(part_s, 4, 0))
        for j in range(4):
            expert_out(b, j).start()

        def narrow(j, carry):
            ret[(b * group + j) // pairs_n, lax.rem(b * group + j, pairs_n)] = r32[pl.ds(pl.multiple_of(j * 8, 8), 8), :].astype(bf16)
            return carry

        lax.fori_loop(0, group, narrow, 0)
        return carry

    lax.fori_loop(0, n // group, experts, 0)

    for o in range(1, ten_n):
        p = lax.rem(spot_t + o, ten_n)
        remote(ret.at[p], got2.at[spot_t], esem.at[4], esem.at[5], tensor=p).start()
    got2[spot_t] = ret[spot_t]
    drain(got2, ten_n - 1, esem.at[5])
    drain(send_s, pairs_n - 1, esem.at[0])

    def total(e, carry):
        s = got2[0, e].astype(f32)
        for t in range(1, ten_n):
            s = s + got2[t, e].astype(f32)
        send_s[e] = s.astype(bf16)
        return carry

    lax.fori_loop(0, pairs_n, total, 0)
    for o in range(1, pairs_n):
        p, to = expert_at(o)
        remote(send_s.at[p], back_g.at[spot_e], esem.at[6], esem.at[7], **to).start()
    back_g[spot_e] = send_s[spot_e]
    for i in range(share):
        pump(0, near, i)
    drain(back_g, pairs_n - 1, esem.at[7])

    def spread(e, carry):
        rows_s[pl.ds(pl.multiple_of(e * 8, 8), 8), :] = back_g[e].astype(f32)
        return carry

    lax.fori_loop(0, slots_n, spread, 0)
    back = rows_s[...].astype(bf16)
    for i in range(share):
        eo_all[c, i] = mm(pick_rows(slots_n, i), back, TN).astype(bf16)

    def trade(o, ref, j, p):
        return remote(ref.at[p], ref.at[p], es.at[j, o], er.at[j, o], context=lax.rem(c + o, ctx_n))

    for o in range(1, ctx_n):
        trade(o, eo_all, 0, c).start()
        trade(o, comb_all, 1, c).start()

    def fetch(step, i, slot):
        img = seq[step] * share + i
        return (
            pltpu.make_async_copy(lo.at[img], a_buf.at[slot], obuf_sem.at[0, slot]),
            pltpu.make_async_copy(x_all.at[img], x_buf, obuf_sem.at[1, slot]),
        )

    def put(step, i, slot):
        img = seq[step] * share + i
        return pltpu.make_async_copy(a_buf.at[slot], lo.at[img], obuf_sem.at[2, slot])

    def backward(i, carry):
        gain1, gain2 = small[0:1, :].astype(f32), small[1:2, :].astype(f32)
        g_low = g_s[i]
        res = resid[of(i), :]
        hat2, spread2 = layer_stats(res)
        second = hat2 * gain2 + small[3:4, :].astype(f32)
        tokens = second.astype(bf16)
        row_scale = lax.rsqrt(jnp.sum(second * second, axis=-1, keepdims=True) + norm_eps)
        unit = second * row_scale
        eo = eo_all[c, i]
        ds = mm(pick_rows(slots_n, i + 4), rows_s[...].astype(bf16), TN).astype(bf16)
        lg = logits[i]
        disp = soft(lg, 1)
        comb = soft(lg, 0)
        mixture = mm(comb.astype(bf16), eo, TN)
        result = res + mixture

        @pl.when(i > 1)
        def _():
            put(0, 0, 0).wait()

        a_buf[lax.rem(i, 2)] = result.astype(bf16)
        put(0, i, lax.rem(i, 2)).start()
        count = 1.0 / (length * width)
        lane = lax.broadcasted_iota(jnp.int32, (8, smalls.shape[2]), 1)
        sums = jnp.where(
            lane == 0,
            jnp.sum(result * result),
            jnp.where(lane == 1, asq[i], jnp.sum(mixture * mixture)),
        )
        at_row = lax.broadcasted_iota(jnp.int32, (8, smalls.shape[2]), 0)
        sblk[plane, :8, :] = jnp.where(at_row == i, jnp.sqrt(sums * count), sblk[plane, :8, :])
        dcomb = mm(eo, g_low, NT)
        ddisp = mm(ds, tokens, NT)
        dtok = mm(disp.astype(bf16), ds, TN)
        dlg = comb * (dcomb - jnp.sum(comb * dcomb, axis=0, keepdims=True)) + disp * (
            ddisp - jnp.sum(disp * ddisp, axis=1, keepdims=True)
        )
        dlg_hi, dlg_lo = halves(dlg)
        dlg_two = jnp.concatenate([dlg_hi, dlg_lo], axis=0).astype(bf16)
        dlg_three = jnp.concatenate([dlg_hi, dlg_hi, dlg_lo], axis=0).astype(bf16)
        dunit = logit_scale * mm(dlg_three, keys_three, TN)
        unit_hi, unit_lo = halves(unit)
        dk_part = mm(dlg_two, unit_hi.astype(bf16))
        dk_part = dk_part[:slots_n] + dk_part[slots_n:] + mm(dlg_two[:slots_n], unit_lo.astype(bf16))
        dsm[4 : 4 + slots_n, :] += logit_scale * dk_part
        dsec = dtok + row_scale * (dunit - unit * jnp.sum(unit * dunit, axis=-1, keepdims=True))
        dsm[1:2, :] += jnp.sum(dsec * hat2, axis=0, keepdims=True)
        dsm[3:4, :] += jnp.sum(dsec, axis=0, keepdims=True)
        dres = g_low.astype(f32) + norm_back(dsec * gain2, hat2, spread2)
        dres_s[...] = dres
        dattn = dres.astype(bf16)
        da_s[of(i), :] = dattn
        hat, spread = layer_stats(x_s[i].astype(f32))
        dn_s[...] = jnp.zeros_like(dn_s)

        def block(cb, carry):
            for at, a, steps, img in (
                ((0, 1), 0, far, 0),
                ((0, 3), 0, far, 1),
                ((1, 0), 0, far, 2),
                ((1, 3), 1, near, 0),
                ((2, 2), 1, far, 0),
                ((2, 3), 1, near, 1),
            ):

                @pl.when(jnp.logical_and(i == at[0], cb == at[1]))
                def _():
                    pump(a, steps, img)

            dheads = mm(dattn, weight(cb, 3 * cols, packed)).astype(bf16)
            qkv_c = qkv[cb, of(i), :]
            along_heads = dheads.astype(f32) * heads[cb, of(i), :].astype(f32)
            grads = [[], [], []]
            for h in range(per):
                q, kk, v = head_parts(qkv_c, h, per)
                at = slice(h * HEAD_DIM, (h + 1) * HEAD_DIM)
                dh = dheads[:, at]
                p = probs[i, cb, h]
                dp = mm(dh, v, NT) - jnp.sum(along_heads[:, at], axis=1, keepdims=True)
                dsc = (p.astype(f32) * dp).astype(bf16)
                grads[0].append((mm(dsc, kk) * 0.125).astype(bf16))
                grads[1].append(mm(dsc, q, TN).astype(bf16))
                grads[2].append(mm(p, dh, TN).astype(bf16))
            dqkv = jnp.concatenate(grads[0] + grads[1] + grads[2], axis=1)
            qkv[cb, of(i), :] = dqkv
            dn_s[...] += mm(dqkv, weight(cb, 0, 3 * cols), NT)
            return carry

        lax.fori_loop(0, ctx_n, block, 0)
        dn = dn_s[...]
        dsm[0:1, :] += jnp.sum(dn * hat, axis=0, keepdims=True)
        dsm[2:3, :] += jnp.sum(dn, axis=0, keepdims=True)
        x_s[i] = (dres_s[...] + norm_back(dn * gain1, hat, spread)).astype(bf16)
        launch(1, i)
        return carry

    sblk[plane] = jnp.zeros(sblk.shape[1:], f32)
    lax.fori_loop(0, share, backward, 0)
    outs = [pltpu.make_async_copy(x_s, dxo.at[pl.ds(c * share, share)], lsem.at[1])]
    for cp in outs:
        cp.start()
    dkeys = dsm[4 : 4 + slots_n, :]
    dsm[4 : 4 + slots_n, :] = key_scale * (dkeys - keys * jnp.sum(keys * dkeys, axis=1, keepdims=True))

    def core(cc):
        return remote(part.at[cc, :, :, 1 - k], rcv1.at[cc], ksem.at[cc], krecv.at[cc], tensor=y * 2 + 1 - k)

    normed_t = n1_s[...].T
    dattn_t = da_s[...].T
    for cc in range(ctx_n):
        from_qkv = mm(normed_t, qkv[cc]).astype(bf16)
        from_proj = mm(dattn_t, heads[cc]).astype(bf16)
        for j in range(plane):
            at = (cc, j // ten_n, (j // 2) % y_n, j % 2)
            part[at + (slice(None), slice(0, 3 * cols))] = from_qkv[j * rows : (j + 1) * rows]
            part[at + (slice(None), slice(3 * cols, packed))] = from_proj[j * rows : (j + 1) * rows]
        core(cc).start()
        if cc == ctx_n - 1:
            pump(1, far, 1)
            pump(1, near, 2)
    for j in range(plane):
        sblk[j, :, :rows] = dsm[:, j * rows : (j + 1) * rows]

    def small1(o):
        j = lax.rem(mine + o, plane)
        return remote(sblk.at[j], srcv.at[o], ss.at[o], sr.at[o], wide=j // ten_n, tensor=lax.rem(j, ten_n))

    for o in range(1, plane):
        small1(o).start()

    def hop(cc, number, o):
        on_wide = (cc % 2 == 0) == (number == 2)
        ss_, rr_ = (s2, r2) if number == 2 else (s3, r3)
        if on_wide:
            p = lax.rem(w + o, wide_n)
            to = {"wide": p}
            frm = rcv1.at[cc, p] if number == 2 else rcv1.at[cc, p, y]
            into = rcv2.at[cc, pl.ds(o * y_n, y_n)] if number == 2 else rcv3.at[cc, o]
        else:
            p = lax.rem(y + o, y_n)
            to = {"tensor": p * 2 + k}
            frm = rcv1.at[cc, :, p] if number == 2 else rcv1.at[cc, w, p]
            into = rcv2.at[cc, pl.ds(o * wide_n, wide_n)] if number == 2 else rcv3.at[cc, o]
        return remote(frm, into, ss_.at[cc, o], rr_.at[cc, o], **to)

    def peers(cc, number):
        on_wide = (cc % 2 == 0) == (number == 2)
        return range(1, wide_n if on_wide else y_n)

    for cc in range(ctx_n):
        core(cc).wait_recv()
        for wi in range(wide_n):
            for yi in range(y_n):
                rcv1[cc, wi, yi] = (part[cc, wi, yi, k].astype(f32) + rcv1[cc, wi, yi].astype(f32)).astype(bf16)
        for o in peers(cc, 2):
            hop(cc, 2, o).start()

    for o in range(1, ctx_n):
        p = lax.rem(c + ctx_n - o, ctx_n)
        trade(o, eo_all, 0, p).wait_recv()
        trade(o, comb_all, 1, p).wait_recv()

    order = [(s, i) for s in range(1, ctx_n) for i in range(share)]
    used = [share]

    def attend_here():
        hat, _ = layer_stats(x_buf[...].astype(f32))
        normed = (hat * small[0:1, :].astype(f32) + small[2:3, :].astype(f32)).astype(bf16)
        dn_s[...] = jnp.zeros_like(dn_s)

        def block(cb, carry):
            qkv_f = mm(normed, weight(cb, 0, 3 * cols))
            qkv_c = jnp.concatenate([qkv_f[:, :cols] * 0.125, qkv_f[:, cols:]], axis=1).astype(bf16)
            mixed = []
            for h in range(per):
                q, kk, v = head_parts(qkv_c, h, per)
                s = mm(q, kk, NT)
                e = jnp.exp(s - jnp.max(s, axis=1, keepdims=True))
                p = (e * (1.0 / jnp.sum(e, axis=1, keepdims=True))).astype(bf16)
                mixed.append(mm(p, v).astype(bf16))
            dn_s[...] += mm(jnp.concatenate(mixed, axis=1), weight(cb, 3 * cols, packed), NT)
            return carry

        lax.fori_loop(0, ctx_n, block, 0)

    def mix(todo):
        for step, i in todo:
            cb = seq[step]
            slot = used[0] % 2
            used[0] += 1
            for side in (0, 1):

                @pl.when(onward(cb, side, 0))
                def _():
                    along(0, cb, i, side, False).wait_send()

            arrived(0, step, i)
            put(step, i, slot).wait()
            far_att, own_x = fetch(step, i, slot)
            own_x.start()
            if spare and step == ctx_n - 1:

                @pl.when(jnp.logical_not(at_end(cb)))
                def _():
                    far_att.start()
                    far_att.wait()
                    dn_s[...] = a_buf[slot].astype(f32)

                own_x.wait()
                pl.when(at_end(cb))(attend_here)
                att = dn_s[...]
            else:
                far_att.start()
                far_att.wait()
                own_x.wait()
                att = a_buf[slot].astype(f32)
            mixed = mm(comb_all[cb, i, :, :length], eo_all[cb, i], TN)
            a_buf[slot] = (x_buf[...].astype(f32) + att + mixed).astype(bf16)
            put(step, i, slot).start()

    third = len(order) // 3
    mix(order[:third] + order[2 * third : 2 * third + 1])
    for cc in range(ctx_n):
        on_wide = cc % 2 == 0
        for o in peers(cc, 2):
            hop(cc, 2, o).wait_recv()
        for j in range(y_n if on_wide else wide_n):
            spot_j = (cc, w, j) if on_wide else (cc, j, y)
            tot = rcv1[spot_j].astype(f32)
            for o in peers(cc, 2):
                tot = tot + rcv2[cc, o * (y_n if on_wide else wide_n) + j].astype(f32)
            rcv1[spot_j] = tot.astype(bf16)
        for o in peers(cc, 3):
            hop(cc, 3, o).start()

    tot = sblk[mine]
    for o in range(1, plane):
        small1(o).wait_recv()
        tot = tot + srcv[o]
    smalls[c, : sblk.shape[1], :] = tot
    smalls[c, sblk.shape[1] :, :] = sblk[plane, :8, :]

    def small2(o, p):
        return remote(
            smalls.at[p], smalls.at[p], ss.at[plane + o], sr.at[plane + o], context=lax.rem(c + o, ctx_n)
        )

    for o in range(1, ctx_n):
        small2(o, c).start()
    pump(1, far, 2)
    mix(order[third : 2 * third])

    def last(cc):
        return remote(acc3.at[cc], rcv4.at[c], s4.at[cc], r4.at[c], context=cc)

    for cc in range(ctx_n):
        for o in peers(cc, 3):
            hop(cc, 3, o).wait_recv()
        tot = rcv1[cc, w, y].astype(f32)
        for o in peers(cc, 3):
            tot = tot + rcv3[cc, o].astype(f32)
        acc3[cc] = tot.astype(bf16)

        @pl.when(c != cc)
        def _():
            last(cc).start()

    mix(order[2 * third + 1 :])
    for step, i in order:
        arrived(1, step, i)
    tot = acc3[c].astype(f32)
    for o in range(1, ctx_n):
        p = lax.rem(c + o, ctx_n)
        remote(acc3.at[0], rcv4.at[p], s4.at[p], r4.at[p], context=p).wait_recv()
        tot = tot + rcv4[p].astype(f32)
    grad[...] = tot

    for slot in (0, 1):
        put(0, 0, slot).wait()
    for j in range(4):
        expert_out(0, j).wait()
    drain(got, ten_n - 1, esem.at[2])
    drain(ret, ten_n - 1, esem.at[4])
    drain(send_s, pairs_n - 1, esem.at[6])
    for o in range(1, ctx_n):
        p = lax.rem(c + ctx_n - o, ctx_n)
        small2(o, p).wait_recv()
        small2(o, c).wait_send()
        trade(o, eo_all, 0, c).wait_send()
        trade(o, comb_all, 1, c).wait_send()
        last(lax.rem(c + o, ctx_n)).wait_send()
    for o in range(1, plane):
        small1(o).wait_send()
    for cc in range(ctx_n):
        core(cc).wait_send()
        for number in (2, 3):
            for o in peers(cc, number):
                hop(cc, number, o).wait_send()
    for cp in outs:
        cp.wait()
    if joined:
        for o in range(1, plane):
            w_small(o).wait_send()
        for cb in range(ctx_n):
            for number in (0, 1):
                for cp in w_legs(cb, number):
                    cp.wait_send()
            w_core(cb).wait_send()
            for side in (0, 1):
                go = (cb >= c, c > 0) if side == 0 else (cb <= c, c < ctx_n - 1)

                @pl.when(jnp.logical_and(*go))
                def _():
                    w_ctx(cb, side, True).wait_send()

    for a in (0, 1):
        for i in range(share):
            for side in (0, 1):

                @pl.when((c > 0) if side == 0 else (c < ctx_n - 1))
                def _():
                    along(a, c, i, side, True).wait_send()

    for step, i in order:
        for side in (0, 1):

            @pl.when(onward(seq[step], side))
            def _():
                along(1, seq[step], i, side, False).wait_send()


def run_block(x_all, g_all, given, slots_n, up, down, rows, share):
    wide_n, ctx_n, ten_n = (lax.axis_size(a) for a in ("wide", "context", "tensor"))
    y_n = ten_n // 2
    plane = wide_n * ten_n
    n = plane * ctx_n
    most = max(wide_n, y_n)
    images, length, width = x_all.shape
    packed = 4 * (width // ctx_n)
    joined = len(given) == 5
    small_rows = 4 + slots_n + -(4 + slots_n) % 16
    if not joined:
        given = tuple(given) + (given[1],) * 3
    up8 = lambda v, m: v + -v % m
    cols = packed // 4
    ff = up.shape[1]
    par8 = 4 + slots_n + -(4 + slots_n) % 8
    lanes = rows + -rows % 128
    blk = (rows, packed)
    acts = (share, length, width)
    wide_len = length + -length % 128
    tall = length + -length % 16
    dma = pltpu.SemaphoreType.DMA
    vm = pl.BlockSpec(memory_space=pltpu.VMEM)
    hbm = pl.BlockSpec(memory_space=pl.ANY)
    V = pltpu.VMEM
    shape = jax.ShapeDtypeStruct
    return pl.pallas_call(
        functools.partial(block_kernel, share, joined),
        out_shape=(
            shape((images, length, width), bf16),
            shape((images, length, width), bf16),
            shape(blk, f32),
            shape((ctx_n, par8 + 8, lanes), f32),
            shape((n * 8, width), bf16),
            shape((n * 8, ff), bf16),
            shape((n * 8, ff), bf16),
            shape((n * 8, width), bf16),
        ),
        in_specs=[hbm, hbm] + [vm] * 2 + [vm if joined else hbm] * 3 + [vm] * 2,
        out_specs=(hbm, hbm, vm, vm) + (hbm,) * 4,
        scratch_shapes=[
            V(acts, bf16), V(acts, bf16), V(acts, bf16),
            V((share * tall, width), bf16),
            V((share * tall, width), bf16),
            V((ctx_n, share * tall, 3 * cols), bf16),
            V((ctx_n, share * tall, cols), bf16),
            V((share, ctx_n, cols // HEAD_DIM, length, length), bf16),
            V((share * tall, width), f32),
            V((share, slots_n, length), f32),
            V((share, 8, lanes), f32),
            V((length, width), f32),
            V((length, width), f32),
            V((slots_n * 8, width), f32),
            V((slots_n, 8, width), bf16),
            V((ten_n, slots_n, 8, width), bf16),
            V((min(n, 32) * 8, width), f32),
            V((4, min(n, 32) * 8, width), bf16),
            V((ten_n, slots_n, 8, width), bf16),
            V((ten_n, slots_n, 8, width), bf16),
            V((slots_n, 8, width), bf16),
            V((ctx_n, share, slots_n, width), bf16),
            V((ctx_n, share, slots_n, wide_len), bf16),
            V((par8, width), f32),
            V((plane + 1, par8, lanes), f32),
            V((ctx_n, wide_n, y_n, 2) + blk, bf16),
            V((ctx_n, wide_n, y_n) + blk, bf16),
            V((ctx_n, wide_n * y_n) + blk, bf16),
            V((ctx_n, most) + blk, bf16),
            V((ctx_n,) + blk, bf16),
            V((ctx_n,) + blk, bf16),
            V((plane, par8, lanes), f32),
            V((2, length, width), bf16),
            V((length, width), bf16),
            V((ctx_n, wide_n, y_n, 2) + blk if joined else (8, 128), bf16),
            V((small_rows, width) if joined else (8, 128), f32),
            V((wide_n, y_n, 2, small_rows, lanes) if joined else (8, 128), bf16),
            V(blk if joined else (8, 128), bf16),
            V((small_rows, lanes) if joined else (8, 128), bf16),
            V((up8(cols, 128), up8(rows, 128)) if joined else (8, 128), f32),
            dma((7, ctx_n, plane) if joined else (1,)), dma((7, ctx_n, plane) if joined else (1,)),
            dma((2,)), dma((8,)), dma((4,)),
            dma((2, 2, ctx_n, share)), dma((2, ctx_n, share)),
            dma((ctx_n,)), dma((ctx_n,)),
            dma((ctx_n, most)), dma((ctx_n, most)),
            dma((ctx_n, most)), dma((ctx_n, most)),
            dma((ctx_n,)), dma((ctx_n,)),
            dma((plane + ctx_n,)), dma((plane + ctx_n,)),
            dma((2, ctx_n)), dma((2, ctx_n)),
            dma((3, 2)),
        ],
        compiler_params=pltpu.CompilerParams(
            collective_id=2, has_side_effects=True, vmem_limit_bytes=67043328
        ),
    )(x_all, g_all, *given, up, down)


def last_kernel(share, params, *refs):
    (
        lo_in, dx_in, e_in, e_act, e_hid, e_dexp, grad, smalls,
        lo, dx, up_grad, down_grad, qkv_grad, proj_grad, gains, biases, router, rms,
        hold, turn, lines, isem, osem, usem,
    ) = refs
    groups = lo_in.shape[0] // share
    moves = [(a, b) for b in range(groups) for a in (0, 1)]

    def take(a, b):
        at = pl.ds(b * share, share)
        return pltpu.make_async_copy((lo_in, dx_in)[a].at[at], hold.at[a, at], isem.at[a, b])

    def give(a, b):
        at = pl.ds(b * share, share)
        return pltpu.make_async_copy(hold.at[a, at], (lo, dx)[a].at[at], osem.at[a, b])

    for m in moves:
        take(*m).start()
    up_grad[...] = mm(e_in[...], e_hid[...], TN)
    for m in moves[: len(moves) // 2]:
        take(*m).wait()
        give(*m).start()
    down_grad[...] = mm(e_act[...], e_dexp[...], TN)
    for m in moves[len(moves) // 2 :]:
        take(*m).wait()
        give(*m).start()
    rows, packed = grad.shape
    cols = packed // 4
    for j in range(3):
        qkv_grad[j] = grad[:, j * cols : (j + 1) * cols]
    turn[:rows, :cols] = grad[:, 3 * cols :]
    proj_grad[...] = turn[...].T[:cols, :rows]
    total = smalls[0]
    for b in range(1, groups):
        total = total + smalls[b]
    gains[...] = total[0:2, :rows]
    biases[...] = total[2:4, :rows]
    router[...] = total[4:params, :rows]
    mark = smalls.shape[1] - 8
    for b in range(groups):
        lines[b * share : (b + 1) * share, :] = smalls[b, mark : mark + share, :]
    rms[...] = lines[...].T[:3, : groups * share]
    for m in moves:
        give(*m).wait()


def run_last(lo, dx, e_in, e_act, e_hid, e_dexp, grad, smalls, share, params):
    rows, packed = grad.shape
    cols = packed // 4
    width, ff = e_in.shape[1], e_act.shape[1]
    images = lo.shape[0]
    groups = images // share
    vm = pl.BlockSpec(memory_space=pltpu.VMEM)
    hbm = pl.BlockSpec(memory_space=pl.ANY)
    shape = jax.ShapeDtypeStruct
    V = pltpu.VMEM
    up8 = lambda v, m: v + -v % m
    dma = pltpu.SemaphoreType.DMA
    return pl.pallas_call(
        functools.partial(last_kernel, share, params),
        out_shape=(
            shape(lo.shape, bf16), shape(dx.shape, bf16),
            shape((width, ff), f32), shape((ff, width), f32),
            shape((3, rows, cols), f32), shape((cols, rows), f32),
            shape((2, rows), f32), shape((2, rows), f32), shape((params - 4, rows), f32),
            shape((3, images), f32),
        ),
        in_specs=[hbm, hbm] + [vm] * 6,
        out_specs=(hbm, hbm) + (vm,) * 8,
        scratch_shapes=[
            V((2,) + lo.shape, bf16),
            V((up8(rows, 128), up8(cols, 128)), f32),
            V((128, 128), f32),
            dma((2, groups)), dma((2, groups)), dma((2,)),
        ],
    )(lo, dx, e_in, e_act, e_hid, e_dexp, grad, smalls)


def on_device(
    layer_input,
    qkv_weight,
    proj_weight,
    norm_gains,
    norm_biases,
    router_keys,
    up_weight,
    down_weight,
    out_cotangent,
):
    images, length, width = layer_input.shape
    wide_n, ctx_n, ten_n = (lax.axis_size(a) for a in ("wide", "context", "tensor"))
    share = images // ctx_n
    slots_n = router_keys.shape[1]
    rows, _, cols = qkv_weight.shape
    lanes = rows + -rows % 128

    params = 4 + slots_n
    if rows % 32 == 0:
        given = (qkv_weight.transpose(1, 0, 2), proj_weight, norm_gains, norm_biases, router_keys.T)
    else:
        pack = jnp.concatenate([qkv_weight.reshape(rows, 3 * cols), proj_weight.T], axis=1)
        small = jnp.concatenate([norm_gains, norm_biases, router_keys.T], axis=0)
        small = jnp.pad(small, ((0, -params % 16), (0, lanes - rows)))
        weights, small = gather_weights(pack, small)
        weights = weights.reshape(ctx_n, width, 4 * cols)
        small = small.reshape((-1,) + small.shape[3:])[:, :params, :rows]
        small = small.transpose(1, 0, 2).reshape(params, width)
        given = (weights, small)
    lo, dx, dpack, dsmall, *sides = run_block(
        layer_input, out_cotangent, given, slots_n, up_weight[0], down_weight[0], rows, share
    )
    lo, dx, up_grad, down_grad, qkv_grad, proj_grad, gains, biases, router, rms = run_last(
        lo, dx, *sides, dpack, dsmall, share, params
    )
    return (
        lo,
        rms.T,
        dx,
        qkv_grad.transpose(1, 0, 2),
        proj_grad,
        gains,
        biases,
        router.T,
        up_grad[None],
        down_grad[None],
    )


def solution(mesh):
    images = P(("wide", "tensor"), None, None)
    qkv = P(("wide", "tensor"), None, "context")
    proj = P("context", ("wide", "tensor"))
    lane = P(None, ("wide", "tensor"))
    rowed = P(("wide", "tensor"), None)
    up = P(("wide", "context"), None, "tensor")
    down = P(("wide", "context"), "tensor", None)
    return jax.shard_map(
        on_device,
        mesh=mesh,
        in_specs=(images, qkv, proj, lane, lane, rowed, up, down, images),
        out_specs=(images, rowed, images, qkv, proj, lane, lane, rowed, up, down),
        check_vma=False,
    )
```
